32 devices in a mesh: elem: 8 (over z, y), comp: 2 (over x), rep: 2 (over core).
Axes of the slice: x: 2, y: 2, z: 4, core: 2. Of those that a mesh axis runs over, the one named last changes fastest.
Arguments:
- velocity: float32 [3, 10, 10, 10, 2, 6144], P(None, 'comp', None, None, None, ('elem', 'rep')), may hold values from -6 to 6
- geometry: float32 [3, 3, 10, 10, 10, 2, 6144], P(None, None, 'comp', None, None, None, ('elem', 'rep')), may hold values from -40 to 40
- element_place: int32 [2, 6144], P('comp', ('elem', 'rep')), may hold values from 0 to 383, as said below
Outputs:
- pressure: float32 [10, 10, 10, 2, 6144], P(None, None, None, 'comp', ('elem', 'rep'))
The draws below stay inside these ranges and needn't reach their ends.
Inputs may be any that keep to these rules, and one draw needn't show every extreme that they name: `element_place`: in each row and each aligned run of 384 entries of it, every value 0 to 383 appears once.
All inputs are finite; a program needn't handle non-finite values.
Results may differ from the reference program's by a relative error of at most 0.000071.
Values sent between devices are 32-bit elements; how exact they have to be, the bound alone decides.
No kernel may reach another device: no remote copies, remote signals or barrier semaphores. Data moves between devices by JAX's collectives and lax.ppermute only.
A program may use at most 192 MiB of HBM per device.

```python
import jax
import jax.numpy as jnp
import numpy as np
from jax import lax

NODES = 10
BLOCK_X = 6
BLOCK_Y = 8
BLOCK_Z = 8
GRID_Y = 4
SUB_ELEMS = 384
ROW_ELEMS = 6144
BOX_X = 12
BOX_Y = 32
BOX_Z = 32
N_COMP = 2
N_REP = 2


def draw_geometry(key, part):
    base_key = jax.random.fold_in(key, 31)
    weight_key, mixing_key = jax.random.split(base_key)
    node_shape = (NODES, NODES, NODES, N_COMP, ROW_ELEMS)
    full_shape = (3, 3) + node_shape
    weights = jax.random.uniform(weight_key, node_shape, jnp.float32, 0.5, 2.0)
    mixing = 0.35 * jax.random.truncated_normal(mixing_key, -4.0, 4.0, full_shape, jnp.float32)
    mixing = mixing + jnp.eye(3, dtype=jnp.float32).reshape(3, 3, 1, 1, 1, 1, 1)
    return (weights[None, None] * mixing).astype(jnp.float32)


def draw_element_place(key, part):
    blocks = N_COMP * ROW_ELEMS // SUB_ELEMS
    block_keys = jax.random.split(jax.random.fold_in(key, 7), blocks)

    def one_order(block_key):
        return jax.random.permutation(block_key, SUB_ELEMS)
    orders = jax.vmap(one_order)(block_keys)
    return orders.reshape(N_COMP, ROW_ELEMS).astype(jnp.int32)


def steps_of(key, shape, pieces, smallest, top_value):
    gain, own = 1.0, jax.random.fold_in(key, 6)
    for axis_at, blocks in pieces:
        draws = jnp.exp(jax.random.uniform(jax.random.fold_in(own, axis_at), (blocks,), jnp.float32, smallest / len(pieces), top_value / len(pieces)))
        gain = gain * jnp.repeat(draws, shape[axis_at] // blocks).reshape([-1 if axis == axis_at else 1 for axis in range(len(shape))])
    return gain


def scatter_about(rng, shape, scale, most, cuts=(), held_as=jnp.bfloat16):
    drawn = jax.random.normal(rng, shape, jnp.float32) * scale
    if len(cuts) > 0:
        drawn = steps_of(rng, shape, cuts, -0.22, 0.18) * drawn
    return jnp.clip(drawn, min=-most, max=most).astype(held_as)


def setup_inputs(seed: int = 0) -> dict:
    key_of = jax.random.split(jax.random.key(seed), 4)
    return {
        "velocity": scatter_about(key_of[0], (3, NODES, NODES, NODES, N_COMP, ROW_ELEMS), 1.0, 6.0, ((1, 2), (5, 16)), jnp.float32),
        "geometry": draw_geometry(jax.random.fold_in(key_of[3], 71), 0),
        "element_place": draw_element_place(jax.random.fold_in(key_of[3], 71), 0),
    }


exact_mode = lax.Precision.HIGHEST


def legendre_columns(points, degree):
    columns = [points * 0.0 + 1.0, points]
    for order in range(2, degree + 1):
        columns.append(((2 * order - 1) * points * columns[order - 1] - (order - 1) * columns[order - 2]) / order)
    return columns


def derivative_table(node_count):
    degree = node_count - 1
    points = np.cos(np.pi * np.arange(node_count) / degree)
    for sweep in range(100):
        columns = legendre_columns(points, degree)
        points = points - (points * columns[degree] - columns[degree - 1]) / (node_count * columns[degree])
    points = np.sort(points)
    values = legendre_columns(points, degree)[degree]
    identity = np.eye(node_count)
    spacing = points[:, None] - points[None, :] + identity
    matrix = values[:, None] / (values[None, :] * spacing)
    matrix = np.where(identity > 0.5, 0.0, matrix)
    matrix[0, 0] = -degree * (degree + 1) / 4.0
    matrix[degree, degree] = degree * (degree + 1) / 4.0
    return matrix


def apply_transpose(deriv_table, flux_r, flux_s, flux_t):
    along_r = jnp.einsum("ia,i...->a...", deriv_table, flux_r, precision=exact_mode)
    along_s = jnp.einsum("ib,ai...->ab...", deriv_table, flux_s, precision=exact_mode)
    along_t = jnp.einsum("ic,abi...->abc...", deriv_table, flux_t, precision=exact_mode)
    return along_r + along_s + along_t


def local_pass(field, direction, block_grid):
    last_node = field.shape[0] - 1
    low_key = tuple(0 if dim_index == direction else slice(None) for dim_index in range(3))
    high_key = tuple(last_node if dim_index == direction else slice(None) for dim_index in range(3))
    lower = field[low_key]
    upper = field[high_key]
    leading = lower.shape[:-1]
    lower = lower.reshape(leading + tuple(block_grid))
    upper = upper.reshape(leading + tuple(block_grid))
    element_axis = len(leading) + direction
    extent = block_grid[direction]
    summed = lax.slice_in_dim(upper, 0, extent - 1, axis=element_axis) + lax.slice_in_dim(lower, 1, extent, axis=element_axis)
    upper = jnp.concatenate([summed, lax.slice_in_dim(upper, extent - 1, extent, axis=element_axis)], axis=element_axis)
    lower = jnp.concatenate([lax.slice_in_dim(lower, 0, 1, axis=element_axis), summed], axis=element_axis)
    field = field.at[low_key].set(lower.reshape(leading + (-1,)))
    return field.at[high_key].set(upper.reshape(leading + (-1,)))


def element_cells(element_place):
    row_index = jnp.arange(ROW_ELEMS, dtype=jnp.int32)[None, :]
    half_index = jnp.arange(N_COMP, dtype=jnp.int32)[:, None]
    block_index = row_index // SUB_ELEMS
    layers = N_COMP * N_REP
    sub_block = (block_index // N_REP) * layers + half_index * N_REP + block_index % N_REP
    cell_x = (sub_block // (GRID_Y * layers)) * BLOCK_X + element_place // (BLOCK_Y * BLOCK_Z)
    cell_y = ((sub_block // layers) % GRID_Y) * BLOCK_Y + (element_place // BLOCK_Z) % BLOCK_Y
    cell_z = (sub_block % layers) * BLOCK_Z + element_place % BLOCK_Z
    return ((cell_x * BOX_Y + cell_y) * BOX_Z + cell_z).astype(jnp.int32)


def reference(velocity, geometry, element_place):
    deriv_table = jnp.asarray(derivative_table(NODES), jnp.float32)
    fluxes = []
    for direction in range(3):
        fluxes.append(geometry[0, direction] * velocity[0] + geometry[1, direction] * velocity[1] + geometry[2, direction] * velocity[2])
    local_div = apply_transpose(deriv_table, fluxes[0], fluxes[1], fluxes[2])
    flat_cells = element_cells(element_place).reshape(-1).astype(jnp.int32)
    flat_local = local_div.reshape(NODES, NODES, NODES, N_COMP * ROW_ELEMS)
    box_field = jnp.zeros((NODES, NODES, NODES, BOX_X * BOX_Y * BOX_Z), jnp.float32)
    box_field = box_field.at[:, :, :, flat_cells].set(flat_local)
    for direction in range(3):
        box_field = local_pass(box_field, direction, (BOX_X, BOX_Y, BOX_Z))
    pressure = box_field[:, :, :, flat_cells]
    return pressure.reshape(NODES, NODES, NODES, N_COMP, ROW_ELEMS)
```

```python
import jax
import jax.numpy as jnp
import numpy as np
from jax import lax
from jax.experimental import pallas as pl
from jax.experimental.pallas import tpu as pltpu
from jax.sharding import PartitionSpec as P

BLOCK_X = 6
BLOCK_Y = 8
BLOCK_Z = 8
GRID_Y = 4
LANES = 128

SLAB_AXES = ((1, 2), (0, 2), (0, 1))


def legendre_columns(points, degree):
    columns = [points * 0.0 + 1.0, points]
    for order in range(2, degree + 1):
        columns.append(
            ((2 * order - 1) * points * columns[order - 1] - (order - 1) * columns[order - 2])
            / order
        )
    return columns


def derivative_table(node_count):
    degree = node_count - 1
    points = np.cos(np.pi * np.arange(node_count) / degree)
    for sweep in range(100):
        columns = legendre_columns(points, degree)
        points = points - (points * columns[degree] - columns[degree - 1]) / (
            node_count * columns[degree]
        )
    points = np.sort(points)
    values = legendre_columns(points, degree)[degree]
    identity = np.eye(node_count)
    spacing = points[:, None] - points[None, :] + identity
    matrix = values[:, None] / (values[None, :] * spacing)
    matrix = np.where(identity > 0.5, 0.0, matrix)
    matrix[0, 0] = -degree * (degree + 1) / 4.0
    matrix[degree, degree] = degree * (degree + 1) / 4.0
    return matrix


def weighted(terms):
    total = None
    for value, factor in terms:
        total = value * factor if total is None else total + value * factor
    return total


def transpose_line(line, table):
    count = len(line)
    half = count // 2
    even = [line[i] + line[count - 1 - i] for i in range(half)]
    odd = [line[i] - line[count - 1 - i] for i in range(half)]
    out = [None] * count
    for m in range(half):
        w = count - 1 - m
        both = weighted([(odd[i], float(0.5 * (table[i, m] + table[i, w]))) for i in range(half)])
        diff = weighted([(even[i], float(0.5 * (table[i, m] - table[i, w]))) for i in range(half)])
        out[m] = both + diff
        out[w] = both - diff
    return out


def rows_padded(node_count):
    return (node_count * node_count + 7) // 8 * 8


def flux_kernel(velocity, geometry, *, node_count):
    n = node_count
    planes = velocity.shape[1]
    groups = velocity.shape[5] // LANES
    halves = velocity.shape[4]
    table = derivative_table(n)
    pad = rows_padded(n)
    inner = n - 2

    def body(v_hbm, g_hbm, keep, send, faces, v, g, f0, f1, st, part, sem):
        step = pl.program_id(0)
        comp = lax.axis_index("comp")

        def copies(plane, slot):
            out = []
            for k in range(groups):
                lanes = pl.ds(k * LANES, LANES)
                subs = pl.ds(k * halves, halves)
                out.append(
                    pltpu.make_async_copy(
                        v_hbm.at[:, plane, :, :, :, lanes], v.at[slot, :, :, :, subs, :], sem.at[2 * k, slot]
                    )
                )
                out.append(
                    pltpu.make_async_copy(
                        g_hbm.at[:, :, plane, :, :, :, lanes],
                        g.at[slot, :, :, :, :, subs, :],
                        sem.at[2 * k + 1, slot],
                    )
                )
            return out

        slot = step % 2

        @pl.when(step == 0)
        def _():
            for c in copies(0, 0):
                c.start()

        @pl.when(step + 1 < planes)
        def _():
            for c in copies(step + 1, 1 - slot):
                c.start()

        for c in copies(step, slot):
            c.wait()

        def along_last(b, carry):
            line = []
            for c in range(n):
                vel = [v[slot, i, b, c] for i in range(3)]
                flux = [weighted([(g[slot, i, j, b, c], vel[i]) for i in range(3)]) for j in range(3)]
                f0[step, b, c] = flux[0]
                f1[b, c] = flux[1]
                line.append(flux[2])
            out = transpose_line(line, table)
            for c in range(n):
                st[step, b, c] = out[c]
            return carry

        lax.fori_loop(0, n, along_last, 0)

        def along_mid(c, carry):
            out = transpose_line([f1[b, c] for b in range(n)], table)
            for b in range(n):
                st[step, b, c] = st[step, b, c] + out[b]
            return carry

        lax.fori_loop(0, n, along_mid, 0)

        @pl.when(step == planes - 1)
        def _():
            first = comp == 0
            low = jnp.where(first, 1.0, 0.0)
            own = (low, 1.0 - low)
            coef = [
                [jnp.where(first, float(table[i, m]), float(table[planes + i, m])) for m in range(n)]
                for i in range(planes)
            ]

            def along_first(b, carry):
                for c in range(n):
                    line = [f0[i, b, c] for i in range(planes)]
                    for m in range(n):
                        total = weighted([(line[i], coef[i][m]) for i in range(planes)])
                        row = m * n * n + b * n + c
                        part[pl.ds(pl.multiple_of(row * 8, 8), 8), :] = total + st[m % planes, b, c] * own[m // planes]
                return carry

            lax.fori_loop(0, n, along_first, 0)
            for a in range(inner):
                for b in range(inner):
                    for k in range(groups):
                        base = ((a + 1) * n * n + (b + 1) * n + 1) * 8 + k * halves
                        zero = part[pl.ds(base, inner, stride=8), :]
                        one = part[pl.ds(base + 1, inner, stride=8), :]
                        dst = pl.ds(((a * inner + b) * groups + k) * inner, inner)
                        keep[dst, :] = jnp.where(first, zero, one)
                        send[dst, :] = jnp.where(first, one, zero)
            for h in range(halves):
                for k in range(groups):
                    sub = k * halves + h
                    for side in range(2):
                        at = side * (n - 1)
                        faces[h, side, k, 0 : n * n, :] = part[pl.ds(at * n * n * 8 + sub, n * n, stride=8), :]
                        for a in range(n):
                            faces[h, 2 + side, k, a * n : a * n + n, :] = part[
                                pl.ds((a * n * n + at * n) * 8 + sub, n, stride=8), :
                            ]
                        faces[h, 4 + side, k, 0 : n * n, :] = part[pl.ds(at * 8 + sub, n * n, stride=8 * n), :]

    tile = (8, LANES)
    count = inner * inner * inner * groups
    return pl.pallas_call(
        body,
        grid=(planes,),
        in_specs=[pl.BlockSpec(memory_space=pltpu.HBM), pl.BlockSpec(memory_space=pltpu.HBM)],
        out_specs=[
            pl.BlockSpec((count, LANES), lambda i: (0, 0)),
            pl.BlockSpec((count, LANES), lambda i: (0, 0)),
            pl.BlockSpec((halves, 6, groups, pad, LANES), lambda i: (0, 0, 0, 0, 0)),
        ],
        out_shape=[
            jax.ShapeDtypeStruct((count, LANES), jnp.float32),
            jax.ShapeDtypeStruct((count, LANES), jnp.float32),
            jax.ShapeDtypeStruct((halves, 6, groups, pad, LANES), jnp.float32),
        ],
        scratch_shapes=[
            pltpu.VMEM((2, 3, n, n) + tile, jnp.float32),
            pltpu.VMEM((2, 3, 3, n, n) + tile, jnp.float32),
            pltpu.VMEM((planes, n, n) + tile, jnp.float32),
            pltpu.VMEM((n, n) + tile, jnp.float32),
            pltpu.VMEM((planes, n, n) + tile, jnp.float32),
            pltpu.VMEM((n * n * n * 8, LANES), jnp.float32),
            pltpu.SemaphoreType.DMA((2 * groups, 2)),
        ],
        compiler_params=pltpu.CompilerParams(vmem_limit_bytes=48 * 2**20),
        name="flux",
    )(velocity, geometry)


def lane_iota(rows):
    return lax.broadcasted_iota(jnp.int32, (rows, LANES), 1)


def lane_part(rows, direction):
    lane = lane_iota(rows)
    if direction == 0:
        return lane // (BLOCK_Y * BLOCK_Z)
    if direction == 1:
        return lane // BLOCK_Z % BLOCK_Y
    return lane % BLOCK_Z


STRIDE = (BLOCK_Y * BLOCK_Z, BLOCK_Z, 1)


def turn(x, by):
    by = by % LANES
    return x if by == 0 else pltpu.roll(x, by, 1)


def split_dot(x, matrix, dims):
    high = x.astype(jnp.bfloat16)
    low = (x - high.astype(jnp.float32)).astype(jnp.bfloat16)
    one = lax.dot_general(high, matrix, (dims, ((), ())), preferred_element_type=jnp.float32)
    return one + lax.dot_general(low, matrix, (dims, ((), ())), preferred_element_type=jnp.float32)


def one_hot(place):
    size = place.shape[1]
    target = lax.broadcasted_iota(jnp.int32, (size, size), 0)
    return jnp.where(target == place, 1.0, 0.0).astype(jnp.bfloat16)


def shell(direction, faces, h, k, high):
    return faces[h, 2 * direction + (1 if high else 0), k]


def slots(direction, groups):
    return LANES // STRIDE[direction] if direction == 0 else (BLOCK_Y, BLOCK_Z)[direction - 1]


def payload_x(faces, groups, pad):
    lane = lane_iota(pad)
    low = lane < STRIDE[0]
    high_out = jnp.where(low, turn(faces[0, 1, groups - 1], STRIDE[0]), faces[1, 1, groups - 1])
    low_out = jnp.where(low, faces[0, 0, 0], turn(faces[1, 0, 0], STRIDE[0]))
    return high_out, low_out


def gather_slots(pad, direction, pieces):
    part = lane_part(pad, direction)
    out = jnp.zeros((pad, LANES), jnp.float32)
    for slot, source, value in pieces:
        out = jnp.where(part == slot, turn(value, (slot - source) * STRIDE[direction]), out)
    return out


def payload_y(faces, groups, pad, halves):
    high_out = gather_slots(
        pad, 1, [(h * groups + k, BLOCK_Y - 1, faces[h, 3, k]) for h in range(halves) for k in range(groups)]
    )
    low_out = gather_slots(
        pad, 1, [(h * groups + k, 0, faces[h, 2, k]) for h in range(halves) for k in range(groups)]
    )
    return high_out, low_out


def row_pick(slab_axes, axis, at, n):
    if slab_axes[0] == axis:
        return pl.ds(at * n, n)
    return pl.ds(at, n, stride=n)


def add_direction(faces, h, direction, remote, up, down, n, groups, pad):
    part = lane_part(pad, direction)
    low = [faces[h, 2 * direction, k] for k in range(groups)]
    high = [faces[h, 2 * direction + 1, k] for k in range(groups)]
    for k in range(groups):
        if direction == 0:
            first = lane_iota(pad) < STRIDE[0]
            here = turn(low[k], STRIDE[0])
            after = turn(low[k + 1], STRIDE[0]) if k + 1 < groups else remote(k, True)
            to_high = jnp.where(first, here, after)
            before = turn(high[k - 1], STRIDE[0]) if k > 0 else remote(k, False)
            to_low = jnp.where(first, before, turn(high[k], STRIDE[0]))
        else:
            last = (BLOCK_Y, BLOCK_Z)[direction - 1] - 1
            to_high = jnp.where(part == last, remote(k, True), turn(low[k], -STRIDE[direction]))
            to_low = jnp.where(part == 0, remote(k, False), turn(high[k], STRIDE[direction]))
        faces[h, 2 * direction, k] = low[k] + to_low
        faces[h, 2 * direction + 1, k] = high[k] + to_high
        up[k] = to_high
        down[k] = to_low
    mine = SLAB_AXES[direction]
    for other in range(3):
        if other == direction:
            continue
        for side in range(2):
            source = row_pick(mine, other, side * (n - 1), n)
            for k in range(groups):
                view = faces.at[h, 2 * other + side, k]
                for at, delta in ((0, down), (n - 1, up)):
                    target = row_pick(SLAB_AXES[other], direction, at, n)
                    view[target, :] = view[target, :] + delta.at[k][source, :]


def parity_split(even, high_out, low_out):
    return jnp.where(even, high_out, low_out), jnp.where(even, low_out, high_out)


def whole(*shapes):
    return [jax.ShapeDtypeStruct(s, jnp.float32) for s in shapes]


def vmem_params():
    return pltpu.CompilerParams(vmem_limit_bytes=40 * 2**20)


def place_kernel(raw, own, other, *, n):
    halves, _, groups, pad, _ = raw.shape

    def body(raw_ref, own_ref, other_ref, faces, out_even, out_odd):
        comp = lax.axis_index("comp")
        line = lax.axis_index("elem") // GRID_Y
        for h in range(halves):
            place = jnp.where(comp == h, own_ref[...], other_ref[...])
            matrix = one_hot(place)
            for s in range(6):
                x = jnp.concatenate([raw_ref[h, s, k] for k in range(groups)], axis=1)
                y = split_dot(x, matrix, ((1,), (1,)))
                for k in range(groups):
                    faces[h, s, k] = y[:, k * LANES : (k + 1) * LANES]
        high_out, low_out = payload_x(faces, groups, pad)
        even, odd = parity_split(line % 2 == 0, high_out, low_out)
        out_even[...] = even
        out_odd[...] = odd

    return pl.pallas_call(
        body,
        out_shape=whole(raw.shape, (pad, LANES), (pad, LANES)),
        compiler_params=vmem_params(),
        name="place",
    )(raw, own, other)


def parity_remote(even, got_even, got_odd):
    return jnp.where(even, got_even, got_odd), jnp.where(even, got_odd, got_even)


def x_kernel(faces_in, got_even, got_odd, *, n):
    halves, _, groups, pad, _ = faces_in.shape

    def body(faces_ref, even_ref, odd_ref, faces, out_even, out_odd, up, down):
        elem = lax.axis_index("elem")
        faces[...] = faces_ref[...]
        for_high, for_low = parity_remote(elem // GRID_Y % 2 == 0, even_ref[...], odd_ref[...])
        for h in range(halves):

            def remote(k, high):
                value = for_high if high else for_low
                return turn(value, STRIDE[0]) if (h == 0) == high else value

            add_direction(faces, h, 0, remote, up, down, n, groups, pad)
        high_out, low_out = payload_y(faces, groups, pad, halves)
        even, odd = parity_split(elem % GRID_Y % 2 == 0, high_out, low_out)
        out_even[...] = even
        out_odd[...] = odd

    return pl.pallas_call(
        body,
        out_shape=whole(faces_in.shape, (pad, LANES), (pad, LANES)),
        scratch_shapes=[pltpu.VMEM((groups, pad, LANES), jnp.float32)] * 2,
        compiler_params=vmem_params(),
        name="add_x",
    )(faces_in, got_even, got_odd)


def y_kernel(faces_in, got_even, got_odd, *, n):
    halves, _, groups, pad, _ = faces_in.shape
    last = BLOCK_Z - 1

    def body(faces_ref, even_ref, odd_ref, faces, out, up, down):
        elem = lax.axis_index("elem")
        rep = lax.axis_index("rep")
        faces[...] = faces_ref[...]
        for_high, for_low = parity_remote(elem % GRID_Y % 2 == 0, even_ref[...], odd_ref[...])
        for h in range(halves):

            def remote(k, high):
                slot = h * groups + k
                if high:
                    return turn(for_high, (BLOCK_Y - 1 - slot) * STRIDE[1])
                return turn(for_low, -slot * STRIDE[1])

            add_direction(faces, h, 1, remote, up, down, n, groups, pad)
        lower = rep == 0
        choices = (((0, 1), (0, 0)), ((1, 0), (0, 1)), ((1, 1), (1, 0)))
        outs = []
        for mine, theirs in choices:
            pair = []
            for h, side in (mine, theirs):
                pair.append((h, side))
            outs.append(pair)
        part = lane_part(pad, 2)
        for page in range(2):
            value = jnp.zeros((pad, LANES), jnp.float32)
            for index, (a, b) in enumerate(outs):
                if index // 2 != page:
                    continue
                for k in range(groups):
                    slot = index % 2 * groups + k
                    one = turn(faces[a[0], 4 + a[1], k], slot - a[1] * last)
                    two = turn(faces[b[0], 4 + b[1], k], slot - b[1] * last)
                    value = jnp.where(part == slot, jnp.where(lower, one, two), value)
            out[page] = value

    return pl.pallas_call(
        body,
        out_shape=whole(faces_in.shape, (2, pad, LANES)),
        scratch_shapes=[pltpu.VMEM((groups, pad, LANES), jnp.float32)] * 2,
        compiler_params=vmem_params(),
        name="add_y",
    )(faces_in, got_even, got_odd)


def pack_layout(n, groups):
    pad = rows_padded(n)
    mid = (n - 2) * n
    tall = (pad // 2 + 7) // 8 * 8
    sizes = [pad * groups, mid * groups, mid * groups, tall, mid // 2, mid // 2]
    starts = [sum(sizes[:i]) for i in range(6)]
    return pad, mid, tall, starts, sum(sizes)


def z_kernel(faces_in, got, *, n):
    halves, _, groups, pad, _ = faces_in.shape
    last = BLOCK_Z - 1
    _, mid, tall, starts, total = pack_layout(n, groups)

    def body(faces_ref, got_ref, keep, send, faces, up, down):
        rep = lax.axis_index("rep")
        comp = lax.axis_index("comp")
        faces[...] = faces_ref[...]
        lower = rep == 0
        arrived = {
            (0, True): (0, 1),
            (0, False): (None, 0),
            (1, True): (2, None),
            (1, False): (1, 2),
        }
        for h in range(halves):

            def remote(k, high):
                values = []
                for index in arrived[(h, high)]:
                    if index is None:
                        values.append(jnp.zeros((pad, LANES), jnp.float32))
                    else:
                        slot = index % 2 * groups + k
                        values.append(turn(got_ref[index // 2], (last if high else 0) - slot))
                return jnp.where(lower, values[0], values[1])

            add_direction(faces, h, 2, remote, up, down, n, groups, pad)
        for dst, h in ((keep, comp), (send, 1 - comp)):
            for k in range(groups):
                dst[pl.ds(starts[0] + k * pad, pad), :] = faces[h, 0, k]
                for s in (1, 2):
                    dst[pl.ds(starts[s] + k * mid, mid), :] = faces[h, 2 * s, k, n : n + mid, :]
            x = faces.at[h, 1, groups - 1]
            dst[pl.ds(starts[3], tall), :] = jnp.where(
                lane_iota(tall) < STRIDE[0], turn(x[0:tall, :], STRIDE[0]), x[pad - tall : pad, :]
            )
            for s in (1, 2):
                pieces = []
                for part in range(2):
                    for k in range(groups):
                        rows = faces[h, 2 * s + 1, k, n + part * (mid // 2) : n + (part + 1) * (mid // 2), :]
                        pieces.append((part * groups + k, (BLOCK_Y, BLOCK_Z)[s - 1] - 1, rows))
                dst[pl.ds(starts[3 + s], mid // 2), :] = gather_slots(mid // 2, s, pieces)

    return pl.pallas_call(
        body,
        out_shape=whole((total, LANES), (total, LANES)),
        scratch_shapes=[pltpu.VMEM(faces_in.shape, jnp.float32)]
        + [pltpu.VMEM((groups, pad, LANES), jnp.float32)] * 2,
        compiler_params=vmem_params(),
        name="add_z",
    )(faces_in, got)


def final_kernel(own_face, got_face, own_in, got_in, place, *, n):
    groups = place.shape[1] // LANES
    pad, mid, tall, starts, total = pack_layout(n, groups)
    inner = n - 2

    def body(of, gf, oi, gi, place_ref, out, out_s, faces, sem):
        matrix = one_hot(place_ref[...])
        faces[...] = of[...] + gf[...]

        def put(x, store):
            y = split_dot(jnp.concatenate(x, axis=1), matrix, ((1,), (0,)))
            for k in range(groups):
                store(k, y[:, k * LANES : (k + 1) * LANES])

        first = lane_iota(pad) < STRIDE[0]
        low = [faces[pl.ds(starts[0] + k * pad, pad), :] for k in range(groups)]
        edge = faces[pl.ds(starts[3], tall), :]
        edge_full = jnp.concatenate([turn(edge, STRIDE[0])[: pad - tall], edge], axis=0)
        high = []
        for k in range(groups):
            after = turn(low[k + 1], STRIDE[0]) if k + 1 < groups else edge_full
            high.append(jnp.where(first, turn(low[k], STRIDE[0]), after))
        for side, x in ((0, low), (1, high)):

            def store(k, y):
                out_s[k, side * (n - 1) * n * n : side * (n - 1) * n * n + n * n, :] = y[: n * n]

            put(x, store)
        for s in (1, 2):
            low = [faces[pl.ds(starts[s] + k * mid, mid), :] for k in range(groups)]
            edge = faces[pl.ds(starts[3 + s], mid // 2), :]
            last = (BLOCK_Y, BLOCK_Z)[s - 1] - 1
            part = lane_part(mid, s)
            high = []
            for k in range(groups):
                far = jnp.concatenate(
                    [turn(edge, (last - (p * groups + k)) * STRIDE[s]) for p in range(2)], axis=0
                )
                high.append(jnp.where(part == last, far, turn(low[k], -STRIDE[s])))
            for side, x in ((0, low), (1, high)):

                def store(k, y):
                    for a in range(inner):
                        base = (a + 1) * n * n
                        if s == 1:
                            out_s[k, base + side * (n - 1) * n : base + side * (n - 1) * n + n, :] = y[
                                a * n : a * n + n
                            ]
                        else:
                            out_s.at[k][pl.ds(base + n + side * (n - 1), inner, stride=n), :] = y[
                                a * n + 1 : a * n + 1 + inner
                            ]

                put(x, store)
        for a in range(inner):
            for b in range(inner):
                for k in range(groups):
                    src = pl.ds(((a * inner + b) * groups + k) * inner, inner)
                    base = (a + 1) * n * n + (b + 1) * n + 1
                    out_s[k, base : base + inner, :] = oi[src, :] + gi[src, :]
        done = [
            pltpu.make_async_copy(out_s.at[k], out.at[:, 0, pl.ds(k * LANES, LANES)], sem.at[k])
            for k in range(groups)
        ]
        for c in done:
            c.start()
        for c in done:
            c.wait()

    return pl.pallas_call(
        body,
        out_shape=jax.ShapeDtypeStruct((n * n * n, 1, groups * LANES), jnp.float32),
        out_specs=pl.BlockSpec(memory_space=pltpu.HBM),
        scratch_shapes=[
            pltpu.VMEM((groups, n * n * n, LANES), jnp.float32),
            pltpu.VMEM((total, LANES), jnp.float32),
            pltpu.SemaphoreType.DMA((groups,)),
        ],
        compiler_params=vmem_params(),
        name="final",
    )(own_face, got_face, own_in, got_in, place)


def swap_pairs(count, position, extent, step, odd):
    pairs = []
    for e in range(count):
        at = position(e)
        up = at % 2 == (1 if odd else 0)
        if 0 <= at + (1 if up else -1) < extent:
            pairs.append((e, e + (step if up else -step)))
    return pairs


def exchange(even, odd, count, position, extent, step):
    got_even = lax.ppermute(even, "elem", swap_pairs(count, position, extent, step, False))
    pairs = swap_pairs(count, position, extent, step, True)
    got_odd = lax.ppermute(odd, "elem", pairs) if pairs else jnp.zeros_like(odd)
    return got_even, got_odd


def body(velocity, geometry, element_place):
    n = velocity.shape[1] * lax.axis_size("comp")
    swap = [(0, 1), (1, 0)]
    count = lax.axis_size("elem")
    other_place = lax.ppermute(element_place, "comp", swap)
    own_in, send_in, raw = flux_kernel(velocity, geometry, node_count=n)
    got_in = lax.ppermute(send_in, "comp", swap)
    faces, even, odd = place_kernel(raw, element_place, other_place, n=n)
    even, odd = exchange(even, odd, count, lambda e: e // GRID_Y, count // GRID_Y, GRID_Y)
    faces, even, odd = x_kernel(faces, even, odd, n=n)
    even, odd = exchange(even, odd, count, lambda e: e % GRID_Y, GRID_Y, 1)
    faces, out = y_kernel(faces, even, odd, n=n)
    got = lax.ppermute(out, "rep", swap)
    own_face, send_face = z_kernel(faces, got, n=n)
    got_face = lax.ppermute(send_face, "comp", swap)
    result = final_kernel(own_face, got_face, own_in, got_in, element_place, n=n)
    return result.reshape(n, n, n, 1, element_place.shape[1])


def solution(mesh):
    placed = (
        P(None, "comp", None, None, None, ("elem", "rep")),
        P(None, None, "comp", None, None, None, ("elem", "rep")),
        P("comp", ("elem", "rep")),
    )

    def run(velocity, geometry, element_place):
        with jax.sharding.use_abstract_mesh(mesh.abstract_mesh):
            return jax.shard_map(
                body,
                mesh=mesh,
                in_specs=placed,
                out_specs=P(None, None, None, "comp", ("elem", "rep")),
                check_vma=False,
            )(velocity, geometry, element_place)

    return run
```

```python
import jax
import jax.numpy as jnp
import numpy as np
from jax import lax
from jax.experimental import pallas as pl
from jax.experimental.pallas import tpu as pltpu
from jax.sharding import PartitionSpec as P


BLOCK_Y = 8
BLOCK_Z = 8
GRID_Y = 4
LANES = 128

SLAB_AXES = ((1, 2), (0, 2), (0, 1))


def legendre_columns(points, degree):
    columns = [points * 0.0 + 1.0, points]
    for order in range(2, degree + 1):
        columns.append(
            ((2 * order - 1) * points * columns[order - 1] - (order - 1) * columns[order - 2])
            / order
        )
    return columns


def derivative_table(node_count):
    degree = node_count - 1
    points = np.cos(np.pi * np.arange(node_count) / degree)
    for _ in range(100):
        columns = legendre_columns(points, degree)
        points = points - (points * columns[degree] - columns[degree - 1]) / (
            node_count * columns[degree]
        )
    points = np.sort(points)
    values = legendre_columns(points, degree)[degree]
    identity = np.eye(node_count)
    spacing = points[:, None] - points[None, :] + identity
    matrix = values[:, None] / (values[None, :] * spacing)
    matrix = np.where(identity > 0.5, 0.0, matrix)
    matrix[0, 0] = -degree * (degree + 1) / 4.0
    matrix[degree, degree] = degree * (degree + 1) / 4.0
    return matrix


def weighted(terms):
    total = None
    for value, factor in terms:
        total = value * factor if total is None else total + value * factor
    return total


def transpose_line(line, table):
    count = len(line)
    half = count // 2
    even = [line[i] + line[count - 1 - i] for i in range(half)]
    odd = [line[i] - line[count - 1 - i] for i in range(half)]
    out = [None] * count
    for m in range(half):
        w = count - 1 - m
        both = weighted([(odd[i], float(0.5 * (table[i, m] + table[i, w]))) for i in range(half)])
        diff = weighted([(even[i], float(0.5 * (table[i, m] - table[i, w]))) for i in range(half)])
        out[m] = both + diff
        out[w] = both - diff
    return out


def rows_padded(node_count):
    return (node_count * node_count + 7) // 8 * 8


def flux_kernel(velocity, geometry, *, node_count):
    n = node_count
    planes = velocity.shape[1]
    groups = velocity.shape[5] // LANES
    halves = velocity.shape[4]
    table = derivative_table(n)
    inner = n - 2
    early = planes // 2 + 1

    def body(v_hbm, g_hbm, send, part, v, g, f0, f1, st, sem):
        comp = lax.axis_index("comp")
        first = comp == 0

        def copies(plane):
            out = []
            for k in range(groups):
                lanes = pl.ds(k * LANES, LANES)
                subs = pl.ds(k * halves, halves)
                out.append(
                    pltpu.make_async_copy(
                        v_hbm.at[:, plane, :, :, :, lanes], v.at[plane, :, :, :, subs, :], sem.at[2 * k, plane]
                    )
                )
                out.append(
                    pltpu.make_async_copy(
                        g_hbm.at[:, :, plane, :, :, :, lanes],
                        g.at[plane, :, :, :, :, subs, :],
                        sem.at[2 * k + 1, plane],
                    )
                )
            return out

        for plane in range(planes):
            for c in copies(plane):
                c.start()

        coef = [
            [jnp.where(first, float(table[i, m]), float(table[planes + i, m])) for m in range(n)]
            for i in range(planes)
        ]
        low = jnp.where(first, 1.0, 0.0)
        own = (low, 1.0 - low)

        def row_of(m, b, c):
            return pl.ds(pl.multiple_of((m * n * n + b * n + c) * 8, 8), 8)

        for plane in range(planes):
            for c in copies(plane):
                c.wait()

            def along_last(b, carry):
                line = []
                for c in range(n):
                    vel = [v[plane, i, b, c] for i in range(3)]
                    flux = [
                        weighted([(g[plane, i, j, b, c], vel[i]) for i in range(3)]) for j in range(3)
                    ]
                    f0[plane, b, c] = flux[0]
                    f1[b, c] = flux[1]
                    line.append(flux[2])
                out = transpose_line(line, table)
                for c in range(n):
                    st[plane, b, c] = out[c]
                return carry

            lax.fori_loop(0, n, along_last, 0)

            def along_mid(c, carry):
                out = transpose_line([f1[b, c] for b in range(n)], table)
                for b in range(n):
                    st[plane, b, c] = st[plane, b, c] + out[b]
                return carry

            lax.fori_loop(0, n, along_mid, 0)
            if plane == early - 1:

                def begin_first(b, carry):
                    for c in range(n):
                        line = [f0[i, b, c] for i in range(early)]
                        for m in range(n):
                            part[row_of(m, b, c), :] = weighted([(line[i], coef[i][m]) for i in range(early)])
                    return carry

                lax.fori_loop(0, n, begin_first, 0)

        def end_first(b, carry):
            for c in range(n):
                line = [f0[i, b, c] for i in range(early, planes)]
                for m in range(n):
                    row = row_of(m, b, c)
                    rest = weighted([(line[i], coef[early + i][m]) for i in range(planes - early)])
                    part[row, :] = part[row, :] + rest + st[m % planes, b, c] * own[m // planes]
            return carry

        lax.fori_loop(0, n, end_first, 0)
        for a in range(inner):
            for b in range(inner):
                for k in range(groups):
                    base = ((a + 1) * n * n + (b + 1) * n + 1) * 8 + k * halves
                    send[pl.ds(((a * inner + b) * groups + k) * inner, inner), :] = part[
                        pl.ds(base + 1 - comp, inner, stride=8), :
                    ]

    tile = (8, LANES)
    return pl.pallas_call(
        body,
        in_specs=[pl.BlockSpec(memory_space=pltpu.HBM), pl.BlockSpec(memory_space=pltpu.HBM)],
        out_shape=whole((inner * inner * inner * groups, LANES), (n * n * n * 8, LANES)),
        scratch_shapes=[
            pltpu.VMEM((planes, 3, n, n) + tile, jnp.float32),
            pltpu.VMEM((planes, 3, 3, n, n) + tile, jnp.float32),
            pltpu.VMEM((planes, n, n) + tile, jnp.float32),
            pltpu.VMEM((n, n) + tile, jnp.float32),
            pltpu.VMEM((planes, n, n) + tile, jnp.float32),
            pltpu.SemaphoreType.DMA((2 * groups, planes)),
        ],
        compiler_params=pltpu.CompilerParams(vmem_limit_bytes=42 * 2**20),
        name="flux",
    )(velocity, geometry)


def keep_kernel(part, *, n, groups, halves):
    inner = n - 2

    def body(part, keep):
        comp = lax.axis_index("comp")
        for a in range(inner):
            for b in range(inner):
                for k in range(groups):
                    base = ((a + 1) * n * n + (b + 1) * n + 1) * 8 + k * halves
                    keep[pl.ds(((a * inner + b) * groups + k) * inner, inner), :] = part[
                        pl.ds(base + comp, inner, stride=8), :
                    ]

    return pl.pallas_call(
        body,
        out_shape=whole((inner * inner * inner * groups, LANES))[0],
        compiler_params=vmem_params(),
        name="keep",
    )(part)


def lane_iota(rows):
    return lax.broadcasted_iota(jnp.int32, (rows, LANES), 1)


def lane_part(rows, direction):
    lane = lane_iota(rows)
    if direction == 0:
        return lane // (BLOCK_Y * BLOCK_Z)
    if direction == 1:
        return lane // BLOCK_Z % BLOCK_Y
    return lane % BLOCK_Z


STRIDE = (BLOCK_Y * BLOCK_Z, BLOCK_Z, 1)


def turn(x, by):
    by = by % LANES
    return x if by == 0 else pltpu.roll(x, by, 1)


def split_dot(x, matrix, dims):
    high = x.astype(jnp.bfloat16)
    low = (x - high.astype(jnp.float32)).astype(jnp.bfloat16)
    both = jnp.concatenate([high, low], axis=1)
    return lax.dot_general(both, matrix, (dims, ((), ())), preferred_element_type=jnp.float32)


def one_hot(place):
    size = place.shape[1]
    target = lax.broadcasted_iota(jnp.int32, (size, size), 0)
    return jnp.where(target == place, 1.0, 0.0).astype(jnp.bfloat16)


def payload_x(faces, groups, pad):
    lane = lane_iota(pad)
    low = lane < STRIDE[0]
    high_out = jnp.where(low, turn(faces[0, 1, groups - 1], STRIDE[0]), faces[1, 1, groups - 1])
    low_out = jnp.where(low, faces[0, 0, 0], turn(faces[1, 0, 0], STRIDE[0]))
    return high_out, low_out


def gather_slots(pad, direction, pieces):
    part = lane_part(pad, direction)
    out = jnp.zeros((pad, LANES), jnp.float32)
    for slot, source, value in pieces:
        out = jnp.where(part == slot, turn(value, (slot - source) * STRIDE[direction]), out)
    return out


def payload_y(faces, groups, pad, halves):
    high_out = gather_slots(
        pad, 1, [(h * groups + k, BLOCK_Y - 1, faces[h, 3, k]) for h in range(halves) for k in range(groups)]
    )
    low_out = gather_slots(
        pad, 1, [(h * groups + k, 0, faces[h, 2, k]) for h in range(halves) for k in range(groups)]
    )
    return high_out, low_out


def row_pick(slab_axes, axis, at, n):
    if slab_axes[0] == axis:
        return pl.ds(at * n, n)
    return pl.ds(at, n, stride=n)


def add_direction(faces, h, direction, remote, up, down, n, groups, pad):
    part = lane_part(pad, direction)
    low = [faces[h, 2 * direction, k] for k in range(groups)]
    high = [faces[h, 2 * direction + 1, k] for k in range(groups)]
    for k in range(groups):
        if direction == 0:
            first = lane_iota(pad) < STRIDE[0]
            here = turn(low[k], STRIDE[0])
            after = turn(low[k + 1], STRIDE[0]) if k + 1 < groups else remote(k, True)
            to_high = jnp.where(first, here, after)
            before = turn(high[k - 1], STRIDE[0]) if k > 0 else remote(k, False)
            to_low = jnp.where(first, before, turn(high[k], STRIDE[0]))
        else:
            last = (BLOCK_Y, BLOCK_Z)[direction - 1] - 1
            to_high = jnp.where(part == last, remote(k, True), turn(low[k], -STRIDE[direction]))
            to_low = jnp.where(part == 0, remote(k, False), turn(high[k], STRIDE[direction]))
        faces[h, 2 * direction, k] = low[k] + to_low
        faces[h, 2 * direction + 1, k] = high[k] + to_high
        up[k] = to_high
        down[k] = to_low
    mine = SLAB_AXES[direction]
    for other in range(3):
        if other == direction:
            continue
        for side in range(2):
            source = row_pick(mine, other, side * (n - 1), n)
            for k in range(groups):
                view = faces.at[h, 2 * other + side, k]
                for at, delta in ((0, down), (n - 1, up)):
                    target = row_pick(SLAB_AXES[other], direction, at, n)
                    view[target, :] = view[target, :] + delta.at[k][source, :]


def parity_split(even, high_out, low_out):
    return jnp.where(even, high_out, low_out), jnp.where(even, low_out, high_out)


def whole(*shapes):
    return [jax.ShapeDtypeStruct(s, jnp.float32) for s in shapes]


def vmem_params():
    return pltpu.CompilerParams(vmem_limit_bytes=40 * 2**20)


def place_kernel(part, own, other, *, n):
    groups = own.shape[1] // LANES
    halves = 2
    pad = rows_padded(n)
    shape = (halves, 6, groups, pad, LANES)

    def body(part_ref, own_ref, other_ref, faces, out_even, out_odd, line_rows):
        comp = lax.axis_index("comp")
        line = lax.axis_index("elem") // GRID_Y
        for h in range(halves):
            place = jnp.where(comp == h, own_ref[...], other_ref[...])
            matrix = one_hot(place)
            matrix = jnp.concatenate([matrix, matrix], axis=1)
            for s in range(6):
                at = s % 2 * (n - 1)
                for k in range(groups):
                    sub = k * halves + h
                    if s // 2 == 0:
                        line_rows[s, k, 0 : n * n, :] = part_ref[pl.ds(at * n * n * 8 + sub, n * n, stride=8), :]
                    elif s // 2 == 2:
                        line_rows[s, k, 0 : n * n, :] = part_ref[pl.ds(at * 8 + sub, n * n, stride=8 * n), :]
                    else:
                        for a in range(n):
                            line_rows[s, k, a * n : a * n + n, :] = part_ref[
                                pl.ds((a * n * n + at * n) * 8 + sub, n, stride=8), :
                            ]
                x = jnp.concatenate([line_rows[s, k] for k in range(groups)], axis=1)
                y = split_dot(x, matrix, ((1,), (1,)))
                for k in range(groups):
                    faces[h, s, k] = y[:, k * LANES : (k + 1) * LANES]
        high_out, low_out = payload_x(faces, groups, pad)
        even, odd = parity_split(line % 2 == 0, high_out, low_out)
        out_even[...] = even
        out_odd[...] = odd

    return pl.pallas_call(
        body,
        out_shape=whole(shape, (pad, LANES), (pad, LANES)),
        scratch_shapes=[pltpu.VMEM(shape[1:], jnp.float32)],
        compiler_params=vmem_params(),
        name="place",
    )(part, own, other)


def parity_remote(even, got_even, got_odd):
    return jnp.where(even, got_even, got_odd), jnp.where(even, got_odd, got_even)


def x_kernel(faces_in, got_even, got_odd, *, n):
    halves, _, groups, pad, _ = faces_in.shape

    def body(faces_ref, even_ref, odd_ref, faces, out_even, out_odd, up, down):
        elem = lax.axis_index("elem")
        faces[...] = faces_ref[...]
        for_high, for_low = parity_remote(elem // GRID_Y % 2 == 0, even_ref[...], odd_ref[...])
        for h in range(halves):

            def remote(k, high):
                value = for_high if high else for_low
                return turn(value, STRIDE[0]) if (h == 0) == high else value

            add_direction(faces, h, 0, remote, up, down, n, groups, pad)
        high_out, low_out = payload_y(faces, groups, pad, halves)
        even, odd = parity_split(elem % GRID_Y % 2 == 0, high_out, low_out)
        out_even[...] = even
        out_odd[...] = odd

    return pl.pallas_call(
        body,
        out_shape=whole(faces_in.shape, (pad, LANES), (pad, LANES)),
        scratch_shapes=[pltpu.VMEM((groups, pad, LANES), jnp.float32)] * 2,
        compiler_params=vmem_params(),
        name="add_x",
    )(faces_in, got_even, got_odd)


def y_kernel(faces_in, got_even, got_odd, *, n):
    halves, _, groups, pad, _ = faces_in.shape
    last = BLOCK_Z - 1

    def body(faces_ref, even_ref, odd_ref, faces, out, up, down):
        elem = lax.axis_index("elem")
        rep = lax.axis_index("rep")
        faces[...] = faces_ref[...]
        for_high, for_low = parity_remote(elem % GRID_Y % 2 == 0, even_ref[...], odd_ref[...])
        for h in range(halves):

            def remote(k, high):
                slot = h * groups + k
                if high:
                    return turn(for_high, (BLOCK_Y - 1 - slot) * STRIDE[1])
                return turn(for_low, -slot * STRIDE[1])

            add_direction(faces, h, 1, remote, up, down, n, groups, pad)
        lower = rep == 0
        choices = (((0, 1), (0, 0)), ((1, 0), (0, 1)), ((1, 1), (1, 0)))
        outs = []
        for mine, theirs in choices:
            pair = []
            for h, side in (mine, theirs):
                pair.append((h, side))
            outs.append(pair)
        part = lane_part(pad, 2)
        for page in range(2):
            value = jnp.zeros((pad, LANES), jnp.float32)
            for index, (a, b) in enumerate(outs):
                if index // 2 != page:
                    continue
                for k in range(groups):
                    slot = index % 2 * groups + k
                    one = turn(faces[a[0], 4 + a[1], k], slot - a[1] * last)
                    two = turn(faces[b[0], 4 + b[1], k], slot - b[1] * last)
                    value = jnp.where(part == slot, jnp.where(lower, one, two), value)
            out[page] = value

    return pl.pallas_call(
        body,
        out_shape=whole(faces_in.shape, (2, pad, LANES)),
        scratch_shapes=[pltpu.VMEM((groups, pad, LANES), jnp.float32)] * 2,
        compiler_params=vmem_params(),
        name="add_y",
    )(faces_in, got_even, got_odd)


def pack_layout(n, groups):
    pad = rows_padded(n)
    mid = (n - 2) * n
    tall = (pad // 2 + 7) // 8 * 8
    sizes = [pad * groups, mid * groups, mid * groups, tall, mid // 2, mid // 2]
    starts = [sum(sizes[:i]) for i in range(6)]
    return pad, mid, tall, starts, sum(sizes)


def z_kernel(faces_in, got, *, n):
    halves, _, groups, pad, _ = faces_in.shape
    last = BLOCK_Z - 1
    _, mid, tall, starts, total = pack_layout(n, groups)

    def body(faces_ref, got_ref, keep, send, faces, up, down):
        rep = lax.axis_index("rep")
        comp = lax.axis_index("comp")
        faces[...] = faces_ref[...]
        lower = rep == 0
        arrived = {
            (0, True): (0, 1),
            (0, False): (None, 0),
            (1, True): (2, None),
            (1, False): (1, 2),
        }
        for h in range(halves):

            def remote(k, high):
                values = []
                for index in arrived[(h, high)]:
                    if index is None:
                        values.append(jnp.zeros((pad, LANES), jnp.float32))
                    else:
                        slot = index % 2 * groups + k
                        values.append(turn(got_ref[index // 2], (last if high else 0) - slot))
                return jnp.where(lower, values[0], values[1])

            add_direction(faces, h, 2, remote, up, down, n, groups, pad)
        for dst, h in ((keep, comp), (send, 1 - comp)):
            for k in range(groups):
                dst[pl.ds(starts[0] + k * pad, pad), :] = faces[h, 0, k]
                for s in (1, 2):
                    dst[pl.ds(starts[s] + k * mid, mid), :] = faces[h, 2 * s, k, n : n + mid, :]
            x = faces.at[h, 1, groups - 1]
            dst[pl.ds(starts[3], tall), :] = jnp.where(
                lane_iota(tall) < STRIDE[0], turn(x[0:tall, :], STRIDE[0]), x[pad - tall : pad, :]
            )
            for s in (1, 2):
                pieces = []
                for part in range(2):
                    for k in range(groups):
                        rows = faces[h, 2 * s + 1, k, n + part * (mid // 2) : n + (part + 1) * (mid // 2), :]
                        pieces.append((part * groups + k, (BLOCK_Y, BLOCK_Z)[s - 1] - 1, rows))
                dst[pl.ds(starts[3 + s], mid // 2), :] = gather_slots(mid // 2, s, pieces)

    return pl.pallas_call(
        body,
        out_shape=whole((total, LANES), (total, LANES)),
        scratch_shapes=[pltpu.VMEM(faces_in.shape, jnp.float32)]
        + [pltpu.VMEM((groups, pad, LANES), jnp.float32)] * 2,
        compiler_params=vmem_params(),
        name="add_z",
    )(faces_in, got)


def final_kernel(own_face, got_face, own_in, got_in, place, *, n):
    groups = place.shape[1] // LANES
    pad, mid, tall, starts, total = pack_layout(n, groups)
    inner = n - 2

    def body(of, gf, oi, gi, place_ref, out, out_s, faces, sem):
        matrix = one_hot(place_ref[...])
        matrix = jnp.concatenate([matrix, matrix], axis=0)
        faces[...] = of[...] + gf[...]

        def put(x, store):
            y = split_dot(jnp.concatenate(x, axis=1), matrix, ((1,), (0,)))
            for k in range(groups):
                store(k, y[:, k * LANES : (k + 1) * LANES])

        first = lane_iota(pad) < STRIDE[0]
        low = [faces[pl.ds(starts[0] + k * pad, pad), :] for k in range(groups)]
        edge = faces[pl.ds(starts[3], tall), :]
        edge_full = jnp.concatenate([turn(edge, STRIDE[0])[: pad - tall], edge], axis=0)
        high = []
        for k in range(groups):
            after = turn(low[k + 1], STRIDE[0]) if k + 1 < groups else edge_full
            high.append(jnp.where(first, turn(low[k], STRIDE[0]), after))
        for side, x in ((0, low), (1, high)):

            def store(k, y):
                out_s[k, side * (n - 1) * n * n : side * (n - 1) * n * n + n * n, :] = y[: n * n]

            put(x, store)
        for s in (1, 2):
            low = [faces[pl.ds(starts[s] + k * mid, mid), :] for k in range(groups)]
            edge = faces[pl.ds(starts[3 + s], mid // 2), :]
            last = (BLOCK_Y, BLOCK_Z)[s - 1] - 1
            part = lane_part(mid, s)
            high = []
            for k in range(groups):
                far = jnp.concatenate(
                    [turn(edge, (last - (p * groups + k)) * STRIDE[s]) for p in range(2)], axis=0
                )
                high.append(jnp.where(part == last, far, turn(low[k], -STRIDE[s])))
            for side, x in ((0, low), (1, high)):

                def store(k, y):
                    for a in range(inner):
                        base = (a + 1) * n * n
                        if s == 1:
                            out_s[k, base + side * (n - 1) * n : base + side * (n - 1) * n + n, :] = y[
                                a * n : a * n + n
                            ]
                        else:
                            out_s.at[k][pl.ds(base + n + side * (n - 1), inner, stride=n), :] = y[
                                a * n + 1 : a * n + 1 + inner
                            ]

                put(x, store)
        for a in range(inner):
            for b in range(inner):
                for k in range(groups):
                    src = pl.ds(((a * inner + b) * groups + k) * inner, inner)
                    base = (a + 1) * n * n + (b + 1) * n + 1
                    out_s[k, base : base + inner, :] = oi[src, :] + gi[src, :]
        done = [
            pltpu.make_async_copy(out_s.at[k], out.at[:, 0, pl.ds(k * LANES, LANES)], sem.at[k])
            for k in range(groups)
        ]
        for c in done:
            c.start()
        for c in done:
            c.wait()

    return pl.pallas_call(
        body,
        out_shape=jax.ShapeDtypeStruct((n * n * n, 1, groups * LANES), jnp.float32),
        out_specs=pl.BlockSpec(memory_space=pltpu.HBM),
        scratch_shapes=[
            pltpu.VMEM((groups, n * n * n, LANES), jnp.float32),
            pltpu.VMEM((total, LANES), jnp.float32),
            pltpu.SemaphoreType.DMA((groups,)),
        ],
        compiler_params=vmem_params(),
        name="final",
    )(own_face, got_face, own_in, got_in, place)


def swap_pairs(count, position, extent, step, odd):
    pairs = []
    for e in range(count):
        at = position(e)
        up = at % 2 == (1 if odd else 0)
        if 0 <= at + (1 if up else -1) < extent:
            pairs.append((e, e + (step if up else -step)))
    return pairs


def exchange(even, odd, count, position, extent, step):
    got_even = lax.ppermute(even, "elem", swap_pairs(count, position, extent, step, False))
    pairs = swap_pairs(count, position, extent, step, True)
    got_odd = lax.ppermute(odd, "elem", pairs) if pairs else jnp.zeros_like(odd)
    return got_even, got_odd


def body(velocity, geometry, element_place):
    n = velocity.shape[1] * lax.axis_size("comp")
    swap = [(0, 1), (1, 0)]
    count = lax.axis_size("elem")
    other_place = lax.ppermute(element_place, "comp", swap)
    velocity = pltpu.with_memory_space_constraint(velocity, pltpu.HBM)
    geometry = pltpu.with_memory_space_constraint(geometry, pltpu.HBM)
    send_in, part = flux_kernel(velocity, geometry, node_count=n)
    got_in = lax.ppermute(send_in, "comp", swap)
    faces, even, odd = place_kernel(part, element_place, other_place, n=n)
    own_in = keep_kernel(part, n=n, groups=element_place.shape[1] // LANES, halves=velocity.shape[4])
    even, odd = exchange(even, odd, count, lambda e: e // GRID_Y, count // GRID_Y, GRID_Y)
    faces, even, odd = x_kernel(faces, even, odd, n=n)
    even, odd = exchange(even, odd, count, lambda e: e % GRID_Y, GRID_Y, 1)
    faces, out = y_kernel(faces, even, odd, n=n)
    got = lax.ppermute(out, "rep", swap)
    own_face, send_face = z_kernel(faces, got, n=n)
    got_face = lax.ppermute(send_face, "comp", swap)
    result = final_kernel(own_face, got_face, own_in, got_in, element_place, n=n)
    return result.reshape(n, n, n, 1, element_place.shape[1])


def solution(mesh):
    placed = (
        P(None, "comp", None, None, None, ("elem", "rep")),
        P(None, None, "comp", None, None, None, ("elem", "rep")),
        P("comp", ("elem", "rep")),
    )

    step = jax.shard_map(
        body,
        mesh=mesh,
        in_specs=placed,
        out_specs=P(None, None, None, "comp", ("elem", "rep")),
        check_vma=False,
    )

    def run(velocity, geometry, element_place):
        with jax.sharding.use_abstract_mesh(mesh.abstract_mesh):
            return step(velocity, geometry, element_place)

    return run
```

```python
import jax
import jax.numpy as jnp
import numpy as np
from jax import lax
from jax.experimental import pallas as pl
from jax.experimental.pallas import tpu as pltpu
from jax.sharding import PartitionSpec as P


BLOCK_Y = 8
BLOCK_Z = 8
GRID_Y = 4
LANES = 128

SLAB_AXES = ((1, 2), (0, 2), (0, 1))


def legendre_columns(points, degree):
    columns = [points * 0.0 + 1.0, points]
    for order in range(2, degree + 1):
        columns.append(
            ((2 * order - 1) * points * columns[order - 1] - (order - 1) * columns[order - 2])
            / order
        )
    return columns


def derivative_table(node_count):
    degree = node_count - 1
    points = np.cos(np.pi * np.arange(node_count) / degree)
    for _ in range(100):
        columns = legendre_columns(points, degree)
        points = points - (points * columns[degree] - columns[degree - 1]) / (
            node_count * columns[degree]
        )
    points = np.sort(points)
    values = legendre_columns(points, degree)[degree]
    identity = np.eye(node_count)
    spacing = points[:, None] - points[None, :] + identity
    matrix = values[:, None] / (values[None, :] * spacing)
    matrix = np.where(identity > 0.5, 0.0, matrix)
    matrix[0, 0] = -degree * (degree + 1) / 4.0
    matrix[degree, degree] = degree * (degree + 1) / 4.0
    return matrix


def weighted(terms):
    total = None
    for value, factor in terms:
        total = value * factor if total is None else total + value * factor
    return total


def transpose_line(line, table):
    count = len(line)
    half = count // 2
    even = [line[i] + line[count - 1 - i] for i in range(half)]
    odd = [line[i] - line[count - 1 - i] for i in range(half)]
    out = [None] * count
    for m in range(half):
        w = count - 1 - m
        both = weighted([(odd[i], float(0.5 * (table[i, m] + table[i, w]))) for i in range(half)])
        diff = weighted([(even[i], float(0.5 * (table[i, m] - table[i, w]))) for i in range(half)])
        out[m] = both + diff
        out[w] = both - diff
    return out


def rows_padded(node_count):
    return (node_count * node_count + 7) // 8 * 8


def plane_at(plane, comp, n):
    return jnp.where(comp == 0, plane, (plane + n // 2) % n) * (n * n * 8)


def flux_kernel(velocity, geometry, *, node_count):
    n = node_count
    planes = velocity.shape[1]
    groups = velocity.shape[5] // LANES
    halves = velocity.shape[4]
    table = derivative_table(n)
    inner = n - 2
    blocks = [(plane, 0, n) for plane in range(planes - 1)]
    blocks += [(planes - 1, 0, n // 2), (planes - 1, n // 2, n - n // 2)]

    def body(v_hbm, g_hbm, send, part, v, g, f0, f1, st, sem):
        comp = lax.axis_index("comp")
        first = comp == 0

        def copies(index):
            plane, start, count = blocks[index]
            rows = pl.ds(start, count)
            out = []
            for k in range(groups):
                lanes = pl.ds(k * LANES, LANES)
                subs = pl.ds(k * halves, halves)
                out.append(
                    pltpu.make_async_copy(
                        v_hbm.at[:, plane, rows, :, :, lanes], v.at[plane, :, rows, :, subs, :], sem.at[2 * k, index]
                    )
                )
                out.append(
                    pltpu.make_async_copy(
                        g_hbm.at[:, :, plane, rows, :, :, lanes],
                        g.at[plane, :, :, rows, :, subs, :],
                        sem.at[2 * k + 1, index],
                    )
                )
            return out

        for index in range(len(blocks)):
            for c in copies(index):
                c.start()

        def row_of(m, b, c):
            return pl.ds(pl.multiple_of((m * n * n + b * n + c) * 8, 8), 8)

        for index, (plane, start, count) in enumerate(blocks):
            for c in copies(index):
                c.wait()

            def along_last(b, carry):
                line = []
                for c in range(n):
                    vel = [v[plane, i, b, c] for i in range(3)]
                    flux = [
                        weighted([(g[plane, i, j, b, c], vel[i]) for i in range(3)]) for j in range(3)
                    ]
                    f0[b, c] = flux[0]
                    f1[b, c] = flux[1]
                    line.append(flux[2])
                out = transpose_line(line, table)
                for c in range(n):
                    st[b, c] = out[c]
                return carry

            lax.fori_loop(start, start + count, along_last, 0)
            if start + count < n:
                continue
            coef = [
                jnp.where(first, float(table[plane, m]), float(table[planes + plane, (m + planes) % n]))
                for m in range(n)
            ]

            def along_others(c, carry):
                out = transpose_line([f1[b, c] for b in range(n)], table)
                for b in range(n):
                    flux = f0[b, c]
                    for m in range(n):
                        value = flux * coef[m]
                        if m == plane:
                            value = value + (st[b, c] + out[b])
                        row = row_of(m, b, c)
                        part[row, :] = value if plane == 0 else part[row, :] + value
                return carry

            lax.fori_loop(0, n, along_others, 0)
        for a in range(inner):
            for b in range(inner):
                for k in range(groups):
                    base = plane_at(a + 1, comp, n) + ((b + 1) * n + 1) * 8 + k * halves
                    send[pl.ds(((a * inner + b) * groups + k) * inner, inner), :] = part[
                        pl.ds(base + 1 - comp, inner, stride=8), :
                    ]

    tile = (8, LANES)
    return pl.pallas_call(
        body,
        in_specs=[pl.BlockSpec(memory_space=pltpu.HBM), pl.BlockSpec(memory_space=pltpu.HBM)],
        out_shape=whole((inner * inner * inner * groups, LANES), (n * n * n * 8, LANES)),
        scratch_shapes=[
            pltpu.VMEM((planes, 3, n, n) + tile, jnp.float32),
            pltpu.VMEM((planes, 3, 3, n, n) + tile, jnp.float32),
            pltpu.VMEM((n, n) + tile, jnp.float32),
            pltpu.VMEM((n, n) + tile, jnp.float32),
            pltpu.VMEM((n, n) + tile, jnp.float32),
            pltpu.SemaphoreType.DMA((2 * groups, planes + 1)),
        ],
        compiler_params=pltpu.CompilerParams(vmem_limit_bytes=42 * 2**20),
        name="flux",
    )(velocity, geometry)


def lane_iota(rows):
    return lax.broadcasted_iota(jnp.int32, (rows, LANES), 1)


def lane_part(rows, direction):
    lane = lane_iota(rows)
    if direction == 0:
        return lane // (BLOCK_Y * BLOCK_Z)
    if direction == 1:
        return lane // BLOCK_Z % BLOCK_Y
    return lane % BLOCK_Z


STRIDE = (BLOCK_Y * BLOCK_Z, BLOCK_Z, 1)


def turn(x, by):
    by = by % LANES
    return x if by == 0 else pltpu.roll(x, by, 1)


def split_dot(x, matrix, dims):
    both = jnp.concatenate(bf16_pair(x), axis=1)
    return lax.dot_general(both, matrix, (dims, ((), ())), preferred_element_type=jnp.float32)


def one_hot(place):
    size = place.shape[1]
    target = lax.broadcasted_iota(jnp.int32, (size, size), 0)
    return jnp.where(target == place, 1.0, 0.0).astype(jnp.bfloat16)


def gather_slots(pad, direction, pieces):
    part = lane_part(pad, direction)
    out = jnp.zeros((pad, LANES), jnp.float32)
    for slot, source, value in pieces:
        out = jnp.where(part == slot, turn(value, (slot - source) * STRIDE[direction]), out)
    return out


def payload_y(faces, groups, pad, halves):
    high_out = gather_slots(
        pad, 1, [(h * groups + k, BLOCK_Y - 1, faces[h, 3, k]) for h in range(halves) for k in range(groups)]
    )
    low_out = gather_slots(
        pad, 1, [(h * groups + k, 0, faces[h, 2, k]) for h in range(halves) for k in range(groups)]
    )
    return high_out, low_out


def row_pick(slab_axes, axis, at, n):
    if slab_axes[0] == axis:
        return pl.ds(at * n, n)
    return pl.ds(at, n, stride=n)


def add_rows(faces, h, direction, up, down, n, picks):
    mine = SLAB_AXES[direction]
    for other in range(3):
        if other == direction:
            continue
        for side in range(2):
            source = row_pick(mine, other, side * (n - 1), n)
            for k, high in picks:
                view = faces.at[h, 2 * other + side, k]
                target = row_pick(SLAB_AXES[other], direction, (n - 1) if high else 0, n)
                delta = up if high else down
                view[target, :] = view[target, :] + delta.at[k][source, :]


def both_picks(groups):
    return [(k, high) for k in range(groups) for high in (False, True)]


def add_direction(faces, h, direction, remote, up, down, n, groups, pad):
    part = lane_part(pad, direction)
    low = [faces[h, 2 * direction, k] for k in range(groups)]
    high = [faces[h, 2 * direction + 1, k] for k in range(groups)]
    zero = jnp.zeros((pad, LANES), jnp.float32)
    for k in range(groups):
        if direction == 0:
            first = lane_iota(pad) < STRIDE[0]
            here = turn(low[k], STRIDE[0])
            after = turn(low[k + 1], STRIDE[0]) if k + 1 < groups else zero
            to_high = jnp.where(first, here, after)
            before = turn(high[k - 1], STRIDE[0]) if k > 0 else zero
            to_low = jnp.where(first, before, turn(high[k], STRIDE[0]))
        else:
            last = (BLOCK_Y, BLOCK_Z)[direction - 1] - 1
            to_high = jnp.where(part == last, remote(k, True), turn(low[k], -STRIDE[direction]))
            to_low = jnp.where(part == 0, remote(k, False), turn(high[k], STRIDE[direction]))
        faces[h, 2 * direction, k] = low[k] + to_low
        faces[h, 2 * direction + 1, k] = high[k] + to_high
        up[k] = to_high
        down[k] = to_low
    add_rows(faces, h, direction, up, down, n, both_picks(groups))


def add_outer_x(faces, h, for_high, for_low, up, down, n, groups, pad):
    first = lane_iota(pad) < STRIDE[0]
    last = groups - 1
    to_high = jnp.where(first, 0.0, turn(for_high, STRIDE[0]) if h == 0 else for_high)
    to_low = jnp.where(first, for_low if h == 0 else turn(for_low, STRIDE[0]), 0.0)
    faces[h, 1, last] = faces[h, 1, last] + to_high
    faces[h, 0, 0] = faces[h, 0, 0] + to_low
    up[last] = to_high
    down[0] = to_low
    add_rows(faces, h, 0, up, down, n, [(last, True), (0, False)])


def parity_split(even, high_out, low_out):
    return jnp.where(even, high_out, low_out), jnp.where(even, low_out, high_out)


def whole(*shapes):
    return [jax.ShapeDtypeStruct(s, jnp.float32) for s in shapes]


def vmem_params():
    return pltpu.CompilerParams(vmem_limit_bytes=40 * 2**20)


def face_rows(part, s, k, h, n, halves, store):
    comp = lax.axis_index("comp")
    at = s % 2 * (n - 1)
    sub = k * halves + h
    if s // 2 == 0:
        store(0, n * n, part[pl.ds(plane_at(at, comp, n) + sub, n * n, stride=8), :])
    elif s // 2 == 2:
        count = n * n // 2
        for p in range(2):
            start = plane_at(p * (n // 2), comp, n) + at * 8 + sub
            store(p * count, count, part[pl.ds(start, count, stride=8 * n), :])
    else:
        for a in range(n):
            store(a * n, n, part[pl.ds(plane_at(a, comp, n) + at * n * 8 + sub, n, stride=8), :])


def bf16_pair(x):
    high = x.astype(jnp.bfloat16)
    return [high, (x - high.astype(jnp.float32)).astype(jnp.bfloat16)]


def edge_kernel(part, own, other, *, n, halves):
    size = own.shape[1]
    groups = size // LANES
    pad = rows_padded(n)
    step = STRIDE[0]

    def body(part_ref, own_ref, other_ref, x_even, x_odd, rows):
        comp = lax.axis_index("comp")
        elem = lax.axis_index("elem")
        payload = []
        for side in range(2):
            pieces = []
            match = []
            for h in range(halves):
                place = jnp.where(comp == h, own_ref[...], other_ref[...])
                lane = lax.broadcasted_iota(jnp.int32, (LANES, size), 0)
                goal = jnp.where(lane // step == h, lane - h * step + (size - step if side else 0), -1)
                one = jnp.where(goal == place, 1.0, 0.0).astype(jnp.bfloat16)
                match += [one, one]
                for k in range(groups):

                    def store(at, count, value):
                        rows[side, h, k, at : at + count, :] = value

                    face_rows(part_ref, side, k, h, n, halves, store)
                pieces += bf16_pair(jnp.concatenate([rows[side, h, k] for k in range(groups)], axis=1))
            payload.append(
                lax.dot_general(
                    jnp.concatenate(pieces, axis=1),
                    jnp.concatenate(match, axis=1),
                    (((1,), (1,)), ((), ())),
                    preferred_element_type=jnp.float32,
                )
            )
        x_even[...], x_odd[...] = parity_split(elem // GRID_Y % 2 == 0, payload[1], payload[0])

    return pl.pallas_call(
        body,
        out_shape=whole((pad, LANES), (pad, LANES)),
        scratch_shapes=[pltpu.VMEM((2, halves, groups, pad, LANES), jnp.float32)],
        compiler_params=vmem_params(),
        name="edge",
    )(part, own, other)


def place_kernel(part, own, other, *, n, halves):
    groups = own.shape[1] // LANES
    pad = rows_padded(n)
    inner = n - 2
    shape = (halves, 6, groups, pad, LANES)

    def body(part_ref, own_ref, other_ref, faces, keep, line_rows, up, down):
        comp = lax.axis_index("comp")
        for h in range(halves):
            place = jnp.where(comp == h, own_ref[...], other_ref[...])
            matrix = one_hot(place)
            matrix = jnp.concatenate([matrix, matrix], axis=1)
            for s in range(6):
                for k in range(groups):

                    def store(at, count, value):
                        line_rows[s, k, at : at + count, :] = value

                    face_rows(part_ref, s, k, h, n, halves, store)
                x = jnp.concatenate([line_rows[s, k] for k in range(groups)], axis=1)
                y = split_dot(x, matrix, ((1,), (1,)))
                for k in range(groups):
                    faces[h, s, k] = y[:, k * LANES : (k + 1) * LANES]
        for h in range(halves):
            add_direction(faces, h, 0, None, up, down, n, groups, pad)
        for a in range(inner):
            for b in range(inner):
                for k in range(groups):
                    base = plane_at(a + 1, comp, n) + ((b + 1) * n + 1) * 8 + k * halves
                    keep[pl.ds(((a * inner + b) * groups + k) * inner, inner), :] = part_ref[
                        pl.ds(base + comp, inner, stride=8), :
                    ]

    return pl.pallas_call(
        body,
        out_shape=whole(shape, (inner * inner * inner * groups, LANES)),
        scratch_shapes=[pltpu.VMEM(shape[1:], jnp.float32)] + [pltpu.VMEM((groups, pad, LANES), jnp.float32)] * 2,
        compiler_params=vmem_params(),
        name="place",
    )(part, own, other)


def parity_remote(even, got_even, got_odd):
    return jnp.where(even, got_even, got_odd), jnp.where(even, got_odd, got_even)


def x_kernel(faces_in, got_even, got_odd, *, n):
    halves, _, groups, pad, _ = faces_in.shape

    def body(faces_ref, even_ref, odd_ref, faces, out_even, out_odd, up, down):
        elem = lax.axis_index("elem")
        for_high, for_low = parity_remote(elem // GRID_Y % 2 == 0, even_ref[...], odd_ref[...])
        for h in range(halves):
            add_outer_x(faces, h, for_high, for_low, up, down, n, groups, pad)
        out_even[...], out_odd[...] = parity_split(
            elem % GRID_Y % 2 == 0, *payload_y(faces, groups, pad, halves)
        )

    return pl.pallas_call(
        body,
        out_shape=whole(faces_in.shape, (pad, LANES), (pad, LANES)),
        scratch_shapes=[pltpu.VMEM((groups, pad, LANES), jnp.float32)] * 2,
        input_output_aliases={0: 0},
        compiler_params=vmem_params(),
        name="add_x",
    )(faces_in, got_even, got_odd)


def y_kernel(faces_in, got_even, got_odd, *, n):
    halves, _, groups, pad, _ = faces_in.shape
    last = BLOCK_Z - 1

    def body(faces_ref, even_ref, odd_ref, faces, out, up, down):
        elem = lax.axis_index("elem")
        rep = lax.axis_index("rep")
        for_high, for_low = parity_remote(elem % GRID_Y % 2 == 0, even_ref[...], odd_ref[...])
        for h in range(halves):

            def remote(k, high):
                slot = h * groups + k
                if high:
                    return turn(for_high, (BLOCK_Y - 1 - slot) * STRIDE[1])
                return turn(for_low, -slot * STRIDE[1])

            add_direction(faces, h, 1, remote, up, down, n, groups, pad)
        lower = rep == 0
        choices = (((0, 1), (0, 0)), ((1, 0), (0, 1)), ((1, 1), (1, 0)))
        outs = []
        for mine, theirs in choices:
            pair = []
            for h, side in (mine, theirs):
                pair.append((h, side))
            outs.append(pair)
        part = lane_part(pad, 2)
        for page in range(2):
            value = jnp.zeros((pad, LANES), jnp.float32)
            for index, (a, b) in enumerate(outs):
                if index // 2 != page:
                    continue
                for k in range(groups):
                    slot = index % 2 * groups + k
                    one = turn(faces[a[0], 4 + a[1], k], slot - a[1] * last)
                    two = turn(faces[b[0], 4 + b[1], k], slot - b[1] * last)
                    value = jnp.where(part == slot, jnp.where(lower, one, two), value)
            out[page] = value

    return pl.pallas_call(
        body,
        out_shape=whole(faces_in.shape, (2, pad, LANES)),
        scratch_shapes=[pltpu.VMEM((groups, pad, LANES), jnp.float32)] * 2,
        input_output_aliases={0: 0},
        compiler_params=vmem_params(),
        name="add_y",
    )(faces_in, got_even, got_odd)


def pack_layout(n, groups):
    pad = rows_padded(n)
    mid = (0, (n - 2) * n, (n - 2) * (n - 2))
    tall = (pad // 2 + 7) // 8 * 8
    sizes = [pad * groups, mid[1] * groups, mid[2] * groups, tall, mid[1] // 2, mid[2] // 2]
    starts = [sum(sizes[:i]) for i in range(6)]
    return pad, mid, tall, starts, sum(sizes)


def middle_rows(view, s, n):
    if s == 1:
        return view[n : n * (n - 1), :]
    return jnp.concatenate([view[a * n + 1 : a * n + n - 1, :] for a in range(1, n - 1)], axis=0)


def z_kernel(faces_in, got, *, n):
    halves, _, groups, pad, _ = faces_in.shape
    last = BLOCK_Z - 1
    _, mid, tall, starts, total = pack_layout(n, groups)

    def body(faces_ref, got_ref, faces, keep, send, up, down):
        rep = lax.axis_index("rep")
        comp = lax.axis_index("comp")
        lower = rep == 0
        arrived = {
            (0, True): (0, 1),
            (0, False): (None, 0),
            (1, True): (2, None),
            (1, False): (1, 2),
        }
        for h in range(halves):

            def remote(k, high):
                values = []
                for index in arrived[(h, high)]:
                    if index is None:
                        values.append(jnp.zeros((pad, LANES), jnp.float32))
                    else:
                        slot = index % 2 * groups + k
                        values.append(turn(got_ref[index // 2], (last if high else 0) - slot))
                return jnp.where(lower, values[0], values[1])

            add_direction(faces, h, 2, remote, up, down, n, groups, pad)
        for dst, h in ((keep, comp), (send, 1 - comp)):
            for k in range(groups):
                dst[pl.ds(starts[0] + k * pad, pad), :] = faces[h, 0, k]
                for s in (1, 2):
                    dst[pl.ds(starts[s] + k * mid[s], mid[s]), :] = middle_rows(faces.at[h, 2 * s, k], s, n)
            x = faces.at[h, 1, groups - 1]
            dst[pl.ds(starts[3], tall), :] = jnp.where(
                lane_iota(tall) < STRIDE[0], turn(x[0:tall, :], STRIDE[0]), x[pad - tall : pad, :]
            )
            for s in (1, 2):
                pieces = []
                size = mid[s] // 2
                for k in range(groups):
                    rows = middle_rows(faces.at[h, 2 * s + 1, k], s, n)
                    for part in range(2):
                        pieces.append(
                            (part * groups + k, (BLOCK_Y, BLOCK_Z)[s - 1] - 1, rows[part * size : (part + 1) * size])
                        )
                dst[pl.ds(starts[3 + s], size), :] = gather_slots(size, s, pieces)

    return pl.pallas_call(
        body,
        out_shape=whole(faces_in.shape, (total, LANES), (total, LANES)),
        scratch_shapes=[pltpu.VMEM((groups, pad, LANES), jnp.float32)] * 2,
        input_output_aliases={0: 0},
        compiler_params=vmem_params(),
        name="add_z",
    )(faces_in, got)[1:]


def unpack(pack, s, n, groups, pad):
    _, mid, tall, starts, _ = pack_layout(n, groups)
    if s == 0:
        first = lane_iota(pad) < STRIDE[0]
        low = [pack[pl.ds(starts[0] + k * pad, pad), :] for k in range(groups)]
        edge = pack[pl.ds(starts[3], tall), :]
        edge_full = jnp.concatenate([turn(edge, STRIDE[0])[: pad - tall], edge], axis=0)
        high = []
        for k in range(groups):
            after = turn(low[k + 1], STRIDE[0]) if k + 1 < groups else edge_full
            high.append(jnp.where(first, turn(low[k], STRIDE[0]), after))
        return low, high
    low = [pack[pl.ds(starts[s] + k * mid[s], mid[s]), :] for k in range(groups)]
    edge = pack[pl.ds(starts[3 + s], mid[s] // 2), :]
    last = (BLOCK_Y, BLOCK_Z)[s - 1] - 1
    part = lane_part(mid[s], s)
    high = []
    for k in range(groups):
        far = jnp.concatenate([turn(edge, (last - (p * groups + k)) * STRIDE[s]) for p in range(2)], axis=0)
        high.append(jnp.where(part == last, far, turn(low[k], -STRIDE[s])))
    return low, high


def to_elements(pack, matrix, s, n, groups, pad, store):
    inner = n - 2
    for side, x in enumerate(unpack(pack, s, n, groups, pad)):
        y = split_dot(jnp.concatenate(x, axis=1), matrix, ((1,), (0,)))
        at = side * (n - 1)
        for k in range(groups):
            z = y[:, k * LANES : (k + 1) * LANES]

            def flat(row, count, step=1):
                return pl.ds(row * groups + k, count, stride=step * groups)

            if s == 0:
                store(flat(at * n * n, n * n), z[: n * n])
            for a in range(inner):
                base = (a + 1) * n * n
                if s == 1:
                    store(flat(base + at * n, n), z[a * n : a * n + n])
                if s == 2:
                    store(flat(base + n + at, inner, n), z[a * inner : (a + 1) * inner])


def early_kernel(own_face, own_in, got_in, place, *, n):
    size = place.shape[1]
    groups = size // LANES
    pad = rows_padded(n)
    inner = n - 2

    def body(of, oi, gi, place_ref, out_s, matrix_ref):
        matrix = one_hot(place_ref[...])
        matrix = jnp.concatenate([matrix, matrix], axis=0)
        matrix_ref[...] = matrix

        def store(rows, value):
            out_s[rows, :] = value

        for s in range(3):
            to_elements(of, matrix, s, n, groups, pad, store)
        for a in range(inner):
            for b in range(inner):
                for k in range(groups):
                    src = pl.ds(((a * inner + b) * groups + k) * inner, inner)
                    base = (a + 1) * n * n + (b + 1) * n + 1
                    out_s[pl.ds(base * groups + k, inner, stride=groups), :] = oi[src, :] + gi[src, :]

    return pl.pallas_call(
        body,
        out_shape=[
            jax.ShapeDtypeStruct((n * n * n * groups, LANES), jnp.float32),
            jax.ShapeDtypeStruct((2 * size, size), jnp.bfloat16),
        ],
        compiler_params=vmem_params(),
        name="early",
    )(own_face, own_in, got_in, place)


def final_kernel(early, matrix, got_face, *, n):
    total = early.shape[0]
    groups = total // (n * n * n)
    pad = rows_padded(n)
    edge = (n * n * groups + 7) // 8 * 8

    def body(early_ref, matrix_ref, gf, out_s, out, sem):
        def store(rows, value):
            out_s[rows, :] = out_s[rows, :] + value

        def copy(index, first, count):
            rows = pl.ds(first, count)
            return pltpu.make_async_copy(out_s.at[rows, :], out.at[rows, :], sem.at[index])

        matrix = matrix_ref[...]
        for s in (1, 2):
            to_elements(gf, matrix, s, n, groups, pad, store)
        done = [copy(0, edge, total - 2 * edge), copy(1, 0, edge), copy(2, total - edge, edge)]
        done[0].start()
        to_elements(gf, matrix, 0, n, groups, pad, store)
        done[1].start()
        done[2].start()
        for c in done:
            c.wait()

    return pl.pallas_call(
        body,
        out_shape=whole(early.shape, early.shape),
        out_specs=[pl.BlockSpec(memory_space=pltpu.VMEM), pl.BlockSpec(memory_space=pltpu.HBM)],
        scratch_shapes=[pltpu.SemaphoreType.DMA((3,))],
        input_output_aliases={0: 0},
        compiler_params=vmem_params(),
        name="final",
    )(early, matrix, got_face)[1]


def pairing(at, extent, odd):
    other = at + (1 if at % 2 == (1 if odd else 0) else -1)
    return other if 0 <= other < extent else None


def neighbour_pairs(count, x_odd, y_odd):
    extent = count // GRID_Y
    pairs = []
    for e in range(count):
        sx, sy = divmod(e, GRID_Y)
        tx = sx if x_odd is None else pairing(sx, extent, x_odd)
        ty = sy if y_odd is None else pairing(sy, GRID_Y, y_odd)
        if tx is not None and ty is not None:
            pairs.append((e, tx * GRID_Y + ty))
    return pairs


def exchange(value, x_odd, y_odd):
    pairs = neighbour_pairs(lax.axis_size("elem"), x_odd, y_odd)
    return lax.ppermute(value, "elem", pairs) if pairs else jnp.zeros_like(value)


def body(velocity, geometry, element_place):
    n = velocity.shape[1] * lax.axis_size("comp")
    swap = [(0, 1), (1, 0)]
    other_place = lax.ppermute(element_place, "comp", swap)
    velocity = pltpu.with_memory_space_constraint(velocity, pltpu.HBM)
    geometry = pltpu.with_memory_space_constraint(geometry, pltpu.HBM)
    send_in, part = flux_kernel(velocity, geometry, node_count=n)
    got_in = lax.ppermute(send_in, "comp", swap)
    halves = velocity.shape[4]
    even, odd = edge_kernel(part, element_place, other_place, n=n, halves=halves)
    even = exchange(even, False, None)
    odd = exchange(odd, True, None)
    faces, own_in = place_kernel(part, element_place, other_place, n=n, halves=halves)
    faces, even, odd = x_kernel(faces, even, odd, n=n)
    odd = exchange(odd, None, True)
    even = exchange(even, None, False)
    faces, out = y_kernel(faces, even, odd, n=n)
    got = lax.ppermute(out, "rep", swap)
    own_face, send_face = z_kernel(faces, got, n=n)
    got_face = lax.ppermute(send_face, "comp", swap)
    early, matrix = early_kernel(own_face, own_in, got_in, element_place, n=n)
    result = final_kernel(early, matrix, got_face, n=n)
    return result.reshape(n, n, n, 1, element_place.shape[1])


def solution(mesh):
    placed = (
        P(None, "comp", None, None, None, ("elem", "rep")),
        P(None, None, "comp", None, None, None, ("elem", "rep")),
        P("comp", ("elem", "rep")),
    )

    step = jax.shard_map(
        body,
        mesh=mesh,
        in_specs=placed,
        out_specs=P(None, None, None, "comp", ("elem", "rep")),
        check_vma=False,
    )

    def run(velocity, geometry, element_place):
        with jax.sharding.use_abstract_mesh(mesh.abstract_mesh):
            return step(velocity, geometry, element_place)

    return run
```

```python
import jax
import jax.numpy as jnp
import numpy as np
from jax import lax
from jax.experimental import pallas as pl
from jax.experimental.pallas import tpu as pltpu
from jax.sharding import PartitionSpec as P


BLOCK_Y = 8
BLOCK_Z = 8
GRID_Y = 4
LANES = 128

SLAB_AXES = ((1, 2), (0, 2), (0, 1))


def legendre_columns(points, degree):
    columns = [points * 0.0 + 1.0, points]
    for order in range(2, degree + 1):
        columns.append(
            ((2 * order - 1) * points * columns[order - 1] - (order - 1) * columns[order - 2])
            / order
        )
    return columns


def derivative_table(node_count):
    degree = node_count - 1
    points = np.cos(np.pi * np.arange(node_count) / degree)
    for _ in range(100):
        columns = legendre_columns(points, degree)
        points = points - (points * columns[degree] - columns[degree - 1]) / (
            node_count * columns[degree]
        )
    points = np.sort(points)
    values = legendre_columns(points, degree)[degree]
    identity = np.eye(node_count)
    spacing = points[:, None] - points[None, :] + identity
    matrix = values[:, None] / (values[None, :] * spacing)
    matrix = np.where(identity > 0.5, 0.0, matrix)
    matrix[0, 0] = -degree * (degree + 1) / 4.0
    matrix[degree, degree] = degree * (degree + 1) / 4.0
    return matrix


def weighted(terms):
    total = None
    for value, factor in terms:
        total = value * factor if total is None else total + value * factor
    return total


def transpose_line(line, table):
    count = len(line)
    half = count // 2
    even = [line[i] + line[count - 1 - i] for i in range(half)]
    odd = [line[i] - line[count - 1 - i] for i in range(half)]
    out = [None] * count
    for m in range(half):
        w = count - 1 - m
        both = weighted([(odd[i], float(0.5 * (table[i, m] + table[i, w]))) for i in range(half)])
        diff = weighted([(even[i], float(0.5 * (table[i, m] - table[i, w]))) for i in range(half)])
        out[m] = both + diff
        out[w] = both - diff
    return out


def rows_padded(node_count):
    return (node_count * node_count + 7) // 8 * 8


def plane_at(plane, comp, n):
    return jnp.where(comp == 0, plane, (plane + n // 2) % n) * (n * n * 8)


def flux_kernel(velocity, geometry, *, node_count):
    n = node_count
    planes = velocity.shape[1]
    groups = velocity.shape[5] // LANES
    halves = velocity.shape[4]
    table = derivative_table(n)
    inner = n - 2
    blocks = [(plane, 0, n) for plane in range(planes - 1)]
    blocks += [(planes - 1, 0, n // 2), (planes - 1, n // 2, n - n // 2)]

    def body(v_hbm, g_hbm, send, part, v, g, f0, f1, st, sem):
        comp = lax.axis_index("comp")
        first = comp == 0

        def copies(index):
            plane, start, count = blocks[index]
            rows = pl.ds(start, count)
            out = []
            for k in range(groups):
                lanes = pl.ds(k * LANES, LANES)
                subs = pl.ds(k * halves, halves)
                out.append(
                    pltpu.make_async_copy(
                        v_hbm.at[:, plane, rows, :, :, lanes], v.at[plane, :, rows, :, subs, :], sem.at[2 * k, index]
                    )
                )
                out.append(
                    pltpu.make_async_copy(
                        g_hbm.at[:, :, plane, rows, :, :, lanes],
                        g.at[plane, :, :, rows, :, subs, :],
                        sem.at[2 * k + 1, index],
                    )
                )
            return out

        for index in range(len(blocks)):
            for c in copies(index):
                c.start()

        def row_of(m, b, c):
            return pl.ds(pl.multiple_of((m * n * n + b * n + c) * 8, 8), 8)

        for index, (plane, start, count) in enumerate(blocks):
            for c in copies(index):
                c.wait()

            def along_last(b, carry):
                line = []
                for c in range(n):
                    vel = [v[plane, i, b, c] for i in range(3)]
                    flux = [
                        weighted([(g[plane, i, j, b, c], vel[i]) for i in range(3)]) for j in range(3)
                    ]
                    f0[b, c] = flux[0]
                    f1[b, c] = flux[1]
                    line.append(flux[2])
                out = transpose_line(line, table)
                for c in range(n):
                    st[b, c] = out[c]
                return carry

            lax.fori_loop(start, start + count, along_last, 0)
            if start + count < n:
                continue
            coef = [
                jnp.where(first, float(table[plane, m]), float(table[planes + plane, (m + planes) % n]))
                for m in range(n)
            ]

            def along_others(c, carry):
                out = transpose_line([f1[b, c] for b in range(n)], table)
                for b in range(n):
                    flux = f0[b, c]
                    for m in range(n):
                        value = flux * coef[m]
                        if m == plane:
                            value = value + (st[b, c] + out[b])
                        row = row_of(m, b, c)
                        part[row, :] = value if plane == 0 else part[row, :] + value
                return carry

            lax.fori_loop(0, n, along_others, 0)
        for a in range(inner):
            for b in range(inner):
                for k in range(groups):
                    base = plane_at(a + 1, comp, n) + ((b + 1) * n + 1) * 8 + k * halves
                    send[pl.ds(((a * inner + b) * groups + k) * inner, inner), :] = part[
                        pl.ds(base + 1 - comp, inner, stride=8), :
                    ]

    tile = (8, LANES)
    return pl.pallas_call(
        body,
        in_specs=[pl.BlockSpec(memory_space=pltpu.HBM), pl.BlockSpec(memory_space=pltpu.HBM)],
        out_shape=whole((inner * inner * inner * groups, LANES), (n * n * n * 8, LANES)),
        scratch_shapes=[
            pltpu.VMEM((planes, 3, n, n) + tile, jnp.float32),
            pltpu.VMEM((planes, 3, 3, n, n) + tile, jnp.float32),
            pltpu.VMEM((n, n) + tile, jnp.float32),
            pltpu.VMEM((n, n) + tile, jnp.float32),
            pltpu.VMEM((n, n) + tile, jnp.float32),
            pltpu.SemaphoreType.DMA((2 * groups, planes + 1)),
        ],
        compiler_params=pltpu.CompilerParams(vmem_limit_bytes=42 * 2**20),
        name="flux",
    )(velocity, geometry)


def lane_iota(rows):
    return lax.broadcasted_iota(jnp.int32, (rows, LANES), 1)


def lane_part(rows, direction):
    lane = lane_iota(rows)
    if direction == 0:
        return lane // (BLOCK_Y * BLOCK_Z)
    if direction == 1:
        return lane // BLOCK_Z % BLOCK_Y
    return lane % BLOCK_Z


STRIDE = (BLOCK_Y * BLOCK_Z, BLOCK_Z, 1)


def turn(x, by):
    by = by % LANES
    return x if by == 0 else pltpu.roll(x, by, 1)


def split_dot(x, matrix, dims):
    both = jnp.concatenate(bf16_pair(x), axis=1)
    return lax.dot_general(both, matrix, (dims, ((), ())), preferred_element_type=jnp.float32)


def one_hot(place):
    size = place.shape[1]
    target = lax.broadcasted_iota(jnp.int32, (size, size), 0)
    return jnp.where(target == place, 1.0, 0.0).astype(jnp.bfloat16)


def gather_slots(pad, direction, pieces):
    part = lane_part(pad, direction)
    out = jnp.zeros((pad, LANES), jnp.float32)
    for slot, source, value in pieces:
        out = jnp.where(part == slot, turn(value, (slot - source) * STRIDE[direction]), out)
    return out


def payload_y(faces, groups, pad, halves):
    high_out = gather_slots(
        pad, 1, [(h * groups + k, BLOCK_Y - 1, faces[h, 3, k]) for h in range(halves) for k in range(groups)]
    )
    low_out = gather_slots(
        pad, 1, [(h * groups + k, 0, faces[h, 2, k]) for h in range(halves) for k in range(groups)]
    )
    return high_out, low_out


def row_pick(slab_axes, axis, at, n):
    if slab_axes[0] == axis:
        return pl.ds(at * n, n)
    return pl.ds(at, n, stride=n)


def add_rows(faces, h, direction, up, down, n, picks):
    mine = SLAB_AXES[direction]
    for other in range(3):
        if other == direction:
            continue
        for side in range(2):
            source = row_pick(mine, other, side * (n - 1), n)
            for k, high in picks:
                view = faces.at[h, 2 * other + side, k]
                target = row_pick(SLAB_AXES[other], direction, (n - 1) if high else 0, n)
                delta = up if high else down
                view[target, :] = view[target, :] + delta.at[k][source, :]


def both_picks(groups):
    return [(k, high) for k in range(groups) for high in (False, True)]


def add_direction(faces, h, direction, remote, up, down, n, groups, pad):
    part = lane_part(pad, direction)
    low = [faces[h, 2 * direction, k] for k in range(groups)]
    high = [faces[h, 2 * direction + 1, k] for k in range(groups)]
    zero = jnp.zeros((pad, LANES), jnp.float32)
    for k in range(groups):
        if direction == 0:
            first = lane_iota(pad) < STRIDE[0]
            here = turn(low[k], STRIDE[0])
            after = turn(low[k + 1], STRIDE[0]) if k + 1 < groups else zero
            to_high = jnp.where(first, here, after)
            before = turn(high[k - 1], STRIDE[0]) if k > 0 else zero
            to_low = jnp.where(first, before, turn(high[k], STRIDE[0]))
        else:
            last = (BLOCK_Y, BLOCK_Z)[direction - 1] - 1
            to_high = jnp.where(part == last, remote(k, True), turn(low[k], -STRIDE[direction]))
            to_low = jnp.where(part == 0, remote(k, False), turn(high[k], STRIDE[direction]))
        faces[h, 2 * direction, k] = low[k] + to_low
        faces[h, 2 * direction + 1, k] = high[k] + to_high
        up[k] = to_high
        down[k] = to_low
    add_rows(faces, h, direction, up, down, n, both_picks(groups))


def add_outer_x(faces, h, for_high, for_low, up, down, n, groups, pad):
    first = lane_iota(pad) < STRIDE[0]
    last = groups - 1
    to_high = jnp.where(first, 0.0, turn(for_high, STRIDE[0]) if h == 0 else for_high)
    to_low = jnp.where(first, for_low if h == 0 else turn(for_low, STRIDE[0]), 0.0)
    faces[h, 1, last] = faces[h, 1, last] + to_high
    faces[h, 0, 0] = faces[h, 0, 0] + to_low
    up[last] = to_high
    down[0] = to_low
    add_rows(faces, h, 0, up, down, n, [(last, True), (0, False)])


def parity_split(even, high_out, low_out):
    return jnp.where(even, high_out, low_out), jnp.where(even, low_out, high_out)


def whole(*shapes):
    return [jax.ShapeDtypeStruct(s, jnp.float32) for s in shapes]


def vmem_params():
    return pltpu.CompilerParams(vmem_limit_bytes=40 * 2**20)


def face_rows(part, s, k, h, n, halves, store):
    comp = lax.axis_index("comp")
    at = s % 2 * (n - 1)
    sub = k * halves + h
    if s // 2 == 0:
        store(0, n * n, part[pl.ds(plane_at(at, comp, n) + sub, n * n, stride=8), :])
    elif s // 2 == 2:
        count = n * n // 2
        for p in range(2):
            start = plane_at(p * (n // 2), comp, n) + at * 8 + sub
            store(p * count, count, part[pl.ds(start, count, stride=8 * n), :])
    else:
        for a in range(n):
            store(a * n, n, part[pl.ds(plane_at(a, comp, n) + at * n * 8 + sub, n, stride=8), :])


def bf16_pair(x):
    high = x.astype(jnp.bfloat16)
    return [high, (x - high.astype(jnp.float32)).astype(jnp.bfloat16)]


def edge_kernel(part, own, other, *, n, halves):
    size = own.shape[1]
    groups = size // LANES
    pad = rows_padded(n)
    step = STRIDE[0]

    def body(part_ref, own_ref, other_ref, x_even, x_odd, rows):
        comp = lax.axis_index("comp")
        elem = lax.axis_index("elem")
        payload = []
        for side in range(2):
            pieces = []
            match = []
            for h in range(halves):
                place = jnp.where(comp == h, own_ref[...], other_ref[...])
                lane = lax.broadcasted_iota(jnp.int32, (LANES, size), 0)
                goal = jnp.where(lane // step == h, lane - h * step + (size - step if side else 0), -1)
                one = jnp.where(goal == place, 1.0, 0.0).astype(jnp.bfloat16)
                match += [one, one]
                for k in range(groups):

                    def store(at, count, value):
                        rows[side, h, k, at : at + count, :] = value

                    face_rows(part_ref, side, k, h, n, halves, store)
                pieces += bf16_pair(jnp.concatenate([rows[side, h, k] for k in range(groups)], axis=1))
            payload.append(
                lax.dot_general(
                    jnp.concatenate(pieces, axis=1),
                    jnp.concatenate(match, axis=1),
                    (((1,), (1,)), ((), ())),
                    preferred_element_type=jnp.float32,
                )
            )
        x_even[...], x_odd[...] = parity_split(elem // GRID_Y % 2 == 0, payload[1], payload[0])

    return pl.pallas_call(
        body,
        out_shape=whole((pad, LANES), (pad, LANES)),
        scratch_shapes=[pltpu.VMEM((2, halves, groups, pad, LANES), jnp.float32)],
        compiler_params=vmem_params(),
        name="edge",
    )(part, own, other)


def place_kernel(part, own, other, *, n, halves):
    groups = own.shape[1] // LANES
    pad = rows_padded(n)
    inner = n - 2
    shape = (halves, 6, groups, pad, LANES)

    def body(part_ref, own_ref, other_ref, faces, keep, line_rows, up, down):
        comp = lax.axis_index("comp")
        for h in range(halves):
            place = jnp.where(comp == h, own_ref[...], other_ref[...])
            matrix = one_hot(place)
            matrix = jnp.concatenate([matrix, matrix], axis=1)
            for s in range(6):
                for k in range(groups):

                    def store(at, count, value):
                        line_rows[s, k, at : at + count, :] = value

                    face_rows(part_ref, s, k, h, n, halves, store)
                x = jnp.concatenate([line_rows[s, k] for k in range(groups)], axis=1)
                y = split_dot(x, matrix, ((1,), (1,)))
                for k in range(groups):
                    faces[h, s, k] = y[:, k * LANES : (k + 1) * LANES]
        for h in range(halves):
            add_direction(faces, h, 0, None, up, down, n, groups, pad)
        for a in range(inner):
            for b in range(inner):
                for k in range(groups):
                    base = plane_at(a + 1, comp, n) + ((b + 1) * n + 1) * 8 + k * halves
                    keep[pl.ds(((a * inner + b) * groups + k) * inner, inner), :] = part_ref[
                        pl.ds(base + comp, inner, stride=8), :
                    ]

    return pl.pallas_call(
        body,
        out_shape=whole(shape, (inner * inner * inner * groups, LANES)),
        scratch_shapes=[pltpu.VMEM(shape[1:], jnp.float32)] + [pltpu.VMEM((groups, pad, LANES), jnp.float32)] * 2,
        compiler_params=vmem_params(),
        name="place",
    )(part, own, other)


def parity_remote(at, extent, got_even, got_odd):
    even = at % 2 == 0
    high = jnp.where(even, got_even, got_odd)
    low = jnp.where(even, got_odd, got_even)
    return jnp.where(at + 1 < extent, high, 0.0), jnp.where(at > 0, low, 0.0)


def x_kernel(faces_in, got_even, got_odd, *, n):
    halves, _, groups, pad, _ = faces_in.shape

    def body(faces_ref, even_ref, odd_ref, faces, out_even, out_odd, up, down):
        elem = lax.axis_index("elem")
        extent = lax.axis_size("elem") // GRID_Y
        for_high, for_low = parity_remote(elem // GRID_Y, extent, even_ref[...], odd_ref[...])
        for h in range(halves):
            add_outer_x(faces, h, for_high, for_low, up, down, n, groups, pad)
        out_even[...], out_odd[...] = parity_split(
            elem % GRID_Y % 2 == 0, *payload_y(faces, groups, pad, halves)
        )

    return pl.pallas_call(
        body,
        out_shape=whole(faces_in.shape, (pad, LANES), (pad, LANES)),
        scratch_shapes=[pltpu.VMEM((groups, pad, LANES), jnp.float32)] * 2,
        input_output_aliases={0: 0},
        compiler_params=vmem_params(),
        name="add_x",
    )(faces_in, got_even, got_odd)


def y_kernel(faces_in, got_even, got_odd, *, n):
    halves, _, groups, pad, _ = faces_in.shape
    last = BLOCK_Z - 1

    def body(faces_ref, even_ref, odd_ref, faces, out, up, down):
        elem = lax.axis_index("elem")
        rep = lax.axis_index("rep")
        for_high, for_low = parity_remote(elem % GRID_Y, GRID_Y, even_ref[...], odd_ref[...])
        for h in range(halves):

            def remote(k, high):
                slot = h * groups + k
                if high:
                    return turn(for_high, (BLOCK_Y - 1 - slot) * STRIDE[1])
                return turn(for_low, -slot * STRIDE[1])

            add_direction(faces, h, 1, remote, up, down, n, groups, pad)
        lower = rep == 0
        choices = (((0, 1), (0, 0)), ((1, 0), (0, 1)), ((1, 1), (1, 0)))
        outs = []
        for mine, theirs in choices:
            pair = []
            for h, side in (mine, theirs):
                pair.append((h, side))
            outs.append(pair)
        part = lane_part(pad, 2)
        for page in range(2):
            value = jnp.zeros((pad, LANES), jnp.float32)
            for index, (a, b) in enumerate(outs):
                if index // 2 != page:
                    continue
                for k in range(groups):
                    slot = index % 2 * groups + k
                    one = turn(faces[a[0], 4 + a[1], k], slot - a[1] * last)
                    two = turn(faces[b[0], 4 + b[1], k], slot - b[1] * last)
                    value = jnp.where(part == slot, jnp.where(lower, one, two), value)
            out[page] = value

    return pl.pallas_call(
        body,
        out_shape=whole(faces_in.shape, (2, pad, LANES)),
        scratch_shapes=[pltpu.VMEM((groups, pad, LANES), jnp.float32)] * 2,
        input_output_aliases={0: 0},
        compiler_params=vmem_params(),
        name="add_y",
    )(faces_in, got_even, got_odd)


def pack_layout(n, groups):
    pad = rows_padded(n)
    mid = (0, (n - 2) * n, (n - 2) * (n - 2))
    tall = (pad // 2 + 7) // 8 * 8
    x_sizes = [pad * groups, tall]
    sizes = [mid[1] * groups, mid[2] * groups, mid[1] // 2, mid[2] // 2]
    starts = [0] + [sum(sizes[:i]) for i in range(4)]
    return pad, mid, tall, starts, (sum(x_sizes), sum(sizes))


def middle_rows(view, s, n):
    if s == 1:
        return view[n : n * (n - 1), :]
    return jnp.concatenate([view[a * n + 1 : a * n + n - 1, :] for a in range(1, n - 1)], axis=0)


def z_kernel(faces_in, got, *, n):
    halves, _, groups, pad, _ = faces_in.shape
    last = BLOCK_Z - 1
    _, mid, tall, starts, totals = pack_layout(n, groups)

    def body(faces_ref, got_ref, faces, keep_x, keep, send_x, send, up, down):
        rep = lax.axis_index("rep")
        comp = lax.axis_index("comp")
        lower = rep == 0
        arrived = {
            (0, True): (0, 1),
            (0, False): (None, 0),
            (1, True): (2, None),
            (1, False): (1, 2),
        }
        for h in range(halves):

            def remote(k, high):
                values = []
                for index in arrived[(h, high)]:
                    if index is None:
                        values.append(jnp.zeros((pad, LANES), jnp.float32))
                    else:
                        slot = index % 2 * groups + k
                        values.append(turn(got_ref[index // 2], (last if high else 0) - slot))
                return jnp.where(lower, values[0], values[1])

            add_direction(faces, h, 2, remote, up, down, n, groups, pad)
        for dst_x, dst, h in ((keep_x, keep, comp), (send_x, send, 1 - comp)):
            for k in range(groups):
                dst_x[pl.ds(k * pad, pad), :] = faces[h, 0, k]
                for s in (1, 2):
                    dst[pl.ds(starts[s] + k * mid[s], mid[s]), :] = middle_rows(faces.at[h, 2 * s, k], s, n)
            x = faces.at[h, 1, groups - 1]
            dst_x[pl.ds(groups * pad, tall), :] = jnp.where(
                lane_iota(tall) < STRIDE[0], turn(x[0:tall, :], STRIDE[0]), x[pad - tall : pad, :]
            )
            for s in (1, 2):
                pieces = []
                size = mid[s] // 2
                for k in range(groups):
                    rows = middle_rows(faces.at[h, 2 * s + 1, k], s, n)
                    for part in range(2):
                        pieces.append(
                            (part * groups + k, (BLOCK_Y, BLOCK_Z)[s - 1] - 1, rows[part * size : (part + 1) * size])
                        )
                dst[pl.ds(starts[2 + s], size), :] = gather_slots(size, s, pieces)

    return pl.pallas_call(
        body,
        out_shape=whole(faces_in.shape, *[(total, LANES) for total in totals * 2]),
        scratch_shapes=[pltpu.VMEM((groups, pad, LANES), jnp.float32)] * 2,
        input_output_aliases={0: 0},
        compiler_params=vmem_params(),
        name="add_z",
    )(faces_in, got)[1:]


def unpack(pack, s, n, groups, pad):
    _, mid, tall, starts, _ = pack_layout(n, groups)
    if s == 0:
        first = lane_iota(pad) < STRIDE[0]
        low = [pack[pl.ds(k * pad, pad), :] for k in range(groups)]
        edge = pack[pl.ds(groups * pad, tall), :]
        edge_full = jnp.concatenate([turn(edge, STRIDE[0])[: pad - tall], edge], axis=0)
        high = []
        for k in range(groups):
            after = turn(low[k + 1], STRIDE[0]) if k + 1 < groups else edge_full
            high.append(jnp.where(first, turn(low[k], STRIDE[0]), after))
        return low, high
    low = [pack[pl.ds(starts[s] + k * mid[s], mid[s]), :] for k in range(groups)]
    edge = pack[pl.ds(starts[2 + s], mid[s] // 2), :]
    last = (BLOCK_Y, BLOCK_Z)[s - 1] - 1
    part = lane_part(mid[s], s)
    high = []
    for k in range(groups):
        far = jnp.concatenate([turn(edge, (last - (p * groups + k)) * STRIDE[s]) for p in range(2)], axis=0)
        high.append(jnp.where(part == last, far, turn(low[k], -STRIDE[s])))
    return low, high


def to_elements(pack, matrix, s, n, groups, pad, store):
    inner = n - 2
    for side, x in enumerate(unpack(pack, s, n, groups, pad)):
        y = split_dot(jnp.concatenate(x, axis=1), matrix, ((1,), (0,)))
        at = side * (n - 1)
        for k in range(groups):
            z = y[:, k * LANES : (k + 1) * LANES]

            def flat(row, count, step=1):
                return pl.ds(row * groups + k, count, stride=step * groups)

            if s == 0:
                store(flat(at * n * n, n * n), z[: n * n])
            for a in range(inner):
                base = (a + 1) * n * n
                if s == 1:
                    store(flat(base + at * n, n), z[a * n : a * n + n])
                if s == 2:
                    store(flat(base + n + at, inner, n), z[a * inner : (a + 1) * inner])


def early_kernel(own_x, own_face, own_in, got_in, place, *, n):
    size = place.shape[1]
    groups = size // LANES
    pad = rows_padded(n)
    inner = n - 2

    def body(ox, of, oi, gi, place_ref, out_s, matrix_ref):
        matrix = one_hot(place_ref[...])
        matrix = jnp.concatenate([matrix, matrix], axis=0)
        matrix_ref[...] = matrix

        def store(rows, value):
            out_s[rows, :] = value

        for s in range(3):
            to_elements(of if s else ox, matrix, s, n, groups, pad, store)
        for a in range(inner):
            for b in range(inner):
                for k in range(groups):
                    src = pl.ds(((a * inner + b) * groups + k) * inner, inner)
                    base = (a + 1) * n * n + (b + 1) * n + 1
                    out_s[pl.ds(base * groups + k, inner, stride=groups), :] = oi[src, :] + gi[src, :]

    return pl.pallas_call(
        body,
        out_shape=[
            jax.ShapeDtypeStruct((n * n * n * groups, LANES), jnp.float32),
            jax.ShapeDtypeStruct((2 * size, size), jnp.bfloat16),
        ],
        compiler_params=vmem_params(),
        name="early",
    )(own_x, own_face, own_in, got_in, place)


def outer_rows(n, groups):
    return (n * n * groups + 7) // 8 * 8


def middle_kernel(early, matrix, got_face, *, n):
    total = early.shape[0]
    groups = total // (n * n * n)
    pad = rows_padded(n)
    edge = outer_rows(n, groups)

    def body(early_ref, matrix_ref, gf, out_s, out, sem):
        def store(rows, value):
            out_s[rows, :] = out_s[rows, :] + value

        matrix = matrix_ref[...]
        for s in (1, 2):
            to_elements(gf, matrix, s, n, groups, pad, store)
        rows = pl.ds(edge, total - 2 * edge)
        done = pltpu.make_async_copy(out_s.at[rows, :], out.at[rows, :], sem)
        done.start()
        done.wait()

    return pl.pallas_call(
        body,
        out_shape=whole(early.shape, early.shape),
        out_specs=[pl.BlockSpec(memory_space=pltpu.VMEM), pl.BlockSpec(memory_space=pltpu.HBM)],
        scratch_shapes=[pltpu.SemaphoreType.DMA],
        input_output_aliases={0: 0},
        compiler_params=vmem_params(),
        name="middle",
    )(early, matrix, got_face)


def final_kernel(early, result, matrix, got_x, *, n):
    total = early.shape[0]
    groups = total // (n * n * n)
    pad = rows_padded(n)
    edge = outer_rows(n, groups)

    def body(early_ref, result_ref, matrix_ref, gx, out, ends, sem):
        far = total - edge
        ends[0:edge, :] = early_ref[0:edge, :]
        ends[edge : 2 * edge, :] = early_ref[far:total, :]

        def store(rows, value):
            start = rows.start if rows.start < edge else rows.start - far + edge
            here = pl.ds(start, rows.size, stride=rows.stride)
            ends[here, :] = ends[here, :] + value

        to_elements(gx, matrix_ref[...], 0, n, groups, pad, store)
        done = [
            pltpu.make_async_copy(ends.at[pl.ds(i * edge, edge), :], out.at[pl.ds(i * far, edge), :], sem.at[i])
            for i in range(2)
        ]
        for c in done:
            c.start()
        for c in done:
            c.wait()

    return pl.pallas_call(
        body,
        out_shape=whole(early.shape)[0],
        in_specs=[
            pl.BlockSpec(memory_space=pltpu.VMEM),
            pl.BlockSpec(memory_space=pltpu.HBM),
            pl.BlockSpec(memory_space=pltpu.VMEM),
            pl.BlockSpec(memory_space=pltpu.VMEM),
        ],
        out_specs=pl.BlockSpec(memory_space=pltpu.HBM),
        scratch_shapes=[pltpu.VMEM((2 * edge, LANES), jnp.float32), pltpu.SemaphoreType.DMA((2,))],
        input_output_aliases={1: 0},
        compiler_params=vmem_params(),
        name="final",
    )(early, result, matrix, got_x)


def pairing(at, extent, odd):
    return (at + (1 if at % 2 == (1 if odd else 0) else -1)) % extent


def neighbour_pairs(count, along_x, odd):
    extent = count // GRID_Y if along_x else GRID_Y
    if extent == 1 or (odd and extent == 2):
        return []
    pairs = []
    for e in range(count):
        sx, sy = divmod(e, GRID_Y)
        to = pairing(sx, extent, odd) * GRID_Y + sy if along_x else sx * GRID_Y + pairing(sy, extent, odd)
        pairs.append((e, to))
    return pairs


def exchange(value, along_x, odd):
    pairs = neighbour_pairs(lax.axis_size("elem"), along_x, odd)
    return lax.ppermute(value, "elem", pairs) if pairs else jnp.zeros_like(value)


def body(velocity, geometry, element_place):
    n = velocity.shape[1] * lax.axis_size("comp")
    swap = [(0, 1), (1, 0)]
    other_place = lax.ppermute(element_place, "comp", swap)
    velocity = pltpu.with_memory_space_constraint(velocity, pltpu.HBM)
    geometry = pltpu.with_memory_space_constraint(geometry, pltpu.HBM)
    send_in, part = flux_kernel(velocity, geometry, node_count=n)
    got_in = lax.ppermute(send_in, "comp", swap)
    halves = velocity.shape[4]
    even, odd = edge_kernel(part, element_place, other_place, n=n, halves=halves)
    even = exchange(even, True, False)
    odd = exchange(odd, True, True)
    faces, own_in = place_kernel(part, element_place, other_place, n=n, halves=halves)
    faces, even, odd = x_kernel(faces, even, odd, n=n)
    odd = exchange(odd, False, True)
    even = exchange(even, False, False)
    faces, out = y_kernel(faces, even, odd, n=n)
    got = lax.ppermute(out, "rep", swap)
    own_x, own_face, send_x, send_face = z_kernel(faces, got, n=n)
    got_face = lax.ppermute(send_face, "comp", swap)
    got_x = lax.ppermute(send_x, "comp", swap)
    early, matrix = early_kernel(own_x, own_face, own_in, got_in, element_place, n=n)
    early, result = middle_kernel(early, matrix, got_face, n=n)
    result = final_kernel(early, result, matrix, got_x, n=n)
    return result.reshape(n, n, n, 1, element_place.shape[1])


def solution(mesh):
    placed = (
        P(None, "comp", None, None, None, ("elem", "rep")),
        P(None, None, "comp", None, None, None, ("elem", "rep")),
        P("comp", ("elem", "rep")),
    )

    step = jax.shard_map(
        body,
        mesh=mesh,
        in_specs=placed,
        out_specs=P(None, None, None, "comp", ("elem", "rep")),
        check_vma=False,
    )

    def run(velocity, geometry, element_place):
        with jax.sharding.use_abstract_mesh(mesh.abstract_mesh):
            return step(velocity, geometry, element_place)

    return run
```

```python
import jax
import jax.numpy as jnp
import numpy as np
from jax import lax
from jax.experimental import pallas as pl
from jax.experimental.pallas import tpu as pltpu
from jax.sharding import PartitionSpec as P


BLOCK_Y = 8
BLOCK_Z = 8
GRID_Y = 4
LANES = 128

SLAB_AXES = ((1, 2), (0, 2), (0, 1))


def legendre_columns(points, degree):
    columns = [points * 0.0 + 1.0, points]
    for order in range(2, degree + 1):
        columns.append(
            ((2 * order - 1) * points * columns[order - 1] - (order - 1) * columns[order - 2])
            / order
        )
    return columns


def derivative_table(node_count):
    degree = node_count - 1
    points = np.cos(np.pi * np.arange(node_count) / degree)
    for _ in range(100):
        columns = legendre_columns(points, degree)
        points = points - (points * columns[degree] - columns[degree - 1]) / (
            node_count * columns[degree]
        )
    points = np.sort(points)
    values = legendre_columns(points, degree)[degree]
    identity = np.eye(node_count)
    spacing = points[:, None] - points[None, :] + identity
    matrix = values[:, None] / (values[None, :] * spacing)
    matrix = np.where(identity > 0.5, 0.0, matrix)
    matrix[0, 0] = -degree * (degree + 1) / 4.0
    matrix[degree, degree] = degree * (degree + 1) / 4.0
    return matrix


def weighted(terms):
    total = None
    for value, factor in terms:
        total = value * factor if total is None else total + value * factor
    return total


def transpose_line(line, table):
    count = len(line)
    half = count // 2
    even = [line[i] + line[count - 1 - i] for i in range(half)]
    odd = [line[i] - line[count - 1 - i] for i in range(half)]
    out = [None] * count
    for m in range(half):
        w = count - 1 - m
        both = weighted([(odd[i], float(0.5 * (table[i, m] + table[i, w]))) for i in range(half)])
        diff = weighted([(even[i], float(0.5 * (table[i, m] - table[i, w]))) for i in range(half)])
        out[m] = both + diff
        out[w] = both - diff
    return out


def rows_padded(node_count):
    return (node_count * node_count + 7) // 8 * 8


def in_pairs(start, count, step):
    def pair(i, carry):
        step(start + 2 * i)
        step(start + 2 * i + 1)
        return carry

    lax.fori_loop(0, count // 2, pair, 0)


def plane_at(plane, comp, n):
    return jnp.where(comp == 0, plane, (plane + n // 2) % n) * (n * n * 8)


def flux_kernel(velocity, geometry, *, node_count):
    n = node_count
    planes = velocity.shape[1]
    groups = velocity.shape[5] // LANES
    halves = velocity.shape[4]
    table = derivative_table(n)
    inner = n - 2
    cut = n // 4 * 2
    blocks = [(0, 0, cut), (0, cut, n - cut)]
    blocks += [(plane, 0, n) for plane in range(1, planes - 1)]
    blocks += [(planes - 1, 0, n - 2), (planes - 1, n - 2, 2)]

    def body(v_hbm, g_hbm, send, part, v, g, f1, sem):
        comp = lax.axis_index("comp")
        first = comp == 0

        def copies(index):
            plane, start, count = blocks[index]
            rows = pl.ds(start, count)
            out = []
            for k in range(groups):
                lanes = pl.ds(k * LANES, LANES)
                subs = pl.ds(k * halves, halves)
                out.append(
                    pltpu.make_async_copy(
                        v_hbm.at[:, plane, rows, :, :, lanes], v.at[plane, :, rows, :, subs, :], sem.at[2 * k, index]
                    )
                )
                out.append(
                    pltpu.make_async_copy(
                        g_hbm.at[:, :, plane, rows, :, :, lanes],
                        g.at[plane, :, :, rows, :, subs, :],
                        sem.at[2 * k + 1, index],
                    )
                )
            return out

        for index in range(len(blocks)):
            for c in copies(index):
                c.start()

        def row_of(m, b, c):
            return pl.ds(pl.multiple_of((m * n * n + b * n + c) * 8, 8), 8)

        for index, (plane, start, count) in enumerate(blocks):
            coef = [
                jnp.where(first, float(table[plane, m]), float(table[planes + plane, (m + planes) % n]))
                for m in range(n)
            ]
            for c in copies(index):
                c.wait()

            def along_ends(b):
                line = []
                rows = []
                for c in range(n):
                    vel = [v[plane, i, b, c] for i in range(3)]
                    flux = [
                        weighted([(g[plane, i, j, b, c], vel[i]) for i in range(3)]) for j in range(3)
                    ]
                    f1[b, c] = flux[1]
                    line.append(flux[2])
                    rows.append([flux[0] * coef[m] for m in range(n)])
                out = transpose_line(line, table)
                for c in range(n):
                    for m in range(n):
                        value = rows[c][m] + out[c] if m == plane else rows[c][m]
                        row = row_of(m, b, c)
                        part[row, :] = value if plane == 0 else part[row, :] + value

            in_pairs(start, count, along_ends)
            if start + count < n:
                continue

            def along_middle(c):
                out = transpose_line([f1[b, c] for b in range(n)], table)
                for b in range(n):
                    row = row_of(plane, b, c)
                    part[row, :] = part[row, :] + out[b]

            in_pairs(0, n, along_middle)
        for a in range(inner):
            base = plane_at(a + 1, comp, n) + 1 - comp
            for b in range(inner):
                for k in range(groups):
                    send[pl.ds(((a * inner + b) * groups + k) * inner, inner), :] = part[
                        pl.ds(base + (((b + 1) * n + 1) * 8 + k * halves), inner, stride=8), :
                    ]

    tile = (8, LANES)
    return pl.pallas_call(
        body,
        in_specs=[pl.BlockSpec(memory_space=pltpu.HBM), pl.BlockSpec(memory_space=pltpu.HBM)],
        out_shape=whole((inner * inner * inner * groups, LANES), (n * n * n * 8, LANES)),
        scratch_shapes=[
            pltpu.VMEM((planes, 3, n, n) + tile, jnp.float32),
            pltpu.VMEM((planes, 3, 3, n, n) + tile, jnp.float32),
            pltpu.VMEM((n, n) + tile, jnp.float32),
            pltpu.SemaphoreType.DMA((2 * groups, planes + 2)),
        ],
        compiler_params=pltpu.CompilerParams(vmem_limit_bytes=42 * 2**20),
        name="flux",
    )(velocity, geometry)


def lane_iota(rows):
    return lax.broadcasted_iota(jnp.int32, (rows, LANES), 1)


def lane_part(rows, direction):
    lane = lane_iota(rows)
    if direction == 0:
        return lane // (BLOCK_Y * BLOCK_Z)
    if direction == 1:
        return lane // BLOCK_Z % BLOCK_Y
    return lane % BLOCK_Z


STRIDE = (BLOCK_Y * BLOCK_Z, BLOCK_Z, 1)


def turn(x, by):
    by = by % LANES
    return x if by == 0 else pltpu.roll(x, by, 1)


def split_dot(x, matrix, dims):
    both = jnp.concatenate(bf16_pair(x), axis=1)
    return lax.dot_general(both, matrix, (dims, ((), ())), preferred_element_type=jnp.float32)


def one_hot(place):
    size = place.shape[1]
    target = lax.broadcasted_iota(jnp.int32, (size, size), 0)
    return jnp.where(target == place, 1.0, 0.0).astype(jnp.bfloat16)


def gather_slots(pad, direction, pieces):
    part = lane_part(pad, direction)
    out = jnp.zeros((pad, LANES), jnp.float32)
    for slot, source, value in pieces:
        out = jnp.where(part == slot, turn(value, (slot - source) * STRIDE[direction]), out)
    return out


def payload_y(faces, groups, pad, halves):
    high_out = gather_slots(
        pad, 1, [(h * groups + k, BLOCK_Y - 1, faces[h, 3, k]) for h in range(halves) for k in range(groups)]
    )
    low_out = gather_slots(
        pad, 1, [(h * groups + k, 0, faces[h, 2, k]) for h in range(halves) for k in range(groups)]
    )
    return high_out, low_out


def row_pick(slab_axes, axis, at, n):
    if slab_axes[0] == axis:
        return pl.ds(at * n, n)
    return pl.ds(at, n, stride=n)


def add_rows(faces, h, direction, up, down, n, picks):
    mine = SLAB_AXES[direction]
    for other in range(3):
        if other == direction:
            continue
        for side in range(2):
            source = row_pick(mine, other, side * (n - 1), n)
            for k, high in picks:
                view = faces.at[h, 2 * other + side, k]
                target = row_pick(SLAB_AXES[other], direction, (n - 1) if high else 0, n)
                delta = up if high else down
                view[target, :] = view[target, :] + delta.at[k][source, :]


def both_picks(groups):
    return [(k, high) for k in range(groups) for high in (False, True)]


def add_direction(faces, h, direction, remote, up, down, n, groups, pad):
    part = lane_part(pad, direction)
    low = [faces[h, 2 * direction, k] for k in range(groups)]
    high = [faces[h, 2 * direction + 1, k] for k in range(groups)]
    zero = jnp.zeros((pad, LANES), jnp.float32)
    for k in range(groups):
        if direction == 0:
            first = lane_iota(pad) < STRIDE[0]
            here = turn(low[k], STRIDE[0])
            after = turn(low[k + 1], STRIDE[0]) if k + 1 < groups else zero
            to_high = jnp.where(first, here, after)
            before = turn(high[k - 1], STRIDE[0]) if k > 0 else zero
            to_low = jnp.where(first, before, turn(high[k], STRIDE[0]))
        else:
            last = (BLOCK_Y, BLOCK_Z)[direction - 1] - 1
            to_high = jnp.where(part == last, remote(k, True), turn(low[k], -STRIDE[direction]))
            to_low = jnp.where(part == 0, remote(k, False), turn(high[k], STRIDE[direction]))
        faces[h, 2 * direction, k] = low[k] + to_low
        faces[h, 2 * direction + 1, k] = high[k] + to_high
        up[k] = to_high
        down[k] = to_low
    add_rows(faces, h, direction, up, down, n, both_picks(groups))


def add_outer_x(faces, h, for_high, for_low, up, down, n, groups, pad):
    first = lane_iota(pad) < STRIDE[0]
    last = groups - 1
    to_high = jnp.where(first, 0.0, turn(for_high, STRIDE[0]) if h == 0 else for_high)
    to_low = jnp.where(first, for_low if h == 0 else turn(for_low, STRIDE[0]), 0.0)
    faces[h, 1, last] = faces[h, 1, last] + to_high
    faces[h, 0, 0] = faces[h, 0, 0] + to_low
    up[last] = to_high
    down[0] = to_low
    add_rows(faces, h, 0, up, down, n, [(last, True), (0, False)])


def parity_split(even, high_out, low_out):
    return jnp.where(even, high_out, low_out), jnp.where(even, low_out, high_out)


def whole(*shapes):
    return [jax.ShapeDtypeStruct(s, jnp.float32) for s in shapes]


def vmem_params():
    return pltpu.CompilerParams(vmem_limit_bytes=40 * 2**20)


def face_rows(part, s, k, h, n, halves, store):
    comp = lax.axis_index("comp")
    at = s % 2 * (n - 1)
    sub = k * halves + h
    if s // 2 == 0:
        store(0, n * n, part[pl.ds(plane_at(at, comp, n) + sub, n * n, stride=8), :])
    elif s // 2 == 2:
        count = n * n // 2
        for p in range(2):
            start = plane_at(p * (n // 2), comp, n) + at * 8 + sub
            store(p * count, count, part[pl.ds(start, count, stride=8 * n), :])
    else:
        for a in range(n):
            store(a * n, n, part[pl.ds(plane_at(a, comp, n) + at * n * 8 + sub, n, stride=8), :])


def bf16_pair(x):
    high = x.astype(jnp.bfloat16)
    return [high, (x - high.astype(jnp.float32)).astype(jnp.bfloat16)]


def edge_kernel(part, own, other, *, n, halves):
    size = own.shape[1]
    groups = size // LANES
    pad = rows_padded(n)
    step = STRIDE[0]

    def body(part_ref, own_ref, other_ref, x_even, x_odd, rows):
        comp = lax.axis_index("comp")
        elem = lax.axis_index("elem")
        payload = []
        for side in range(2):
            pieces = []
            match = []
            for h in range(halves):
                place = jnp.where(comp == h, own_ref[...], other_ref[...])
                lane = lax.broadcasted_iota(jnp.int32, (LANES, size), 0)
                goal = jnp.where(lane // step == h, lane - h * step + (size - step if side else 0), -1)
                one = jnp.where(goal == place, 1.0, 0.0).astype(jnp.bfloat16)
                match += [one, one]
                for k in range(groups):

                    def store(at, count, value):
                        rows[side, h, k, at : at + count, :] = value

                    face_rows(part_ref, side, k, h, n, halves, store)
                pieces += bf16_pair(jnp.concatenate([rows[side, h, k] for k in range(groups)], axis=1))
            payload.append(
                lax.dot_general(
                    jnp.concatenate(pieces, axis=1),
                    jnp.concatenate(match, axis=1),
                    (((1,), (1,)), ((), ())),
                    preferred_element_type=jnp.float32,
                )
            )
        x_even[...], x_odd[...] = parity_split(elem // GRID_Y % 2 == 0, payload[1], payload[0])

    return pl.pallas_call(
        body,
        out_shape=whole((pad, LANES), (pad, LANES)),
        scratch_shapes=[pltpu.VMEM((2, halves, groups, pad, LANES), jnp.float32)],
        compiler_params=vmem_params(),
        name="edge",
    )(part, own, other)


def place_kernel(part, own, other, *, n, halves):
    groups = own.shape[1] // LANES
    pad = rows_padded(n)
    inner = n - 2
    shape = (halves, 6, groups, pad, LANES)

    def body(part_ref, own_ref, other_ref, faces, keep, line_rows, up, down):
        comp = lax.axis_index("comp")
        for h in range(halves):
            place = jnp.where(comp == h, own_ref[...], other_ref[...])
            matrix = one_hot(place)
            matrix = jnp.concatenate([matrix, matrix], axis=1)
            for s in range(6):
                for k in range(groups):

                    def store(at, count, value):
                        line_rows[s, k, at : at + count, :] = value

                    face_rows(part_ref, s, k, h, n, halves, store)
                x = jnp.concatenate([line_rows[s, k] for k in range(groups)], axis=1)
                y = split_dot(x, matrix, ((1,), (1,)))
                for k in range(groups):
                    faces[h, s, k] = y[:, k * LANES : (k + 1) * LANES]
        for h in range(halves):
            add_direction(faces, h, 0, None, up, down, n, groups, pad)
        for a in range(inner):
            for b in range(inner):
                for k in range(groups):
                    base = plane_at(a + 1, comp, n) + ((b + 1) * n + 1) * 8 + k * halves
                    keep[pl.ds(((a * inner + b) * groups + k) * inner, inner), :] = part_ref[
                        pl.ds(base + comp, inner, stride=8), :
                    ]

    return pl.pallas_call(
        body,
        out_shape=whole(shape, (inner * inner * inner * groups, LANES)),
        scratch_shapes=[pltpu.VMEM(shape[1:], jnp.float32)] + [pltpu.VMEM((groups, pad, LANES), jnp.float32)] * 2,
        compiler_params=vmem_params(),
        name="place",
    )(part, own, other)


def parity_remote(at, extent, got_even, got_odd):
    even = at % 2 == 0
    high = jnp.where(even, got_even, got_odd)
    low = jnp.where(even, got_odd, got_even)
    return jnp.where(at + 1 < extent, high, 0.0), jnp.where(at > 0, low, 0.0)


def x_kernel(faces_in, got_even, got_odd, *, n):
    halves, _, groups, pad, _ = faces_in.shape

    def body(faces_ref, even_ref, odd_ref, faces, out_even, out_odd, up, down):
        elem = lax.axis_index("elem")
        extent = lax.axis_size("elem") // GRID_Y
        for_high, for_low = parity_remote(elem // GRID_Y, extent, even_ref[...], odd_ref[...])
        for h in range(halves):
            add_outer_x(faces, h, for_high, for_low, up, down, n, groups, pad)
        out_even[...], out_odd[...] = parity_split(
            elem % GRID_Y % 2 == 0, *payload_y(faces, groups, pad, halves)
        )

    return pl.pallas_call(
        body,
        out_shape=whole(faces_in.shape, (pad, LANES), (pad, LANES)),
        scratch_shapes=[pltpu.VMEM((groups, pad, LANES), jnp.float32)] * 2,
        input_output_aliases={0: 0},
        compiler_params=vmem_params(),
        name="add_x",
    )(faces_in, got_even, got_odd)


def y_kernel(faces_in, got_even, got_odd, *, n):
    halves, _, groups, pad, _ = faces_in.shape
    last = BLOCK_Z - 1

    def body(faces_ref, even_ref, odd_ref, faces, out, up, down):
        elem = lax.axis_index("elem")
        rep = lax.axis_index("rep")
        for_high, for_low = parity_remote(elem % GRID_Y, GRID_Y, even_ref[...], odd_ref[...])
        for h in range(halves):

            def remote(k, high):
                slot = h * groups + k
                if high:
                    return turn(for_high, (BLOCK_Y - 1 - slot) * STRIDE[1])
                return turn(for_low, -slot * STRIDE[1])

            add_direction(faces, h, 1, remote, up, down, n, groups, pad)
        lower = rep == 0
        choices = (((0, 1), (0, 0)), ((1, 0), (0, 1)), ((1, 1), (1, 0)))
        outs = []
        for mine, theirs in choices:
            pair = []
            for h, side in (mine, theirs):
                pair.append((h, side))
            outs.append(pair)
        part = lane_part(pad, 2)
        for page in range(2):
            value = jnp.zeros((pad, LANES), jnp.float32)
            for index, (a, b) in enumerate(outs):
                if index // 2 != page:
                    continue
                for k in range(groups):
                    slot = index % 2 * groups + k
                    one = turn(faces[a[0], 4 + a[1], k], slot - a[1] * last)
                    two = turn(faces[b[0], 4 + b[1], k], slot - b[1] * last)
                    value = jnp.where(part == slot, jnp.where(lower, one, two), value)
            out[page] = value

    return pl.pallas_call(
        body,
        out_shape=whole(faces_in.shape, (2, pad, LANES)),
        scratch_shapes=[pltpu.VMEM((groups, pad, LANES), jnp.float32)] * 2,
        input_output_aliases={0: 0},
        compiler_params=vmem_params(),
        name="add_y",
    )(faces_in, got_even, got_odd)


def pack_layout(n, groups):
    pad = rows_padded(n)
    mid = (0, (n - 2) * n, (n - 2) * (n - 2))
    tall = (pad // 2 + 7) // 8 * 8
    x_sizes = [pad * groups, tall]
    sizes = [mid[1] * groups, mid[2] * groups, mid[1] // 2, mid[2] // 2]
    starts = [0] + [sum(sizes[:i]) for i in range(4)]
    return pad, mid, tall, starts, (sum(x_sizes), sum(sizes))


def middle_rows(view, s, n):
    if s == 1:
        return view[n : n * (n - 1), :]
    return jnp.concatenate([view[a * n + 1 : a * n + n - 1, :] for a in range(1, n - 1)], axis=0)


def z_kernel(faces_in, got, *, n):
    halves, _, groups, pad, _ = faces_in.shape
    last = BLOCK_Z - 1
    _, mid, tall, starts, totals = pack_layout(n, groups)

    def body(faces_ref, got_ref, faces, keep_x, keep, send_x, send, up, down):
        rep = lax.axis_index("rep")
        comp = lax.axis_index("comp")
        lower = rep == 0
        arrived = {
            (0, True): (0, 1),
            (0, False): (None, 0),
            (1, True): (2, None),
            (1, False): (1, 2),
        }
        for h in range(halves):

            def remote(k, high):
                values = []
                for index in arrived[(h, high)]:
                    if index is None:
                        values.append(jnp.zeros((pad, LANES), jnp.float32))
                    else:
                        slot = index % 2 * groups + k
                        values.append(turn(got_ref[index // 2], (last if high else 0) - slot))
                return jnp.where(lower, values[0], values[1])

            add_direction(faces, h, 2, remote, up, down, n, groups, pad)
        for dst_x, dst, h in ((keep_x, keep, comp), (send_x, send, 1 - comp)):
            for k in range(groups):
                dst_x[pl.ds(k * pad, pad), :] = faces[h, 0, k]
                for s in (1, 2):
                    dst[pl.ds(starts[s] + k * mid[s], mid[s]), :] = middle_rows(faces.at[h, 2 * s, k], s, n)
            x = faces.at[h, 1, groups - 1]
            dst_x[pl.ds(groups * pad, tall), :] = jnp.where(
                lane_iota(tall) < STRIDE[0], turn(x[0:tall, :], STRIDE[0]), x[pad - tall : pad, :]
            )
            for s in (1, 2):
                pieces = []
                size = mid[s] // 2
                for k in range(groups):
                    rows = middle_rows(faces.at[h, 2 * s + 1, k], s, n)
                    for part in range(2):
                        pieces.append(
                            (part * groups + k, (BLOCK_Y, BLOCK_Z)[s - 1] - 1, rows[part * size : (part + 1) * size])
                        )
                dst[pl.ds(starts[2 + s], size), :] = gather_slots(size, s, pieces)

    return pl.pallas_call(
        body,
        out_shape=whole(faces_in.shape, *[(total, LANES) for total in totals * 2]),
        scratch_shapes=[pltpu.VMEM((groups, pad, LANES), jnp.float32)] * 2,
        input_output_aliases={0: 0},
        compiler_params=vmem_params(),
        name="add_z",
    )(faces_in, got)[1:]


def unpack(pack, s, n, groups, pad):
    _, mid, tall, starts, _ = pack_layout(n, groups)
    if s == 0:
        first = lane_iota(pad) < STRIDE[0]
        low = [pack[pl.ds(k * pad, pad), :] for k in range(groups)]
        edge = pack[pl.ds(groups * pad, tall), :]
        edge_full = jnp.concatenate([turn(edge, STRIDE[0])[: pad - tall], edge], axis=0)
        high = []
        for k in range(groups):
            after = turn(low[k + 1], STRIDE[0]) if k + 1 < groups else edge_full
            high.append(jnp.where(first, turn(low[k], STRIDE[0]), after))
        return low, high
    low = [pack[pl.ds(starts[s] + k * mid[s], mid[s]), :] for k in range(groups)]
    edge = pack[pl.ds(starts[2 + s], mid[s] // 2), :]
    last = (BLOCK_Y, BLOCK_Z)[s - 1] - 1
    part = lane_part(mid[s], s)
    high = []
    for k in range(groups):
        far = jnp.concatenate([turn(edge, (last - (p * groups + k)) * STRIDE[s]) for p in range(2)], axis=0)
        high.append(jnp.where(part == last, far, turn(low[k], -STRIDE[s])))
    return low, high


def to_elements(pack, matrix, s, n, groups, pad, store):
    inner = n - 2
    for side, x in enumerate(unpack(pack, s, n, groups, pad)):
        y = split_dot(jnp.concatenate(x, axis=1), matrix, ((1,), (0,)))
        at = side * (n - 1)
        for k in range(groups):
            z = y[:, k * LANES : (k + 1) * LANES]

            def flat(row, count, step=1):
                return pl.ds(row * groups + k, count, stride=step * groups)

            if s == 0:
                store(flat(at * n * n, n * n), z[: n * n])
            for a in range(inner):
                base = (a + 1) * n * n
                if s == 1:
                    store(flat(base + at * n, n), z[a * n : a * n + n])
                if s == 2:
                    store(flat(base + n + at, inner, n), z[a * inner : (a + 1) * inner])


def early_kernel(own_x, own_face, own_in, got_in, place, *, n):
    size = place.shape[1]
    groups = size // LANES
    pad = rows_padded(n)
    inner = n - 2

    def body(ox, of, oi, gi, place_ref, out_s, matrix_ref):
        matrix = one_hot(place_ref[...])
        matrix = jnp.concatenate([matrix, matrix], axis=0)
        matrix_ref[...] = matrix

        def store(rows, value):
            out_s[rows, :] = value

        for s in range(3):
            to_elements(of if s else ox, matrix, s, n, groups, pad, store)
        for a in range(inner):
            for b in range(inner):
                for k in range(groups):
                    src = pl.ds(((a * inner + b) * groups + k) * inner, inner)
                    base = (a + 1) * n * n + (b + 1) * n + 1
                    out_s[pl.ds(base * groups + k, inner, stride=groups), :] = oi[src, :] + gi[src, :]

    return pl.pallas_call(
        body,
        out_shape=[
            jax.ShapeDtypeStruct((n * n * n * groups, LANES), jnp.float32),
            jax.ShapeDtypeStruct((2 * size, size), jnp.bfloat16),
        ],
        compiler_params=vmem_params(),
        name="early",
    )(own_x, own_face, own_in, got_in, place)


def outer_rows(n, groups):
    return (n * n * groups + 7) // 8 * 8


def middle_kernel(early, matrix, got_face, *, n):
    total = early.shape[0]
    groups = total // (n * n * n)
    pad = rows_padded(n)
    edge = outer_rows(n, groups)

    def body(early_ref, matrix_ref, gf, out_s, out, sem):
        def store(rows, value):
            out_s[rows, :] = out_s[rows, :] + value

        matrix = matrix_ref[...]
        for s in (1, 2):
            to_elements(gf, matrix, s, n, groups, pad, store)
        rows = pl.ds(edge, total - 2 * edge)
        done = pltpu.make_async_copy(out_s.at[rows, :], out.at[rows, :], sem)
        done.start()
        done.wait()

    return pl.pallas_call(
        body,
        out_shape=whole(early.shape, early.shape),
        out_specs=[pl.BlockSpec(memory_space=pltpu.VMEM), pl.BlockSpec(memory_space=pltpu.HBM)],
        scratch_shapes=[pltpu.SemaphoreType.DMA],
        input_output_aliases={0: 0},
        compiler_params=vmem_params(),
        name="middle",
    )(early, matrix, got_face)


def final_kernel(early, result, matrix, got_x, *, n):
    total = early.shape[0]
    groups = total // (n * n * n)
    pad = rows_padded(n)
    edge = outer_rows(n, groups)

    def body(early_ref, result_ref, matrix_ref, gx, out, ends, sem):
        far = total - edge
        ends[0:edge, :] = early_ref[0:edge, :]
        ends[edge : 2 * edge, :] = early_ref[far:total, :]

        def store(rows, value):
            start = rows.start if rows.start < edge else rows.start - far + edge
            here = pl.ds(start, rows.size, stride=rows.stride)
            ends[here, :] = ends[here, :] + value

        to_elements(gx, matrix_ref[...], 0, n, groups, pad, store)
        done = [
            pltpu.make_async_copy(ends.at[pl.ds(i * edge, edge), :], out.at[pl.ds(i * far, edge), :], sem.at[i])
            for i in range(2)
        ]
        for c in done:
            c.start()
        for c in done:
            c.wait()

    return pl.pallas_call(
        body,
        out_shape=whole(early.shape)[0],
        in_specs=[
            pl.BlockSpec(memory_space=pltpu.VMEM),
            pl.BlockSpec(memory_space=pltpu.HBM),
            pl.BlockSpec(memory_space=pltpu.VMEM),
            pl.BlockSpec(memory_space=pltpu.VMEM),
        ],
        out_specs=pl.BlockSpec(memory_space=pltpu.HBM),
        scratch_shapes=[pltpu.VMEM((2 * edge, LANES), jnp.float32), pltpu.SemaphoreType.DMA((2,))],
        input_output_aliases={1: 0},
        compiler_params=vmem_params(),
        name="final",
    )(early, result, matrix, got_x)


def pairing(at, extent, odd):
    return (at + (1 if at % 2 == (1 if odd else 0) else -1)) % extent


def neighbour_pairs(count, along_x, odd):
    extent = count // GRID_Y if along_x else GRID_Y
    if extent == 1 or (odd and extent == 2):
        return []
    pairs = []
    for e in range(count):
        sx, sy = divmod(e, GRID_Y)
        to = pairing(sx, extent, odd) * GRID_Y + sy if along_x else sx * GRID_Y + pairing(sy, extent, odd)
        pairs.append((e, to))
    return pairs


def exchange(value, along_x, odd):
    pairs = neighbour_pairs(lax.axis_size("elem"), along_x, odd)
    return lax.ppermute(value, "elem", pairs) if pairs else jnp.zeros_like(value)


def body(velocity, geometry, element_place):
    n = velocity.shape[1] * lax.axis_size("comp")
    swap = [(0, 1), (1, 0)]
    other_place = lax.ppermute(element_place, "comp", swap)
    velocity = pltpu.with_memory_space_constraint(velocity, pltpu.HBM)
    geometry = pltpu.with_memory_space_constraint(geometry, pltpu.HBM)
    send_in, part = flux_kernel(velocity, geometry, node_count=n)
    got_in = lax.ppermute(send_in, "comp", swap)
    halves = velocity.shape[4]
    even, odd = edge_kernel(part, element_place, other_place, n=n, halves=halves)
    even = exchange(even, True, False)
    odd = exchange(odd, True, True)
    faces, own_in = place_kernel(part, element_place, other_place, n=n, halves=halves)
    faces, even, odd = x_kernel(faces, even, odd, n=n)
    odd = exchange(odd, False, True)
    even = exchange(even, False, False)
    faces, out = y_kernel(faces, even, odd, n=n)
    got = lax.ppermute(out, "rep", swap)
    own_x, own_face, send_x, send_face = z_kernel(faces, got, n=n)
    got_face = lax.ppermute(send_face, "comp", swap)
    got_x = lax.ppermute(send_x, "comp", swap)
    early, matrix = early_kernel(own_x, own_face, own_in, got_in, element_place, n=n)
    early, result = middle_kernel(early, matrix, got_face, n=n)
    result = final_kernel(early, result, matrix, got_x, n=n)
    return result.reshape(n, n, n, 1, element_place.shape[1])


def solution(mesh):
    placed = (
        P(None, "comp", None, None, None, ("elem", "rep")),
        P(None, None, "comp", None, None, None, ("elem", "rep")),
        P("comp", ("elem", "rep")),
    )

    step = jax.shard_map(
        body,
        mesh=mesh,
        in_specs=placed,
        out_specs=P(None, None, None, "comp", ("elem", "rep")),
        check_vma=False,
    )

    def run(velocity, geometry, element_place):
        with jax.sharding.use_abstract_mesh(mesh.abstract_mesh):
            return step(velocity, geometry, element_place)

    return run
```

```python
import jax
import jax.numpy as jnp
import numpy as np
from jax import lax
from jax.experimental import pallas as pl
from jax.experimental.pallas import tpu as pltpu
from jax.sharding import PartitionSpec as P


BLOCK_Y = 8
BLOCK_Z = 8
GRID_Y = 4
LANES = 128

SLAB_AXES = ((1, 2), (0, 2), (0, 1))


def legendre_columns(points, degree):
    columns = [points * 0.0 + 1.0, points]
    for order in range(2, degree + 1):
        columns.append(
            ((2 * order - 1) * points * columns[order - 1] - (order - 1) * columns[order - 2])
            / order
        )
    return columns


def derivative_table(node_count):
    degree = node_count - 1
    points = np.cos(np.pi * np.arange(node_count) / degree)
    for _ in range(100):
        columns = legendre_columns(points, degree)
        points = points - (points * columns[degree] - columns[degree - 1]) / (
            node_count * columns[degree]
        )
    points = np.sort(points)
    values = legendre_columns(points, degree)[degree]
    identity = np.eye(node_count)
    spacing = points[:, None] - points[None, :] + identity
    matrix = values[:, None] / (values[None, :] * spacing)
    matrix = np.where(identity > 0.5, 0.0, matrix)
    matrix[0, 0] = -degree * (degree + 1) / 4.0
    matrix[degree, degree] = degree * (degree + 1) / 4.0
    return matrix


def weighted(terms):
    total = None
    for value, factor in terms:
        total = value * factor if total is None else total + value * factor
    return total


def transpose_line(line, table):
    count = len(line)
    half = count // 2
    even = [line[i] + line[count - 1 - i] for i in range(half)]
    odd = [line[i] - line[count - 1 - i] for i in range(half)]
    out = [None] * count
    for m in range(half):
        w = count - 1 - m
        both = weighted([(odd[i], float(0.5 * (table[i, m] + table[i, w]))) for i in range(half)])
        diff = weighted([(even[i], float(0.5 * (table[i, m] - table[i, w]))) for i in range(half)])
        out[m] = both + diff
        out[w] = both - diff
    return out


def rows_padded(node_count):
    return (node_count * node_count + 7) // 8 * 8


def in_pairs(start, count, step):
    def pair(i, carry):
        step(start + 2 * i)
        step(start + 2 * i + 1)
        return carry

    lax.fori_loop(0, count // 2, pair, 0)


def plane_at(plane, comp, n):
    return jnp.where(comp == 0, plane, (plane + n // 2) % n) * (n * n * 8)


def flux_kernel(velocity, geometry, *, node_count):
    n = node_count
    planes = velocity.shape[1]
    groups = velocity.shape[5] // LANES
    halves = velocity.shape[4]
    table = derivative_table(n)
    inner = n - 2
    cut = n // 4 * 2
    blocks = [(0, 0, cut), (0, cut, n - cut)]
    blocks += [(plane, 0, n) for plane in range(1, planes - 1)]
    blocks += [(planes - 1, 0, n - 2), (planes - 1, n - 2, 2)]

    def body(v_hbm, g_hbm, send, part, v, g, f1, sem):
        comp = lax.axis_index("comp")
        first = comp == 0

        def copies(index):
            plane, start, count = blocks[index]
            rows = pl.ds(start, count)
            out = []
            for k in range(groups):
                lanes = pl.ds(k * LANES, LANES)
                subs = pl.ds(k * halves, halves)
                out.append(
                    pltpu.make_async_copy(
                        v_hbm.at[:, plane, rows, :, :, lanes], v.at[plane, :, rows, :, subs, :], sem.at[2 * k, index]
                    )
                )
                out.append(
                    pltpu.make_async_copy(
                        g_hbm.at[:, :, plane, rows, :, :, lanes],
                        g.at[plane, :, :, rows, :, subs, :],
                        sem.at[2 * k + 1, index],
                    )
                )
            return out

        for index in range(len(blocks)):
            for c in copies(index):
                c.start()

        def row_of(m, b, c):
            return pl.ds(pl.multiple_of((m * n * n + b * n + c) * 8, 8), 8)

        for index, (plane, start, count) in enumerate(blocks):
            coef = [
                jnp.where(first, float(table[plane, m]), float(table[planes + plane, (m + planes) % n]))
                for m in range(n)
            ]
            for c in copies(index):
                c.wait()

            def along_ends(b):
                line = []
                rows = []
                for c in range(n):
                    vel = [v[plane, i, b, c] for i in range(3)]
                    flux = [
                        weighted([(g[plane, i, j, b, c], vel[i]) for i in range(3)]) for j in range(3)
                    ]
                    f1[b, c] = flux[1]
                    line.append(flux[2])
                    rows.append([flux[0] * coef[m] for m in range(n)])
                out = transpose_line(line, table)
                for c in range(n):
                    for m in range(n):
                        value = rows[c][m] + out[c] if m == plane else rows[c][m]
                        row = row_of(m, b, c)
                        part[row, :] = value if plane == 0 else part[row, :] + value

            in_pairs(start, count, along_ends)
            if start + count < n:
                continue

            def along_middle(c):
                out = transpose_line([f1[b, c] for b in range(n)], table)
                for b in range(n):
                    row = row_of(plane, b, c)
                    part[row, :] = part[row, :] + out[b]

            in_pairs(0, n, along_middle)
        for a in range(inner):
            base = plane_at(a + 1, comp, n) + 1 - comp
            for b in range(inner):
                for k in range(groups):
                    send[pl.ds(((a * inner + b) * groups + k) * inner, inner), :] = part[
                        pl.ds(base + (((b + 1) * n + 1) * 8 + k * halves), inner, stride=8), :
                    ]

    tile = (8, LANES)
    return pl.pallas_call(
        body,
        in_specs=[pl.BlockSpec(memory_space=pltpu.HBM), pl.BlockSpec(memory_space=pltpu.HBM)],
        out_shape=whole((inner * inner * inner * groups, LANES), (n * n * n * 8, LANES)),
        scratch_shapes=[
            pltpu.VMEM((planes, 3, n, n) + tile, jnp.float32),
            pltpu.VMEM((planes, 3, 3, n, n) + tile, jnp.float32),
            pltpu.VMEM((n, n) + tile, jnp.float32),
            pltpu.SemaphoreType.DMA((2 * groups, planes + 2)),
        ],
        compiler_params=pltpu.CompilerParams(vmem_limit_bytes=42 * 2**20),
        name="flux",
    )(velocity, geometry)


def lane_iota(rows):
    return lax.broadcasted_iota(jnp.int32, (rows, LANES), 1)


def lane_part(rows, direction):
    lane = lane_iota(rows)
    if direction == 0:
        return lane // (BLOCK_Y * BLOCK_Z)
    if direction == 1:
        return lane // BLOCK_Z % BLOCK_Y
    return lane % BLOCK_Z


STRIDE = (BLOCK_Y * BLOCK_Z, BLOCK_Z, 1)


def turn(x, by):
    by = by % LANES
    return x if by == 0 else pltpu.roll(x, by, 1)


def split_dot(x, matrix, dims):
    both = jnp.concatenate(bf16_pair(x), axis=1)
    return lax.dot_general(both, matrix, (dims, ((), ())), preferred_element_type=jnp.float32)


def one_hot(place):
    size = place.shape[1]
    target = lax.broadcasted_iota(jnp.int32, (size, size), 0)
    return jnp.where(target == place, 1.0, 0.0).astype(jnp.bfloat16)


def gather_slots(pad, direction, pieces):
    part = lane_part(pad, direction)
    out = jnp.zeros((pad, LANES), jnp.float32)
    for slot, source, value in pieces:
        out = jnp.where(part == slot, turn(value, (slot - source) * STRIDE[direction]), out)
    return out


def payload_y(faces, groups, pad, halves):
    high_out = gather_slots(
        pad, 1, [(h * groups + k, BLOCK_Y - 1, faces[h, 3, k]) for h in range(halves) for k in range(groups)]
    )
    low_out = gather_slots(
        pad, 1, [(h * groups + k, 0, faces[h, 2, k]) for h in range(halves) for k in range(groups)]
    )
    return high_out, low_out


def row_pick(slab_axes, axis, at, n):
    if slab_axes[0] == axis:
        return pl.ds(at * n, n)
    return pl.ds(at, n, stride=n)


def add_rows(faces, h, direction, up, down, n, picks):
    mine = SLAB_AXES[direction]
    for other in range(3):
        if other == direction:
            continue
        for side in range(2):
            source = row_pick(mine, other, side * (n - 1), n)
            for k, high in picks:
                view = faces.at[h, 2 * other + side, k]
                target = row_pick(SLAB_AXES[other], direction, (n - 1) if high else 0, n)
                delta = up if high else down
                view[target, :] = view[target, :] + delta.at[k][source, :]


def both_picks(groups):
    return [(k, high) for k in range(groups) for high in (False, True)]


def add_direction(faces, h, direction, remote, up, down, n, groups, pad):
    part = lane_part(pad, direction)
    low = [faces[h, 2 * direction, k] for k in range(groups)]
    high = [faces[h, 2 * direction + 1, k] for k in range(groups)]
    zero = jnp.zeros((pad, LANES), jnp.float32)
    for k in range(groups):
        if direction == 0:
            first = lane_iota(pad) < STRIDE[0]
            here = turn(low[k], STRIDE[0])
            after = turn(low[k + 1], STRIDE[0]) if k + 1 < groups else zero
            to_high = jnp.where(first, here, after)
            before = turn(high[k - 1], STRIDE[0]) if k > 0 else zero
            to_low = jnp.where(first, before, turn(high[k], STRIDE[0]))
        else:
            last = (BLOCK_Y, BLOCK_Z)[direction - 1] - 1
            to_high = jnp.where(part == last, remote(k, True), turn(low[k], -STRIDE[direction]))
            to_low = jnp.where(part == 0, remote(k, False), turn(high[k], STRIDE[direction]))
        faces[h, 2 * direction, k] = low[k] + to_low
        faces[h, 2 * direction + 1, k] = high[k] + to_high
        up[k] = to_high
        down[k] = to_low
    add_rows(faces, h, direction, up, down, n, both_picks(groups))


def add_outer_x(faces, h, for_high, for_low, up, down, n, groups, pad):
    first = lane_iota(pad) < STRIDE[0]
    last = groups - 1
    to_high = jnp.where(first, 0.0, turn(for_high, STRIDE[0]) if h == 0 else for_high)
    to_low = jnp.where(first, for_low if h == 0 else turn(for_low, STRIDE[0]), 0.0)
    faces[h, 1, last] = faces[h, 1, last] + to_high
    faces[h, 0, 0] = faces[h, 0, 0] + to_low
    up[last] = to_high
    down[0] = to_low
    add_rows(faces, h, 0, up, down, n, [(last, True), (0, False)])


def parity_split(even, high_out, low_out):
    return jnp.where(even, high_out, low_out), jnp.where(even, low_out, high_out)


def whole(*shapes):
    return [jax.ShapeDtypeStruct(s, jnp.float32) for s in shapes]


def vmem_params():
    return pltpu.CompilerParams(vmem_limit_bytes=40 * 2**20)


def face_rows(part, s, k, h, n, halves, store):
    comp = lax.axis_index("comp")
    at = s % 2 * (n - 1)
    sub = k * halves + h
    if s // 2 == 0:
        store(0, n * n, part[pl.ds(plane_at(at, comp, n) + sub, n * n, stride=8), :])
    elif s // 2 == 2:
        count = n * n // 2
        for p in range(2):
            start = plane_at(p * (n // 2), comp, n) + at * 8 + sub
            store(p * count, count, part[pl.ds(start, count, stride=8 * n), :])
    else:
        for a in range(n):
            store(a * n, n, part[pl.ds(plane_at(a, comp, n) + at * n * 8 + sub, n, stride=8), :])


def bf16_pair(x):
    high = x.astype(jnp.bfloat16)
    return [high, (x - high.astype(jnp.float32)).astype(jnp.bfloat16)]


def edge_kernel(part, own, other, *, n, halves):
    size = own.shape[1]
    groups = size // LANES
    pad = rows_padded(n)
    step = STRIDE[0]

    def body(part_ref, own_ref, other_ref, x_even, x_odd, rows):
        comp = lax.axis_index("comp")
        elem = lax.axis_index("elem")
        payload = []
        for side in range(2):
            pieces = []
            match = []
            for h in range(halves):
                place = jnp.where(comp == h, own_ref[...], other_ref[...])
                lane = lax.broadcasted_iota(jnp.int32, (LANES, size), 0)
                goal = jnp.where(lane // step == h, lane - h * step + (size - step if side else 0), -1)
                one = jnp.where(goal == place, 1.0, 0.0).astype(jnp.bfloat16)
                match += [one, one]
                for k in range(groups):

                    def store(at, count, value):
                        rows[side, h, k, at : at + count, :] = value

                    face_rows(part_ref, side, k, h, n, halves, store)
                pieces += bf16_pair(jnp.concatenate([rows[side, h, k] for k in range(groups)], axis=1))
            payload.append(
                lax.dot_general(
                    jnp.concatenate(pieces, axis=1),
                    jnp.concatenate(match, axis=1),
                    (((1,), (1,)), ((), ())),
                    preferred_element_type=jnp.float32,
                )
            )
        x_even[...], x_odd[...] = parity_split(elem // GRID_Y % 2 == 0, payload[1], payload[0])

    return pl.pallas_call(
        body,
        out_shape=whole((pad, LANES), (pad, LANES)),
        scratch_shapes=[pltpu.VMEM((2, halves, groups, pad, LANES), jnp.float32)],
        compiler_params=vmem_params(),
        name="edge",
    )(part, own, other)


def place_kernel(part, own, other, *, n, halves):
    groups = own.shape[1] // LANES
    pad = rows_padded(n)
    shape = (halves, 6, groups, pad, LANES)

    def body(part_ref, own_ref, other_ref, faces, line_rows, up, down):
        comp = lax.axis_index("comp")
        for h in range(halves):
            place = jnp.where(comp == h, own_ref[...], other_ref[...])
            matrix = one_hot(place)
            matrix = jnp.concatenate([matrix, matrix], axis=1)
            for s in range(6):
                for k in range(groups):

                    def store(at, count, value):
                        line_rows[s, k, at : at + count, :] = value

                    face_rows(part_ref, s, k, h, n, halves, store)
                x = jnp.concatenate([line_rows[s, k] for k in range(groups)], axis=1)
                y = split_dot(x, matrix, ((1,), (1,)))
                for k in range(groups):
                    faces[h, s, k] = y[:, k * LANES : (k + 1) * LANES]
        for h in range(halves):
            add_direction(faces, h, 0, None, up, down, n, groups, pad)

    return pl.pallas_call(
        body,
        out_shape=whole(shape)[0],
        scratch_shapes=[pltpu.VMEM(shape[1:], jnp.float32)] + [pltpu.VMEM((groups, pad, LANES), jnp.float32)] * 2,
        compiler_params=vmem_params(),
        name="place",
    )(part, own, other)


def parity_remote(at, extent, got_even, got_odd):
    even = at % 2 == 0
    high = jnp.where(even, got_even, got_odd)
    low = jnp.where(even, got_odd, got_even)
    return jnp.where(at + 1 < extent, high, 0.0), jnp.where(at > 0, low, 0.0)


def x_kernel(faces_in, got_even, got_odd, *, n):
    halves, _, groups, pad, _ = faces_in.shape

    def body(faces_ref, even_ref, odd_ref, faces, out_even, out_odd, up, down):
        elem = lax.axis_index("elem")
        extent = lax.axis_size("elem") // GRID_Y
        for_high, for_low = parity_remote(elem // GRID_Y, extent, even_ref[...], odd_ref[...])
        for h in range(halves):
            add_outer_x(faces, h, for_high, for_low, up, down, n, groups, pad)
        out_even[...], out_odd[...] = parity_split(
            elem % GRID_Y % 2 == 0, *payload_y(faces, groups, pad, halves)
        )

    return pl.pallas_call(
        body,
        out_shape=whole(faces_in.shape, (pad, LANES), (pad, LANES)),
        scratch_shapes=[pltpu.VMEM((groups, pad, LANES), jnp.float32)] * 2,
        input_output_aliases={0: 0},
        compiler_params=vmem_params(),
        name="add_x",
    )(faces_in, got_even, got_odd)


def y_kernel(faces_in, got_even, got_odd, *, n):
    halves, _, groups, pad, _ = faces_in.shape
    last = BLOCK_Z - 1

    def body(faces_ref, even_ref, odd_ref, faces, out, up, down):
        elem = lax.axis_index("elem")
        rep = lax.axis_index("rep")
        for_high, for_low = parity_remote(elem % GRID_Y, GRID_Y, even_ref[...], odd_ref[...])
        for h in range(halves):

            def remote(k, high):
                slot = h * groups + k
                if high:
                    return turn(for_high, (BLOCK_Y - 1 - slot) * STRIDE[1])
                return turn(for_low, -slot * STRIDE[1])

            add_direction(faces, h, 1, remote, up, down, n, groups, pad)
        lower = rep == 0
        choices = (((0, 1), (0, 0)), ((1, 0), (0, 1)), ((1, 1), (1, 0)))
        outs = []
        for mine, theirs in choices:
            pair = []
            for h, side in (mine, theirs):
                pair.append((h, side))
            outs.append(pair)
        part = lane_part(pad, 2)
        for page in range(2):
            value = jnp.zeros((pad, LANES), jnp.float32)
            for index, (a, b) in enumerate(outs):
                if index // 2 != page:
                    continue
                for k in range(groups):
                    slot = index % 2 * groups + k
                    one = turn(faces[a[0], 4 + a[1], k], slot - a[1] * last)
                    two = turn(faces[b[0], 4 + b[1], k], slot - b[1] * last)
                    value = jnp.where(part == slot, jnp.where(lower, one, two), value)
            out[page] = value

    return pl.pallas_call(
        body,
        out_shape=whole(faces_in.shape, (2, pad, LANES)),
        scratch_shapes=[pltpu.VMEM((groups, pad, LANES), jnp.float32)] * 2,
        input_output_aliases={0: 0},
        compiler_params=vmem_params(),
        name="add_y",
    )(faces_in, got_even, got_odd)


def pack_layout(n, groups):
    pad = rows_padded(n)
    mid = (0, (n - 2) * n, (n - 2) * (n - 2))
    tall = n * n // 2
    x_sizes = [n * n * groups, tall]
    sizes = [mid[1] * groups, mid[2] * groups, mid[1] // 2, mid[2] // 2]
    starts = [0] + [sum(sizes[:i]) for i in range(4)]
    return pad, mid, tall, starts, (sum(x_sizes), sum(sizes))


def middle_rows(view, s, n):
    if s == 1:
        return view[n : n * (n - 1), :]
    return jnp.concatenate([view[a * n + 1 : a * n + n - 1, :] for a in range(1, n - 1)], axis=0)


def z_kernel(faces_in, got, *, n):
    halves, _, groups, pad, _ = faces_in.shape
    last = BLOCK_Z - 1
    _, mid, tall, starts, totals = pack_layout(n, groups)

    def body(faces_ref, got_ref, faces, keep_x, keep, send_x, send, up, down):
        rep = lax.axis_index("rep")
        comp = lax.axis_index("comp")
        lower = rep == 0
        arrived = {
            (0, True): (0, 1),
            (0, False): (None, 0),
            (1, True): (2, None),
            (1, False): (1, 2),
        }
        for h in range(halves):

            def remote(k, high):
                values = []
                for index in arrived[(h, high)]:
                    if index is None:
                        values.append(jnp.zeros((pad, LANES), jnp.float32))
                    else:
                        slot = index % 2 * groups + k
                        values.append(turn(got_ref[index // 2], (last if high else 0) - slot))
                return jnp.where(lower, values[0], values[1])

            add_direction(faces, h, 2, remote, up, down, n, groups, pad)
        for dst_x, dst, h in ((keep_x, keep, comp), (send_x, send, 1 - comp)):
            for k in range(groups):
                dst_x[k * n * n : (k + 1) * n * n, :] = faces[h, 0, k, 0 : n * n, :]
                for s in (1, 2):
                    dst[pl.ds(starts[s] + k * mid[s], mid[s]), :] = middle_rows(faces.at[h, 2 * s, k], s, n)
            x = faces.at[h, 1, groups - 1]
            dst_x[groups * n * n : groups * n * n + tall, :] = jnp.where(
                lane_iota(tall) < STRIDE[0], turn(x[0:tall, :], STRIDE[0]), x[tall : n * n, :]
            )
            for s in (1, 2):
                pieces = []
                size = mid[s] // 2
                for k in range(groups):
                    rows = middle_rows(faces.at[h, 2 * s + 1, k], s, n)
                    for part in range(2):
                        pieces.append(
                            (part * groups + k, (BLOCK_Y, BLOCK_Z)[s - 1] - 1, rows[part * size : (part + 1) * size])
                        )
                dst[pl.ds(starts[2 + s], size), :] = gather_slots(size, s, pieces)

    return pl.pallas_call(
        body,
        out_shape=whole(faces_in.shape, *[(total, LANES) for total in totals * 2]),
        scratch_shapes=[pltpu.VMEM((groups, pad, LANES), jnp.float32)] * 2,
        input_output_aliases={0: 0},
        compiler_params=vmem_params(),
        name="add_z",
    )(faces_in, got)[1:]


def unpack(pack, s, n, groups):
    _, mid, tall, starts, _ = pack_layout(n, groups)
    if s == 0:
        first = lane_iota(n * n) < STRIDE[0]
        low = [pack[k * n * n : (k + 1) * n * n, :] for k in range(groups)]
        edge = pack[groups * n * n : groups * n * n + tall, :]
        edge_full = jnp.concatenate([turn(edge, STRIDE[0]), edge], axis=0)
        high = []
        for k in range(groups):
            after = turn(low[k + 1], STRIDE[0]) if k + 1 < groups else edge_full
            high.append(jnp.where(first, turn(low[k], STRIDE[0]), after))
        return low, high
    low = [pack[pl.ds(starts[s] + k * mid[s], mid[s]), :] for k in range(groups)]
    edge = pack[pl.ds(starts[2 + s], mid[s] // 2), :]
    last = (BLOCK_Y, BLOCK_Z)[s - 1] - 1
    part = lane_part(mid[s], s)
    high = []
    for k in range(groups):
        far = jnp.concatenate([turn(edge, (last - (p * groups + k)) * STRIDE[s]) for p in range(2)], axis=0)
        high.append(jnp.where(part == last, far, turn(low[k], -STRIDE[s])))
    return low, high


def to_elements(pack, matrix, s, n, groups, store, after=None):
    inner = n - 2
    for side, x in enumerate(unpack(pack, s, n, groups)):
        y = split_dot(jnp.concatenate(x, axis=1), matrix, ((1,), (0,)))
        at = side * (n - 1)
        for k in range(groups):
            z = y[:, k * LANES : (k + 1) * LANES]

            def flat(row, count, step=1):
                return pl.ds(row * groups + k, count, stride=step * groups)

            if s == 0:
                store(flat(at * n * n, n * n), z[: n * n])
            for a in range(inner):
                base = (a + 1) * n * n
                if s == 1:
                    store(flat(base + at * n, n), z[a * n : a * n + n])
                if s == 2:
                    store(flat(base + n + at, inner, n), z[a * inner : (a + 1) * inner])
        if after is not None:
            after(side)


def early_kernel(own_x, own_face, part, got_in, place, *, n, halves):
    size = place.shape[1]
    groups = size // LANES
    inner = n - 2

    def body(ox, of, part_ref, gi, place_ref, out_s, matrix_ref):
        comp = lax.axis_index("comp")
        matrix = one_hot(place_ref[...])
        matrix = jnp.concatenate([matrix, matrix], axis=0)
        matrix_ref[...] = matrix

        def store(rows, value):
            out_s[rows, :] = value

        for s in range(3):
            to_elements(of if s else ox, matrix, s, n, groups, store)
        for a in range(inner):
            start = plane_at(a + 1, comp, n) + comp
            for b in range(inner):
                for k in range(groups):
                    src = pl.ds(((a * inner + b) * groups + k) * inner, inner)
                    base = (a + 1) * n * n + (b + 1) * n + 1
                    own = part_ref[pl.ds(start + (((b + 1) * n + 1) * 8 + k * halves), inner, stride=8), :]
                    out_s[pl.ds(base * groups + k, inner, stride=groups), :] = own + gi[src, :]

    return pl.pallas_call(
        body,
        out_shape=[
            jax.ShapeDtypeStruct((n * n * n * groups, LANES), jnp.float32),
            jax.ShapeDtypeStruct((2 * size, size), jnp.bfloat16),
        ],
        compiler_params=vmem_params(),
        name="early",
    )(own_x, own_face, part, got_in, place)


def outer_rows(n, groups):
    return (n * n * groups + 7) // 8 * 8


def middle_kernel(early, matrix, got_face, *, n):
    total = early.shape[0]
    groups = total // (n * n * n)
    edge = outer_rows(n, groups)

    def body(early_ref, matrix_ref, gf, out_s, out, sem):
        def store(rows, value):
            out_s[rows, :] = out_s[rows, :] + value

        matrix = matrix_ref[...]
        for s in (1, 2):
            to_elements(gf, matrix, s, n, groups, store)
        rows = pl.ds(edge, total - 2 * edge)
        done = pltpu.make_async_copy(out_s.at[rows, :], out.at[rows, :], sem)
        done.start()
        done.wait()

    return pl.pallas_call(
        body,
        out_shape=whole(early.shape, early.shape),
        out_specs=[pl.BlockSpec(memory_space=pltpu.VMEM), pl.BlockSpec(memory_space=pltpu.HBM)],
        scratch_shapes=[pltpu.SemaphoreType.DMA],
        input_output_aliases={0: 0},
        compiler_params=vmem_params(),
        name="middle",
    )(early, matrix, got_face)


def final_kernel(early, result, matrix, got_x, *, n):
    total = early.shape[0]
    groups = total // (n * n * n)
    edge = outer_rows(n, groups)

    def body(early_ref, result_ref, matrix_ref, gx, out, ends, sem):
        far = total - edge
        ends[0:edge, :] = early_ref[0:edge, :]
        ends[edge : 2 * edge, :] = early_ref[far:total, :]

        def store(rows, value):
            start = rows.start if rows.start < edge else rows.start - far + edge
            here = pl.ds(start, rows.size, stride=rows.stride)
            ends[here, :] = ends[here, :] + value

        done = [
            pltpu.make_async_copy(ends.at[pl.ds(i * edge, edge), :], out.at[pl.ds(i * far, edge), :], sem.at[i])
            for i in range(2)
        ]
        to_elements(gx, matrix_ref[...], 0, n, groups, store, lambda side: done[side].start())
        for c in done:
            c.wait()

    return pl.pallas_call(
        body,
        out_shape=whole(early.shape)[0],
        in_specs=[
            pl.BlockSpec(memory_space=pltpu.VMEM),
            pl.BlockSpec(memory_space=pltpu.HBM),
            pl.BlockSpec(memory_space=pltpu.VMEM),
            pl.BlockSpec(memory_space=pltpu.VMEM),
        ],
        out_specs=pl.BlockSpec(memory_space=pltpu.HBM),
        scratch_shapes=[pltpu.VMEM((2 * edge, LANES), jnp.float32), pltpu.SemaphoreType.DMA((2,))],
        input_output_aliases={1: 0},
        compiler_params=vmem_params(),
        name="final",
    )(early, result, matrix, got_x)


def pairing(at, extent, odd):
    return (at + (1 if at % 2 == (1 if odd else 0) else -1)) % extent


def neighbour_pairs(count, along_x, odd):
    extent = count // GRID_Y if along_x else GRID_Y
    if extent == 1 or (odd and extent == 2):
        return []
    pairs = []
    for e in range(count):
        sx, sy = divmod(e, GRID_Y)
        to = pairing(sx, extent, odd) * GRID_Y + sy if along_x else sx * GRID_Y + pairing(sy, extent, odd)
        pairs.append((e, to))
    return pairs


def exchange(value, along_x, odd):
    pairs = neighbour_pairs(lax.axis_size("elem"), along_x, odd)
    return lax.ppermute(value, "elem", pairs) if pairs else jnp.zeros_like(value)


def body(velocity, geometry, element_place):
    n = velocity.shape[1] * lax.axis_size("comp")
    swap = [(0, 1), (1, 0)]
    other_place = lax.ppermute(element_place, "comp", swap)
    velocity = pltpu.with_memory_space_constraint(velocity, pltpu.HBM)
    geometry = pltpu.with_memory_space_constraint(geometry, pltpu.HBM)
    send_in, part = flux_kernel(velocity, geometry, node_count=n)
    got_in = lax.ppermute(send_in, "comp", swap)
    halves = velocity.shape[4]
    even, odd = edge_kernel(part, element_place, other_place, n=n, halves=halves)
    even = exchange(even, True, False)
    odd = exchange(odd, True, True)
    faces = place_kernel(part, element_place, other_place, n=n, halves=halves)
    faces, even, odd = x_kernel(faces, even, odd, n=n)
    odd = exchange(odd, False, True)
    even = exchange(even, False, False)
    faces, out = y_kernel(faces, even, odd, n=n)
    got = lax.ppermute(out, "rep", swap)
    own_x, own_face, send_x, send_face = z_kernel(faces, got, n=n)
    got_face = lax.ppermute(send_face, "comp", swap)
    got_x = lax.ppermute(send_x, "comp", swap)
    early, matrix = early_kernel(own_x, own_face, part, got_in, element_place, n=n, halves=halves)
    early, result = middle_kernel(early, matrix, got_face, n=n)
    result = final_kernel(early, result, matrix, got_x, n=n)
    return result.reshape(n, n, n, 1, element_place.shape[1])


def solution(mesh):
    placed = (
        P(None, "comp", None, None, None, ("elem", "rep")),
        P(None, None, "comp", None, None, None, ("elem", "rep")),
        P("comp", ("elem", "rep")),
    )

    step = jax.shard_map(
        body,
        mesh=mesh,
        in_specs=placed,
        out_specs=P(None, None, None, "comp", ("elem", "rep")),
        check_vma=False,
    )

    def run(velocity, geometry, element_place):
        with jax.sharding.use_abstract_mesh(mesh.abstract_mesh):
            return step(velocity, geometry, element_place)

    return run
```

```python
import jax
import jax.numpy as jnp
import numpy as np
from jax import lax
from jax.experimental import pallas as pl
from jax.experimental.pallas import tpu as pltpu
from jax.sharding import PartitionSpec as P


BLOCK_Y = 8
BLOCK_Z = 8
GRID_Y = 4
LANES = 128

SLAB_AXES = ((1, 2), (0, 2), (0, 1))


def legendre_columns(points, degree):
    columns = [points * 0.0 + 1.0, points]
    for order in range(2, degree + 1):
        columns.append(
            ((2 * order - 1) * points * columns[order - 1] - (order - 1) * columns[order - 2])
            / order
        )
    return columns


def derivative_table(node_count):
    degree = node_count - 1
    points = np.cos(np.pi * np.arange(node_count) / degree)
    for _ in range(100):
        columns = legendre_columns(points, degree)
        points = points - (points * columns[degree] - columns[degree - 1]) / (
            node_count * columns[degree]
        )
    points = np.sort(points)
    values = legendre_columns(points, degree)[degree]
    identity = np.eye(node_count)
    spacing = points[:, None] - points[None, :] + identity
    matrix = values[:, None] / (values[None, :] * spacing)
    matrix = np.where(identity > 0.5, 0.0, matrix)
    matrix[0, 0] = -degree * (degree + 1) / 4.0
    matrix[degree, degree] = degree * (degree + 1) / 4.0
    return matrix


def weighted(terms):
    total = None
    for value, factor in terms:
        total = value * factor if total is None else total + value * factor
    return total


def transpose_line(line, table):
    count = len(line)
    half = count // 2
    even = [line[i] + line[count - 1 - i] for i in range(half)]
    odd = [line[i] - line[count - 1 - i] for i in range(half)]
    out = [None] * count
    for m in range(half):
        w = count - 1 - m
        both = weighted([(odd[i], float(0.5 * (table[i, m] + table[i, w]))) for i in range(half)])
        diff = weighted([(even[i], float(0.5 * (table[i, m] - table[i, w]))) for i in range(half)])
        out[m] = both + diff
        out[w] = both - diff
    return out


def rows_padded(node_count):
    return (node_count * node_count + 7) // 8 * 8


def in_pairs(start, count, step):
    def pair(i, carry):
        step(start + 2 * i)
        step(start + 2 * i + 1)
        return carry

    lax.fori_loop(0, count // 2, pair, 0)


def plane_at(plane, comp, n):
    return jnp.where(comp == 0, plane, (plane + n // 2) % n) * (n * n * 8)


def flux_kernel(velocity, geometry, *, node_count):
    n = node_count
    planes = velocity.shape[1]
    groups = velocity.shape[5] // LANES
    halves = velocity.shape[4]
    table = derivative_table(n)
    inner = n - 2
    cut = n // 4 * 2
    blocks = [(0, 0, cut), (0, cut, n - cut)]
    blocks += [(plane, 0, n) for plane in range(1, planes - 1)]
    blocks += [(planes - 1, 0, n - 2), (planes - 1, n - 2, 2)]

    def body(v_hbm, g_hbm, send, part, v, g, f1, sem):
        comp = lax.axis_index("comp")
        first = comp == 0

        def copies(index):
            plane, start, count = blocks[index]
            rows = pl.ds(start, count)
            out = []
            for k in range(groups):
                lanes = pl.ds(k * LANES, LANES)
                subs = pl.ds(k * halves, halves)
                out.append(
                    pltpu.make_async_copy(
                        v_hbm.at[:, plane, rows, :, :, lanes], v.at[plane, :, rows, :, subs, :], sem.at[2 * k, index]
                    )
                )
                out.append(
                    pltpu.make_async_copy(
                        g_hbm.at[:, :, plane, rows, :, :, lanes],
                        g.at[plane, :, :, rows, :, subs, :],
                        sem.at[2 * k + 1, index],
                    )
                )
            return out

        for index in range(len(blocks)):
            for c in copies(index):
                c.start()

        def row_of(m, b, c):
            return pl.ds(pl.multiple_of((m * n * n + b * n + c) * 8, 8), 8)

        for index, (plane, start, count) in enumerate(blocks):
            coef = [
                jnp.where(first, float(table[plane, m]), float(table[planes + plane, (m + planes) % n]))
                for m in range(n)
            ]
            for c in copies(index):
                c.wait()

            def along_ends(b):
                line = []
                rows = []
                for c in range(n):
                    vel = [v[plane, i, b, c] for i in range(3)]
                    flux = [
                        weighted([(g[plane, i, j, b, c], vel[i]) for i in range(3)]) for j in range(3)
                    ]
                    f1[b, c] = flux[1]
                    line.append(flux[2])
                    rows.append([flux[0] * coef[m] for m in range(n)])
                out = transpose_line(line, table)
                for c in range(n):
                    for m in range(n):
                        value = rows[c][m] + out[c] if m == plane else rows[c][m]
                        row = row_of(m, b, c)
                        part[row, :] = value if plane == 0 else part[row, :] + value

            in_pairs(start, count, along_ends)
            if start + count < n:
                continue

            def along_middle(c):
                out = transpose_line([f1[b, c] for b in range(n)], table)
                for b in range(n):
                    row = row_of(plane, b, c)
                    part[row, :] = part[row, :] + out[b]

            in_pairs(0, n, along_middle)
        for a in range(inner):
            base = plane_at(a + 1, comp, n) + 1 - comp
            for b in range(inner):
                for k in range(groups):
                    send[pl.ds(((a * inner + b) * groups + k) * inner, inner), :] = part[
                        pl.ds(base + (((b + 1) * n + 1) * 8 + k * halves), inner, stride=8), :
                    ]

    tile = (8, LANES)
    return pl.pallas_call(
        body,
        in_specs=[pl.BlockSpec(memory_space=pltpu.HBM), pl.BlockSpec(memory_space=pltpu.HBM)],
        out_shape=whole((inner * inner * inner * groups, LANES), (n * n * n * 8, LANES)),
        scratch_shapes=[
            pltpu.VMEM((planes, 3, n, n) + tile, jnp.float32),
            pltpu.VMEM((planes, 3, 3, n, n) + tile, jnp.float32),
            pltpu.VMEM((n, n) + tile, jnp.float32),
            pltpu.SemaphoreType.DMA((2 * groups, planes + 2)),
        ],
        compiler_params=pltpu.CompilerParams(vmem_limit_bytes=42 * 2**20),
        name="flux",
    )(velocity, geometry)


def lane_iota(rows):
    return lax.broadcasted_iota(jnp.int32, (rows, LANES), 1)


def lane_part(rows, direction):
    lane = lane_iota(rows)
    if direction == 0:
        return lane // (BLOCK_Y * BLOCK_Z)
    if direction == 1:
        return lane // BLOCK_Z % BLOCK_Y
    return lane % BLOCK_Z


STRIDE = (BLOCK_Y * BLOCK_Z, BLOCK_Z, 1)


def turn(x, by):
    by = by % LANES
    return x if by == 0 else pltpu.roll(x, by, 1)


def split_dot(x, matrix, dims):
    both = jnp.concatenate(bf16_pair(x), axis=1)
    return lax.dot_general(both, matrix, (dims, ((), ())), preferred_element_type=jnp.float32)


def one_hot(place):
    size = place.shape[1]
    target = lax.broadcasted_iota(jnp.int32, (size, size), 0)
    return jnp.where(target == place, 1.0, 0.0).astype(jnp.bfloat16)


def gather_slots(pad, direction, pieces):
    part = lane_part(pad, direction)
    out = jnp.zeros((pad, LANES), jnp.float32)
    for slot, source, value in pieces:
        out = jnp.where(part == slot, turn(value, (slot - source) * STRIDE[direction]), out)
    return out


def payload_y(faces, groups, pad, halves):
    high_out = gather_slots(
        pad, 1, [(h * groups + k, BLOCK_Y - 1, faces[h, 3, k]) for h in range(halves) for k in range(groups)]
    )
    low_out = gather_slots(
        pad, 1, [(h * groups + k, 0, faces[h, 2, k]) for h in range(halves) for k in range(groups)]
    )
    return high_out, low_out


def row_pick(slab_axes, axis, at, n):
    if slab_axes[0] == axis:
        return pl.ds(at * n, n)
    return pl.ds(at, n, stride=n)


def add_rows(faces, h, direction, up, down, n, picks):
    mine = SLAB_AXES[direction]
    for other in range(3):
        if other == direction:
            continue
        for side in range(2):
            source = row_pick(mine, other, side * (n - 1), n)
            for k, high in picks:
                view = faces.at[h, 2 * other + side, k]
                target = row_pick(SLAB_AXES[other], direction, (n - 1) if high else 0, n)
                delta = up if high else down
                view[target, :] = view[target, :] + delta.at[k][source, :]


def both_picks(groups):
    return [(k, high) for k in range(groups) for high in (False, True)]


def add_direction(faces, h, direction, remote, up, down, n, groups, pad):
    part = lane_part(pad, direction)
    low = [faces[h, 2 * direction, k] for k in range(groups)]
    high = [faces[h, 2 * direction + 1, k] for k in range(groups)]
    zero = jnp.zeros((pad, LANES), jnp.float32)
    for k in range(groups):
        if direction == 0:
            first = lane_iota(pad) < STRIDE[0]
            here = turn(low[k], STRIDE[0])
            after = turn(low[k + 1], STRIDE[0]) if k + 1 < groups else zero
            to_high = jnp.where(first, here, after)
            before = turn(high[k - 1], STRIDE[0]) if k > 0 else zero
            to_low = jnp.where(first, before, turn(high[k], STRIDE[0]))
        else:
            last = (BLOCK_Y, BLOCK_Z)[direction - 1] - 1
            to_high = jnp.where(part == last, remote(k, True), turn(low[k], -STRIDE[direction]))
            to_low = jnp.where(part == 0, remote(k, False), turn(high[k], STRIDE[direction]))
        faces[h, 2 * direction, k] = low[k] + to_low
        faces[h, 2 * direction + 1, k] = high[k] + to_high
        up[k] = to_high
        down[k] = to_low
    add_rows(faces, h, direction, up, down, n, both_picks(groups))


def add_outer_x(faces, h, for_high, for_low, up, down, n, groups, pad):
    first = lane_iota(pad) < STRIDE[0]
    last = groups - 1
    to_high = jnp.where(first, 0.0, turn(for_high, STRIDE[0]) if h == 0 else for_high)
    to_low = jnp.where(first, for_low if h == 0 else turn(for_low, STRIDE[0]), 0.0)
    faces[h, 1, last] = faces[h, 1, last] + to_high
    faces[h, 0, 0] = faces[h, 0, 0] + to_low
    up[last] = to_high
    down[0] = to_low
    add_rows(faces, h, 0, up, down, n, [(last, True), (0, False)])


def parity_split(even, high_out, low_out):
    return jnp.where(even, high_out, low_out), jnp.where(even, low_out, high_out)


def whole(*shapes):
    return [jax.ShapeDtypeStruct(s, jnp.float32) for s in shapes]


def vmem_params():
    return pltpu.CompilerParams(vmem_limit_bytes=40 * 2**20)


def face_rows(part, s, k, h, n, halves, store, direction=None):
    comp = lax.axis_index("comp")
    direction = s // 2 if direction is None else direction
    at = s % 2 * (n - 1)
    sub = k * halves + h
    if direction == 0:
        store(0, n * n, part[pl.ds(plane_at(at, comp, n) + sub, n * n, stride=8), :])
    elif direction == 2:
        count = n * n // 2
        for p in range(2):
            start = plane_at(p * (n // 2), comp, n) + at * 8 + sub
            store(p * count, count, part[pl.ds(start, count, stride=8 * n), :])
    else:
        for a in range(n):
            store(a * n, n, part[pl.ds(plane_at(a, comp, n) + at * n * 8 + sub, n, stride=8), :])


def bf16_pair(x):
    high = x.astype(jnp.bfloat16)
    return [high, (x - high.astype(jnp.float32)).astype(jnp.bfloat16)]


def edge_kernel(part, own, other, *, n, halves):
    size = own.shape[1]
    groups = size // LANES
    pad = rows_padded(n)
    step = STRIDE[0]

    single = lax.axis_size("elem") // GRID_Y <= 2

    def body(part_ref, own_ref, other_ref, x_even, *refs):
        x_odd, rows = refs[:-1], refs[-1]
        comp = lax.axis_index("comp")
        elem = lax.axis_index("elem")
        up = elem // GRID_Y % 2 == 0
        sides = [jnp.where(up, 1, 0)] if single else [0, 1]
        payload = []
        for index, side in enumerate(sides):
            pieces = []
            match = []
            for h in range(halves):
                place = jnp.where(comp == h, own_ref[...], other_ref[...])
                lane = lax.broadcasted_iota(jnp.int32, (LANES, size), 0)
                goal = jnp.where(lane // step == h, lane - h * step + side * (size - step), -1)
                one = jnp.where(goal == place, 1.0, 0.0).astype(jnp.bfloat16)
                match += [one, one]
                for k in range(groups):

                    def store(at, count, value):
                        rows[index, h, k, at : at + count, :] = value

                    face_rows(part_ref, side, k, h, n, halves, store, 0)
                pieces += bf16_pair(jnp.concatenate([rows[index, h, k] for k in range(groups)], axis=1))
            payload.append(
                lax.dot_general(
                    jnp.concatenate(pieces, axis=1),
                    jnp.concatenate(match, axis=1),
                    (((1,), (1,)), ((), ())),
                    preferred_element_type=jnp.float32,
                )
            )
        if single:
            x_even[...] = payload[0]
        else:
            x_even[...], x_odd[0][...] = parity_split(up, payload[1], payload[0])

    outs = pl.pallas_call(
        body,
        out_shape=whole(*[(pad, LANES)] * (1 if single else 2)),
        scratch_shapes=[pltpu.VMEM((2, halves, groups, pad, LANES), jnp.float32)],
        compiler_params=vmem_params(),
        name="edge",
    )(part, own, other)
    return outs[0], outs[-1]


def place_kernel(part, own, other, *, n, halves):
    groups = own.shape[1] // LANES
    pad = rows_padded(n)
    shape = (halves, 6, groups, pad, LANES)

    def body(part_ref, own_ref, other_ref, faces, line_rows, up, down):
        comp = lax.axis_index("comp")
        for h in range(halves):
            place = jnp.where(comp == h, own_ref[...], other_ref[...])
            matrix = one_hot(place)
            matrix = jnp.concatenate([matrix, matrix], axis=1)
            for s in range(6):
                for k in range(groups):

                    def store(at, count, value):
                        line_rows[s, k, at : at + count, :] = value

                    face_rows(part_ref, s, k, h, n, halves, store)
                x = jnp.concatenate([line_rows[s, k] for k in range(groups)], axis=1)
                y = split_dot(x, matrix, ((1,), (1,)))
                for k in range(groups):
                    faces[h, s, k] = y[:, k * LANES : (k + 1) * LANES]
        for h in range(halves):
            add_direction(faces, h, 0, None, up, down, n, groups, pad)

    return pl.pallas_call(
        body,
        out_shape=whole(shape)[0],
        scratch_shapes=[pltpu.VMEM(shape[1:], jnp.float32)] + [pltpu.VMEM((groups, pad, LANES), jnp.float32)] * 2,
        compiler_params=vmem_params(),
        name="place",
    )(part, own, other)


def parity_remote(at, extent, got_even, got_odd):
    even = at % 2 == 0
    high = jnp.where(even, got_even, got_odd)
    low = jnp.where(even, got_odd, got_even)
    return jnp.where(at + 1 < extent, high, 0.0), jnp.where(at > 0, low, 0.0)


def x_kernel(faces_in, got_even, got_odd, *, n):
    halves, _, groups, pad, _ = faces_in.shape

    def body(faces_ref, even_ref, odd_ref, faces, out_even, out_odd, up, down):
        elem = lax.axis_index("elem")
        extent = lax.axis_size("elem") // GRID_Y
        for_high, for_low = parity_remote(elem // GRID_Y, extent, even_ref[...], odd_ref[...])
        for h in range(halves):
            add_outer_x(faces, h, for_high, for_low, up, down, n, groups, pad)
        out_even[...], out_odd[...] = parity_split(
            elem % GRID_Y % 2 == 0, *payload_y(faces, groups, pad, halves)
        )

    return pl.pallas_call(
        body,
        out_shape=whole(faces_in.shape, (pad, LANES), (pad, LANES)),
        scratch_shapes=[pltpu.VMEM((groups, pad, LANES), jnp.float32)] * 2,
        input_output_aliases={0: 0},
        compiler_params=vmem_params(),
        name="add_x",
    )(faces_in, got_even, got_odd)


def y_kernel(faces_in, got_even, got_odd, *, n):
    halves, _, groups, pad, _ = faces_in.shape
    last = BLOCK_Z - 1

    def body(faces_ref, even_ref, odd_ref, faces, out, up, down):
        elem = lax.axis_index("elem")
        rep = lax.axis_index("rep")
        for_high, for_low = parity_remote(elem % GRID_Y, GRID_Y, even_ref[...], odd_ref[...])
        for h in range(halves):

            def remote(k, high):
                slot = h * groups + k
                if high:
                    return turn(for_high, (BLOCK_Y - 1 - slot) * STRIDE[1])
                return turn(for_low, -slot * STRIDE[1])

            add_direction(faces, h, 1, remote, up, down, n, groups, pad)
        lower = rep == 0
        choices = (((0, 1), (0, 0)), ((1, 0), (0, 1)), ((1, 1), (1, 0)))
        outs = []
        for mine, theirs in choices:
            pair = []
            for h, side in (mine, theirs):
                pair.append((h, side))
            outs.append(pair)
        part = lane_part(pad, 2)
        for page in range(2):
            value = jnp.zeros((pad, LANES), jnp.float32)
            for index, (a, b) in enumerate(outs):
                if index // 2 != page:
                    continue
                for k in range(groups):
                    slot = index % 2 * groups + k
                    one = turn(faces[a[0], 4 + a[1], k], slot - a[1] * last)
                    two = turn(faces[b[0], 4 + b[1], k], slot - b[1] * last)
                    value = jnp.where(part == slot, jnp.where(lower, one, two), value)
            out[page] = value

    return pl.pallas_call(
        body,
        out_shape=whole(faces_in.shape, (2, pad, LANES)),
        scratch_shapes=[pltpu.VMEM((groups, pad, LANES), jnp.float32)] * 2,
        input_output_aliases={0: 0},
        compiler_params=vmem_params(),
        name="add_y",
    )(faces_in, got_even, got_odd)


def pack_layout(n, groups):
    pad = rows_padded(n)
    mid = (0, (n - 2) * n, (n - 2) * (n - 2))
    tall = n * n // 2
    x_sizes = [n * (n - 1) * groups, tall, n]
    sizes = [mid[1] * groups, mid[2] * groups, mid[1] // 2, mid[2] // 2]
    starts = [0] + [sum(sizes[:i]) for i in range(4)]
    return pad, mid, tall, starts, (sum(x_sizes), sum(sizes))


def middle_rows(view, s, n):
    if s == 1:
        return view[n : n * (n - 1), :]
    return jnp.concatenate([view[a * n + 1 : a * n + n - 1, :] for a in range(1, n - 1)], axis=0)


def z_kernel(faces_in, got, *, n):
    halves, _, groups, pad, _ = faces_in.shape
    last = BLOCK_Z - 1
    _, mid, tall, starts, totals = pack_layout(n, groups)
    short = n * (n - 1)

    def body(faces_ref, got_ref, faces, keep_x, keep, send_x, send, up, down):
        rep = lax.axis_index("rep")
        comp = lax.axis_index("comp")
        lower = rep == 0
        arrived = {
            (0, True): (0, 1),
            (0, False): (None, 0),
            (1, True): (2, None),
            (1, False): (1, 2),
        }
        for h in range(halves):

            def remote(k, high):
                values = []
                for index in arrived[(h, high)]:
                    if index is None:
                        values.append(jnp.zeros((pad, LANES), jnp.float32))
                    else:
                        slot = index % 2 * groups + k
                        values.append(turn(got_ref[index // 2], (last if high else 0) - slot))
                return jnp.where(lower, values[0], values[1])

            add_direction(faces, h, 2, remote, up, down, n, groups, pad)
        for dst_x, dst, h in ((keep_x, keep, comp), (send_x, send, 1 - comp)):
            for k in range(groups):
                dst_x[k * short : (k + 1) * short, :] = faces[h, 0, k, 0:short, :]
                for s in (1, 2):
                    dst[pl.ds(starts[s] + k * mid[s], mid[s]), :] = middle_rows(faces.at[h, 2 * s, k], s, n)
            x = faces.at[h, 1, groups - 1]
            dst_x[groups * short + tall : groups * short + tall + n, :] = gather_slots(
                n, 1, [(k, BLOCK_Y - 1, faces[h, 0, k, short : n * n, :]) for k in range(groups)]
            )
            dst_x[groups * short : groups * short + tall, :] = jnp.where(
                lane_iota(tall) < STRIDE[0], turn(x[0:tall, :], STRIDE[0]), x[tall : n * n, :]
            )
            for s in (1, 2):
                pieces = []
                size = mid[s] // 2
                for k in range(groups):
                    rows = middle_rows(faces.at[h, 2 * s + 1, k], s, n)
                    for part in range(2):
                        pieces.append(
                            (part * groups + k, (BLOCK_Y, BLOCK_Z)[s - 1] - 1, rows[part * size : (part + 1) * size])
                        )
                dst[pl.ds(starts[2 + s], size), :] = gather_slots(size, s, pieces)

    return pl.pallas_call(
        body,
        out_shape=whole(faces_in.shape, *[(total, LANES) for total in totals * 2]),
        scratch_shapes=[pltpu.VMEM((groups, pad, LANES), jnp.float32)] * 2,
        input_output_aliases={0: 0},
        compiler_params=vmem_params(),
        name="add_z",
    )(faces_in, got)[1:]


def unpack(pack, s, n, groups):
    _, mid, tall, starts, _ = pack_layout(n, groups)
    if s == 0:
        first = lane_iota(n * n) < STRIDE[0]
        short = n * (n - 1)
        low = []
        outer = pack[groups * short + tall : groups * short + tall + n, :]
        for k in range(groups):
            rows = pack[k * short : (k + 1) * short, :]
            far = turn(outer, (BLOCK_Y - 1 - k) * STRIDE[1])
            near = turn(rows[:n], -STRIDE[1])
            low.append(jnp.concatenate([rows, jnp.where(lane_part(n, 1) == BLOCK_Y - 1, far, near)], axis=0))
        edge = pack[groups * short : groups * short + tall, :]
        edge_full = jnp.concatenate([turn(edge, STRIDE[0]), edge], axis=0)
        high = []
        for k in range(groups):
            after = turn(low[k + 1], STRIDE[0]) if k + 1 < groups else edge_full
            high.append(jnp.where(first, turn(low[k], STRIDE[0]), after))
        return low, high
    low = [pack[pl.ds(starts[s] + k * mid[s], mid[s]), :] for k in range(groups)]
    edge = pack[pl.ds(starts[2 + s], mid[s] // 2), :]
    last = (BLOCK_Y, BLOCK_Z)[s - 1] - 1
    part = lane_part(mid[s], s)
    high = []
    for k in range(groups):
        far = jnp.concatenate([turn(edge, (last - (p * groups + k)) * STRIDE[s]) for p in range(2)], axis=0)
        high.append(jnp.where(part == last, far, turn(low[k], -STRIDE[s])))
    return low, high


def to_elements(pack, matrix, s, n, groups, store, after=None):
    inner = n - 2
    for side, x in enumerate(unpack(pack, s, n, groups)):
        y = split_dot(jnp.concatenate(x, axis=1), matrix, ((1,), (0,)))
        at = side * (n - 1)
        for k in range(groups):
            z = y[:, k * LANES : (k + 1) * LANES]

            def flat(row, count, step=1):
                return pl.ds(row * groups + k, count, stride=step * groups)

            if s == 0:
                store(flat(at * n * n, n * n), z[: n * n])
            for a in range(inner):
                base = (a + 1) * n * n
                if s == 1:
                    store(flat(base + at * n, n), z[a * n : a * n + n])
                if s == 2:
                    store(flat(base + n + at, inner, n), z[a * inner : (a + 1) * inner])
        if after is not None:
            after(side)


def early_kernel(own_x, own_face, part, got_in, place, *, n, halves):
    size = place.shape[1]
    groups = size // LANES
    inner = n - 2

    def body(ox, of, part_ref, gi, place_ref, out_s, matrix_ref):
        comp = lax.axis_index("comp")
        matrix = one_hot(place_ref[...])
        matrix = jnp.concatenate([matrix, matrix], axis=0)
        matrix_ref[...] = matrix

        def store(rows, value):
            out_s[rows, :] = value

        for s in range(3):
            to_elements(of if s else ox, matrix, s, n, groups, store)
        for a in range(inner):
            start = plane_at(a + 1, comp, n) + comp
            for b in range(inner):
                for k in range(groups):
                    src = pl.ds(((a * inner + b) * groups + k) * inner, inner)
                    base = (a + 1) * n * n + (b + 1) * n + 1
                    own = part_ref[pl.ds(start + (((b + 1) * n + 1) * 8 + k * halves), inner, stride=8), :]
                    out_s[pl.ds(base * groups + k, inner, stride=groups), :] = own + gi[src, :]

    return pl.pallas_call(
        body,
        out_shape=[
            jax.ShapeDtypeStruct((n * n * n * groups, LANES), jnp.float32),
            jax.ShapeDtypeStruct((2 * size, size), jnp.bfloat16),
        ],
        compiler_params=vmem_params(),
        name="early",
    )(own_x, own_face, part, got_in, place)


def outer_rows(n, groups):
    return (n * n * groups + 7) // 8 * 8


def middle_kernel(early, matrix, got_face, *, n):
    total = early.shape[0]
    groups = total // (n * n * n)
    edge = outer_rows(n, groups)

    def body(early_ref, matrix_ref, gf, out_s, out, sem):
        def store(rows, value):
            out_s[rows, :] = out_s[rows, :] + value

        matrix = matrix_ref[...]
        for s in (1, 2):
            to_elements(gf, matrix, s, n, groups, store)
        rows = pl.ds(edge, total - 2 * edge)
        done = pltpu.make_async_copy(out_s.at[rows, :], out.at[rows, :], sem)
        done.start()
        done.wait()

    return pl.pallas_call(
        body,
        out_shape=whole(early.shape, early.shape),
        out_specs=[pl.BlockSpec(memory_space=pltpu.VMEM), pl.BlockSpec(memory_space=pltpu.HBM)],
        scratch_shapes=[pltpu.SemaphoreType.DMA],
        input_output_aliases={0: 0},
        compiler_params=vmem_params(),
        name="middle",
    )(early, matrix, got_face)


def final_kernel(early, result, matrix, got_x, *, n):
    total = early.shape[0]
    groups = total // (n * n * n)
    edge = outer_rows(n, groups)

    def body(early_ref, result_ref, matrix_ref, gx, out, ends, sem):
        far = total - edge
        ends[0:edge, :] = early_ref[0:edge, :]
        ends[edge : 2 * edge, :] = early_ref[far:total, :]

        def store(rows, value):
            start = rows.start if rows.start < edge else rows.start - far + edge
            here = pl.ds(start, rows.size, stride=rows.stride)
            ends[here, :] = ends[here, :] + value

        done = [
            pltpu.make_async_copy(ends.at[pl.ds(i * edge, edge), :], out.at[pl.ds(i * far, edge), :], sem.at[i])
            for i in range(2)
        ]
        to_elements(gx, matrix_ref[...], 0, n, groups, store, lambda side: done[side].start())
        for c in done:
            c.wait()

    return pl.pallas_call(
        body,
        out_shape=whole(early.shape)[0],
        in_specs=[
            pl.BlockSpec(memory_space=pltpu.VMEM),
            pl.BlockSpec(memory_space=pltpu.HBM),
            pl.BlockSpec(memory_space=pltpu.VMEM),
            pl.BlockSpec(memory_space=pltpu.VMEM),
        ],
        out_specs=pl.BlockSpec(memory_space=pltpu.HBM),
        scratch_shapes=[pltpu.VMEM((2 * edge, LANES), jnp.float32), pltpu.SemaphoreType.DMA((2,))],
        input_output_aliases={1: 0},
        compiler_params=vmem_params(),
        name="final",
    )(early, result, matrix, got_x)


def pairing(at, extent, odd):
    return (at + (1 if at % 2 == (1 if odd else 0) else -1)) % extent


def neighbour_pairs(count, along_x, odd):
    extent = count // GRID_Y if along_x else GRID_Y
    if extent == 1 or (odd and extent == 2):
        return []
    pairs = []
    for e in range(count):
        sx, sy = divmod(e, GRID_Y)
        to = pairing(sx, extent, odd) * GRID_Y + sy if along_x else sx * GRID_Y + pairing(sy, extent, odd)
        pairs.append((e, to))
    return pairs


def exchange(value, along_x, odd):
    pairs = neighbour_pairs(lax.axis_size("elem"), along_x, odd)
    return lax.ppermute(value, "elem", pairs) if pairs else jnp.zeros_like(value)


def body(velocity, geometry, element_place):
    n = velocity.shape[1] * lax.axis_size("comp")
    swap = [(0, 1), (1, 0)]
    other_place = lax.ppermute(element_place, "comp", swap)
    velocity = pltpu.with_memory_space_constraint(velocity, pltpu.HBM)
    geometry = pltpu.with_memory_space_constraint(geometry, pltpu.HBM)
    send_in, part = flux_kernel(velocity, geometry, node_count=n)
    got_in = lax.ppermute(send_in, "comp", swap)
    halves = velocity.shape[4]
    even, odd = edge_kernel(part, element_place, other_place, n=n, halves=halves)
    even = exchange(even, True, False)
    odd = exchange(odd, True, True)
    faces = place_kernel(part, element_place, other_place, n=n, halves=halves)
    faces, even, odd = x_kernel(faces, even, odd, n=n)
    odd = exchange(odd, False, True)
    even = exchange(even, False, False)
    faces, out = y_kernel(faces, even, odd, n=n)
    got = lax.ppermute(out, "rep", swap)
    own_x, own_face, send_x, send_face = z_kernel(faces, got, n=n)
    got_face = lax.ppermute(send_face, "comp", swap)
    got_x = lax.ppermute(send_x, "comp", swap)
    early, matrix = early_kernel(own_x, own_face, part, got_in, element_place, n=n, halves=halves)
    early, result = middle_kernel(early, matrix, got_face, n=n)
    result = final_kernel(early, result, matrix, got_x, n=n)
    return result.reshape(n, n, n, 1, element_place.shape[1])


def solution(mesh):
    placed = (
        P(None, "comp", None, None, None, ("elem", "rep")),
        P(None, None, "comp", None, None, None, ("elem", "rep")),
        P("comp", ("elem", "rep")),
    )

    step = jax.shard_map(
        body,
        mesh=mesh,
        in_specs=placed,
        out_specs=P(None, None, None, "comp", ("elem", "rep")),
        check_vma=False,
    )

    def run(velocity, geometry, element_place):
        with jax.sharding.use_abstract_mesh(mesh.abstract_mesh):
            return step(velocity, geometry, element_place)

    return run
```
